128 devices in a mesh: seq: 64 (over y, z_hi, x, core), tp: 2 (over z_lo).
Axes of the slice: x: 4, y: 4, z: 4 (z_hi: 2, z_lo: 2; z = z_hi * 2 + z_lo), core: 2. Of those that a mesh axis runs over, the one named last changes fastest.
Arguments:
- query_rows: bfloat16 [8192, 2048], P('seq', 'tp'), may hold values from -350 to 350
- key_rows: bfloat16 [8192, 512], P('seq', 'tp'), may hold values from -6 to 6
- stored_value_rows: bfloat16 [8192, 512], P('seq', 'tp'), may hold values from -6 to 6
- output_grad: bfloat16 [8192, 2048], P('seq', 'tp'), may hold values from -96 to 96
- layer_input: bfloat16 [8192, 4096], P('seq', 'tp'), may hold values from -16 to 16
- key_matrix: bfloat16 [4096, 512], P(None, 'tp'), may hold values from -0.09375 to 0.09375
- value_matrix: bfloat16 [4096, 512], P(None, 'tp'), may hold values from -0.09375 to 0.09375
- run_placement: int32 [64, 64], replicated, may hold values from 0 to 63, as said below
Outputs:
- query_grad: bfloat16 [8192, 2048], P('seq', 'tp')
- input_grad: bfloat16 [8192, 4096], P('seq', 'tp')
- key_weight_grad: float32 [4096, 512], P('seq', 'tp')
- value_weight_grad: float32 [4096, 512], P('seq', 'tp')
The draws below stay inside these ranges and needn't reach their ends.
Inputs may be any that keep to these rules, and one draw needn't show every extreme that they name: `run_placement`: row j gives, for each storing index d of seq, the slot within sequence block j of the 2 consecutive positions that d holds; every row is a permutation of 0 to 63.
All inputs are finite; a program needn't handle non-finite values.
Results may differ from the reference program's by a relative error of at most 0.0081.
Values may be sent and summed in bfloat16 or wider, within the bound.
No kernel may reach another device: no remote copies, remote signals or barrier semaphores. Data moves between devices by JAX's collectives and lax.ppermute only.
A program may use at most 128 MiB of HBM per device.

```python
import math
import jax
import jax.numpy as jnp
from jax import lax

MODEL_WIDTH = 4096
HEAD_SIZE = 128
WINDOW_LENGTH = 4096
QUERY_HEADS = 16
KEY_VALUE_HEADS = 4
TOK_DEV = 128
SEQUENCE_TOKENS = 8192
N_SEQ = 64


def slot_table(key):
    row_keys = jax.random.split(jax.random.fold_in(key, 101), N_SEQ)
    return jax.vmap(lambda row_key: jax.random.permutation(row_key, N_SEQ))(row_keys).astype(jnp.int32)


def key_sample(key):
    start_offset = jnp.clip(jax.random.normal(jax.random.fold_in(key, 202), (SEQUENCE_TOKENS, KEY_VALUE_HEADS, HEAD_SIZE), jnp.float32), -4.0, 4.0)
    return start_offset


def draw_run_placement(key, part):
    return slot_table(key)


def draw_key_rows(key, part):
    return key_sample(key).reshape(SEQUENCE_TOKENS, KEY_VALUE_HEADS * HEAD_SIZE).astype(jnp.bfloat16)


def draw_query_rows(key, part):
    start_offset = jnp.clip(jax.random.normal(jax.random.fold_in(key, 303), (SEQUENCE_TOKENS, QUERY_HEADS * HEAD_SIZE), jnp.float32), -4.0, 4.0)
    return start_offset.astype(jnp.bfloat16)


def spiked(drawn, key, source, target, parts, factor):
    owner, partner = [(jnp.arange(drawn.shape[dim]) // (drawn.shape[dim] // parts)).reshape([-1 if axis == dim else 1 for axis in range(drawn.ndim)]) for dim in (source, target)]
    chosen = jax.random.permutation(key, parts)[partner]
    strong = (owner == chosen) | (owner == (partner + parts // 2) % parts)
    return jnp.where(strong, factor * drawn, drawn)


def level_of(own_key, dims, shards, low, largest):
    def one(dim, blocks):
        steps = jax.random.uniform(jax.random.fold_in(jax.random.fold_in(own_key, 6), dim), (blocks,), jnp.float32, low / len(shards), largest / len(shards))
        return jnp.repeat(jnp.exp(steps), dims[dim] // blocks).reshape((-1,) + (1,) * (len(dims) - dim - 1))

    level = one(*shards[0])
    for cut in shards[1:]:
        level = level * one(*cut)
    return level


def normal_values(key, dims, width, reach, cuts=(), kind=jnp.bfloat16):
    drawn = width * jax.random.normal(key, dims, jnp.float32)
    if cuts:
        drawn = drawn * level_of(key, dims, cuts, -0.22, 0.18)
    return jnp.clip(drawn, -reach, reach).astype(kind)


def gaussian_with(rng, extent, scale, bound, cuts, heavy, held_as=jnp.bfloat16):
    array = scale * jax.random.normal(rng, extent, jnp.float32)
    if cuts:
        array = array * level_of(rng, extent, cuts, -0.22, 0.18)
    return jnp.clip(spiked(array, jax.random.fold_in(rng, 3), *heavy), -bound, bound).astype(held_as)


def setup_inputs(seed: int = 0) -> dict:
    key_list = jax.random.split(jax.random.key(seed), 9)
    return {
        "query_rows": draw_query_rows(jax.random.fold_in(key_list[8], 71), 0),
        "key_rows": draw_key_rows(jax.random.fold_in(key_list[8], 71), 0),
        "stored_value_rows": normal_values(key_list[2], (SEQUENCE_TOKENS, KEY_VALUE_HEADS * HEAD_SIZE), 1.0, 6.0, ((0, 64), (1, 2))),
        "output_grad": normal_values(key_list[3], (SEQUENCE_TOKENS, QUERY_HEADS * HEAD_SIZE), 16.0, 96.0, ((0, 64), (1, 2))),
        "layer_input": gaussian_with(key_list[4], (SEQUENCE_TOKENS, MODEL_WIDTH), 1.0, 16.0, ((0, 64), (1, 2)), (0, 1, 64, 4.0)),
        "key_matrix": normal_values(key_list[5], (MODEL_WIDTH, KEY_VALUE_HEADS * HEAD_SIZE), MODEL_WIDTH ** -0.5, 0.09375, ((1, 2),)),
        "value_matrix": normal_values(key_list[6], (MODEL_WIDTH, KEY_VALUE_HEADS * HEAD_SIZE), MODEL_WIDTH ** -0.5, 0.09375, ((1, 2),)),
        "run_placement": draw_run_placement(jax.random.fold_in(key_list[8], 71), 0),
    }


masked_value = -1e+30

def to_sequence(matrix, run_placement):
    run_rows = TOK_DEV // N_SEQ
    columns = matrix.shape[1]
    stored = matrix.reshape(N_SEQ, N_SEQ, run_rows, columns).transpose(1, 0, 2, 3)
    inverse = jnp.argsort(run_placement, axis=1).astype(jnp.int32)
    picked = jnp.take_along_axis(stored, inverse[:, :, None, None], axis=1)
    return picked.reshape(SEQUENCE_TOKENS, columns)

def into_stored_order(matrix, run_placement):
    run_rows = TOK_DEV // N_SEQ
    columns = matrix.shape[1]
    blocks = matrix.reshape(N_SEQ, N_SEQ, run_rows, columns)
    picked = jnp.take_along_axis(blocks, run_placement.astype(jnp.int32)[:, :, None, None], axis=1)
    return picked.transpose(1, 0, 2, 3).reshape(SEQUENCE_TOKENS, columns)

def rounded(values):
    return lax.optimization_barrier(values.astype(jnp.bfloat16)).astype(jnp.float32)

def reference(query_rows, key_rows, stored_value_rows, output_grad, layer_input, key_matrix, value_matrix, run_placement):
    score_scale = 1.0 / math.sqrt(HEAD_SIZE)
    query_group = QUERY_HEADS // KEY_VALUE_HEADS
    queries = to_sequence(query_rows, run_placement)
    grads = to_sequence(output_grad, run_placement)
    empty_rows = jnp.zeros((WINDOW_LENGTH, KEY_VALUE_HEADS * HEAD_SIZE), jnp.bfloat16)
    padded_keys = jnp.concatenate([empty_rows, to_sequence(key_rows, run_placement)], axis=0)
    padded_values = jnp.concatenate([empty_rows, to_sequence(stored_value_rows, run_placement)], axis=0)
    window_keys = WINDOW_LENGTH + TOK_DEV

    def one_block(carry, block_index):
        leading_row = block_index * TOK_DEV
        q_block = lax.dynamic_slice_in_dim(queries, leading_row, TOK_DEV, 0).astype(jnp.float32).reshape(TOK_DEV, QUERY_HEADS, HEAD_SIZE)
        g_block = lax.dynamic_slice_in_dim(grads, leading_row, TOK_DEV, 0).astype(jnp.float32).reshape(TOK_DEV, QUERY_HEADS, HEAD_SIZE)
        key_block = lax.dynamic_slice_in_dim(padded_keys, leading_row, window_keys, 0).astype(jnp.float32).reshape(window_keys, KEY_VALUE_HEADS, HEAD_SIZE)
        value_block = lax.dynamic_slice_in_dim(padded_values, leading_row, window_keys, 0).astype(jnp.float32).reshape(window_keys, KEY_VALUE_HEADS, HEAD_SIZE)
        k_heads = jnp.repeat(key_block, query_group, axis=1)
        v_heads = jnp.repeat(value_block, query_group, axis=1)
        query_pos = leading_row + jnp.arange(TOK_DEV, dtype=jnp.int32)
        key_pos = leading_row - WINDOW_LENGTH + jnp.arange(window_keys, dtype=jnp.int32)
        in_window = (key_pos[None, :] <= query_pos[:, None]) & (key_pos[None, :] > query_pos[:, None] - WINDOW_LENGTH) & (key_pos[None, :] >= 0)
        logits = jnp.einsum('qhd,khd->hqk', q_block, k_heads) * score_scale
        row_top = lax.optimization_barrier(jnp.max(jnp.where(in_window[None], logits, masked_value), axis=2))
        exponent = jnp.where(in_window[None], jnp.exp(logits - row_top[:, :, None]), 0.0)
        row_total = lax.optimization_barrier(jnp.sum(exponent, axis=2))
        log_total = row_top + jnp.log(row_total)
        prob_grad = jnp.einsum('qhd,khd->hqk', g_block, v_heads)
        row_delta = lax.optimization_barrier(jnp.sum(exponent * prob_grad, axis=2)) / row_total
        probs = jnp.where(in_window[None], jnp.exp(logits - log_total[:, :, None]), 0.0)
        score_grad = probs * (prob_grad - row_delta[:, :, None])
        probs_b = rounded(probs)
        score_b = rounded(score_grad)
        query_part = (jnp.einsum('hqk,khd->qhd', score_b, k_heads) * score_scale).astype(jnp.bfloat16)
        key_portion = jnp.einsum('hqk,qhd->khd', score_b, q_block) * score_scale
        key_portion = key_portion.reshape(window_keys, KEY_VALUE_HEADS, query_group, HEAD_SIZE).sum(axis=2).reshape(window_keys, KEY_VALUE_HEADS * HEAD_SIZE)
        value_portion = jnp.einsum('hqk,qhd->khd', probs_b, g_block)
        value_portion = value_portion.reshape(window_keys, KEY_VALUE_HEADS, query_group, HEAD_SIZE).sum(axis=2).reshape(window_keys, KEY_VALUE_HEADS * HEAD_SIZE)
        update = jnp.concatenate([key_portion, value_portion], axis=1)
        current = lax.dynamic_slice_in_dim(carry, leading_row, window_keys, 0)
        carry = lax.dynamic_update_slice_in_dim(carry, current + update, leading_row, 0)
        return (carry, query_part.reshape(TOK_DEV, QUERY_HEADS * HEAD_SIZE))
    gradient_start = jnp.zeros((WINDOW_LENGTH + SEQUENCE_TOKENS, 2 * KEY_VALUE_HEADS * HEAD_SIZE), jnp.float32)
    final, query_parts = lax.scan(one_block, gradient_start, jnp.arange(N_SEQ, dtype=jnp.int32))
    key_value_pair = final[WINDOW_LENGTH:]
    key_gradient = into_stored_order(key_value_pair[:, :KEY_VALUE_HEADS * HEAD_SIZE].astype(jnp.bfloat16), run_placement)
    value_gradient = into_stored_order(key_value_pair[:, KEY_VALUE_HEADS * HEAD_SIZE:].astype(jnp.bfloat16), run_placement)
    query_grad = into_stored_order(query_parts.reshape(SEQUENCE_TOKENS, QUERY_HEADS * HEAD_SIZE), run_placement)
    key_weight_grad = jnp.dot(layer_input.T, key_gradient, preferred_element_type=jnp.float32)
    value_weight_grad = jnp.dot(layer_input.T, value_gradient, preferred_element_type=jnp.float32)
    input_grad = jnp.dot(key_gradient, key_matrix.T, preferred_element_type=jnp.float32)
    input_grad = (input_grad + jnp.dot(value_gradient, value_matrix.T, preferred_element_type=jnp.float32)).astype(jnp.bfloat16)
    return (query_grad, input_grad, key_weight_grad, value_weight_grad)
```

```python
import math

import jax
import jax.numpy as jnp
from jax import lax
from jax.experimental import pallas as pl
from jax.experimental.pallas import tpu as pltpu
from jax.sharding import Mesh
from jax.sharding import PartitionSpec as P

HEAD = 128
WINDOW = 4096
GROUP = 4
TOK = 128
SEQ = ("y", "z", "x", "c")
BF = jnp.bfloat16
F32 = jnp.float32
NEG = -1e30

PARTS = 4
T = TOK // PARTS
SLOTS = 32
KR = SLOTS * T
QR = 4 * GROUP * T
SPAN = PARTS // 2
SCALE = 1.0 / math.sqrt(HEAD)
SCORE2 = SCALE * math.log2(math.e)
VMEM_LIMIT = 60 * 1024 * 1024


def moved(array, axis, by):
    n = lax.axis_size(axis)
    return lax.ppermute(array, axis, [(i, (i + by) % n) for i in range(n)])


def nt(a, b):
    return lax.dot_general(a, b, (((1,), (1,)), ((), ())), preferred_element_type=F32)


def nn(a, b):
    return lax.dot_general(a, b, (((1,), (0,)), ((), ())), preferred_element_type=F32)


def load_parts(k_refs, v_refs, qg_refs, kpos_ref, ks, vs, qs, gs, kposb):
    for part in range(PARTS):
        tok = slice(part * T, (part + 1) * T)
        for a in range(4):
            ks[part, a * 8 * T : (a + 1) * 8 * T, :] = k_refs[a][:, :, tok, :].reshape(8 * T, HEAD)
            for b in range(4):
                row = (a * 8 + b * 2) * T
                vs[part, row : row + 2 * T, :] = v_refs[b][a, :, tok, :].reshape(2 * T, HEAD)
        for h in range(GROUP):
            for s in range(2):
                row = (h * 4 + s * 2) * T
                qs[part, row : row + 2 * T, :] = qg_refs[s][:, tok, h * HEAD : (h + 1) * HEAD].reshape(2 * T, HEAD)
                col = (GROUP + h) * HEAD
                gs[part, row : row + 2 * T, :] = qg_refs[s][:, tok, col : col + HEAD].reshape(2 * T, HEAD)
    for slot in range(SLOTS):
        column = jnp.broadcast_to(kpos_ref[slot : slot + 1, :], (TOK, 128)).T
        for part in range(PARTS):
            kposb[part, slot * T : (slot + 1) * T, :] = column[part * T : (part + 1) * T, :]


def masked_scores(delta, i, ip, ks, qs, kposb, qpos_ref):
    s = nt(ks[ip], qs[i]) * SCORE2
    if delta == 0 or delta == SPAN:
        kp = jnp.concatenate([kposb[ip]] * (QR // 128), axis=1)
        qp = qpos_ref[i][0:1, :]
        valid = (kp <= qp) if delta == 0 else (kp > qp - float(WINDOW))
        s = jnp.where(valid, s, NEG)
    return s


def stats_kernel(*refs):
    k_refs, v_refs, qg_refs = refs[0:4], refs[4:8], refs[8:10]
    kpos_ref, qpos_ref, out_ref, sent_ref = refs[10:14]
    ks, vs, qs, gs, kposb, ms, ls, ws = refs[14:]
    load_parts(k_refs, v_refs, qg_refs, kpos_ref, ks, vs, qs, gs, kposb)
    ms[...] = jnp.full(ms.shape, NEG, F32)
    ls[...] = jnp.zeros(ls.shape, F32)
    ws[...] = jnp.zeros(ws.shape, F32)
    for delta in range(SPAN + 1):

        def body(i, carry, delta=delta):
            ip = i - delta
            s = masked_scores(delta, i, ip, ks, qs, kposb, qpos_ref).reshape(KR // 8, 8, QR)
            dp = nt(vs[ip], gs[i]).reshape(KR // 8, 8, QR)
            old = ms[i]
            new = jnp.maximum(old, jnp.max(s, axis=0))
            e = jnp.exp2(s - new[None])
            fade = jnp.exp2(old - new)
            ls[i] = ls[i] * fade + jnp.sum(e, axis=0)
            ws[i] = ws[i] * fade + jnp.sum(e * dp, axis=0)
            ms[i] = new
            return carry

        lax.fori_loop(delta, PARTS, body, 0)
    for i in range(PARTS):
        m8 = ms[i]
        top = jnp.max(m8, axis=0, keepdims=True)
        fade = jnp.exp2(m8 - top)
        total = jnp.sum(ls[i] * fade, axis=0, keepdims=True)
        weighted = jnp.sum(ws[i] * fade, axis=0, keepdims=True)
        stats = jnp.concatenate([top, total, weighted, jnp.zeros((5, QR), F32)], axis=0)
        out_ref[i] = stats
        lane = lax.broadcasted_iota(jnp.int32, (8, QR), 1)
        low = (lane // (2 * T)) % 2 == 0
        sent_ref[i] = jnp.where(low, pltpu.roll(stats, QR - 2 * T, 1), pltpu.roll(stats, 2 * T, 1))


def grads_kernel(*refs):
    k_refs, v_refs, qg_refs = refs[0:4], refs[4:8], refs[8:10]
    kpos_ref, qpos_ref, st_a, st_b = refs[10:14]
    dk_refs, dv_refs, dq_refs = refs[14:18], refs[18:22], refs[22:24]
    ks, vs, qs, gs, kposb, kt, dks, dvs, dqt = refs[24:]
    load_parts(k_refs, v_refs, qg_refs, kpos_ref, ks, vs, qs, gs, kposb)
    for part in range(PARTS):
        kt[part] = ks[part].T
    for delta in range(SPAN + 1):

        def body(i, carry, delta=delta):
            ip = i - delta
            sa, sb = st_a[i], st_b[i]
            top = jnp.maximum(sa[0:1], sb[0:1])
            fa, fb = jnp.exp2(sa[0:1] - top), jnp.exp2(sb[0:1] - top)
            total = sa[1:2] * fa + sb[1:2] * fb
            lse2 = top + jnp.log2(total)
            row_delta = (sa[2:3] * fa + sb[2:3] * fb) / total
            q, g = qs[i], gs[i]
            p = jnp.exp2(masked_scores(delta, i, ip, ks, qs, kposb, qpos_ref) - lse2)
            ds = (p * (nt(vs[ip], g) - row_delta)).astype(BF)
            p = p.astype(BF)
            dk, dv, dq = nn(ds, q), nn(p, g), nn(kt[ip], ds)
            if delta == 0:
                dks[ip], dvs[ip], dqt[i] = dk, dv, dq
            else:
                dks[ip] += dk
                dvs[ip] += dv
                dqt[i] += dq
            return carry

        lax.fori_loop(delta, PARTS, body, 0)
    for part in range(PARTS):
        tok = slice(part * T, (part + 1) * T)
        for a in range(4):
            rows = dks[part, a * 8 * T : (a + 1) * 8 * T, :] * SCALE
            dk_refs[a][:, :, tok, :] = rows.astype(BF).reshape(4, 2, T, HEAD)
            for b in range(4):
                row = (a * 8 + b * 2) * T
                dv_refs[b][a, :, tok, :] = dvs[part, row : row + 2 * T, :].astype(BF).reshape(2, T, HEAD)
        dq = dqt[part].T * SCALE
        for h in range(GROUP):
            for s in range(2):
                row = (h * 4 + s * 2) * T
                piece = dq[row : row + 2 * T, :].reshape(2, T, HEAD)
                dq_refs[s][:, tok, h * HEAD : (h + 1) * HEAD] = piece.astype(dq_refs[s].dtype)


def common_scratch():
    return [
        pltpu.VMEM((PARTS, KR, HEAD), BF),
        pltpu.VMEM((PARTS, KR, HEAD), BF),
        pltpu.VMEM((PARTS, QR, HEAD), BF),
        pltpu.VMEM((PARTS, QR, HEAD), BF),
        pltpu.VMEM((PARTS, KR, 128), F32),
    ]


def run_stats(ks, vs, qgs, kpos, qpos):
    return pl.pallas_call(
        stats_kernel,
        out_shape=[jax.ShapeDtypeStruct((PARTS, 8, QR), F32)] * 2,
        scratch_shapes=common_scratch() + [pltpu.VMEM((PARTS, 8, QR), F32)] * 3,
        compiler_params=pltpu.CompilerParams(vmem_limit_bytes=VMEM_LIMIT),
        cost_estimate=pl.CostEstimate(flops=6_000_000_000, bytes_accessed=3_000_000, transcendentals=5_000_000),
        name="stats",
    )(*ks, *vs, *qgs, kpos, qpos)


def run_grads(ks, vs, qgs, kpos, qpos, st_a, st_b):
    kv = jax.ShapeDtypeStruct((4, 2, TOK, HEAD), BF)
    outs = [kv] * 8 + [
        jax.ShapeDtypeStruct((2, TOK, GROUP * HEAD), F32),
        jax.ShapeDtypeStruct((2, TOK, GROUP * HEAD), BF),
    ]
    out = pl.pallas_call(
        grads_kernel,
        out_shape=outs,
        scratch_shapes=common_scratch()
        + [
            pltpu.VMEM((PARTS, HEAD, KR), BF),
            pltpu.VMEM((PARTS, KR, HEAD), F32),
            pltpu.VMEM((PARTS, KR, HEAD), F32),
            pltpu.VMEM((PARTS, HEAD, QR), F32),
        ],
        compiler_params=pltpu.CompilerParams(vmem_limit_bytes=VMEM_LIMIT),
        cost_estimate=pl.CostEstimate(flops=12_000_000_000, bytes_accessed=6_000_000, transcendentals=5_000_000),
        name="grads",
    )(*ks, *vs, *qgs, kpos, qpos, st_a, st_b)
    return out[0:4], out[4:8], out[8], out[9]


def positions(run_placement, y, z, x, c):
    def device(yy, zz, xx, cc):
        return (((yy % 4) * 2 + zz % 2) * 4 + xx % 4) * 2 + cc % 2

    a, b, e = jnp.meshgrid(jnp.arange(4), jnp.arange(4), jnp.arange(2), indexing="ij")
    keys = device(y + a, z, x + b, c + e).reshape(32)
    a, e = jnp.meshgrid(jnp.arange(2), jnp.arange(2), indexing="ij")
    queries = device(y, z + a, x, c + e).reshape(4)
    index = jnp.concatenate([keys, queries]).astype(jnp.int32)
    pick = (index[:, None] == jnp.arange(64, dtype=jnp.int32)[None, :]).astype(BF)
    slots = nt(pick, run_placement.astype(BF)).astype(BF)
    lane = jnp.arange(TOK, dtype=jnp.int32)
    spread = jnp.where(lane[None, :] // 2 == jnp.arange(64, dtype=jnp.int32)[:, None], 2.0, 0.0).astype(BF)
    pos = nn(slots, spread) + ((lane // 2) * TOK + lane % 2).astype(F32)[None, :]
    kpos = pos[:32]
    qpos = pos[32:].reshape(4, PARTS, T).transpose(1, 0, 2).reshape(PARTS, 1, 1, 4 * T)
    qpos = jnp.broadcast_to(qpos, (PARTS, 8, GROUP, 4 * T)).reshape(PARTS, 8, QR)
    return kpos, qpos


def own_first(c, mine, other, axis):
    return jnp.where(c == 0, jnp.concatenate([mine, other], axis), jnp.concatenate([other, mine], axis))


def local(query_rows, key_rows, value_rows, output_grad, layer_input, key_matrix, value_matrix, run_placement):
    y, z, x, c, t = (lax.axis_index(a) for a in ("y", "z", "x", "c", "tp"))
    wide = GROUP * HEAD

    def head_of(which):
        q = lax.dynamic_slice_in_dim(query_rows, which * wide, wide, 1)
        g = lax.dynamic_slice_in_dim(output_grad, which * wide, wide, 1)
        k = lax.dynamic_slice_in_dim(key_rows, which * HEAD, HEAD, 1)
        v = lax.dynamic_slice_in_dim(value_rows, which * HEAD, HEAD, 1)
        return jnp.concatenate([q, g, k, v], axis=1)

    both = jnp.stack([head_of(c), moved(head_of(1 - c), "c", 1)])
    qg = both[:, :, : 2 * wide]
    k_own = both[:, :, 2 * wide : 2 * wide + HEAD]
    v_own = both[:, :, 2 * wide + HEAD :]
    kpos, qpos = positions(run_placement, y, z, x, c)

    k_row = jnp.stack([k_own] + [moved(k_own, "x", -o) for o in (1, 2, 3)])
    v_col = jnp.stack([v_own] + [moved(v_own, "y", -o) for o in (1, 2, 3)])
    ks = [k_row] + [moved(k_row, "y", -o) for o in (1, 2, 3)]
    vs = [v_col] + [moved(v_col, "x", -o) for o in (1, 2, 3)]
    qgs = [qg, moved(qg, "z", 1)]

    st_a, st_sent = run_stats(ks, vs, qgs, kpos, qpos)
    st_b = moved(st_sent, "z", 1)
    dks, dvs, dq_own, dq_out = run_grads(ks, vs, qgs, kpos, qpos, st_a, st_b)

    def x_columns(target):
        cuts = [lax.dynamic_slice_in_dim(layer_input, n * 4 * HEAD + (target % 4) * HEAD, HEAD, 1) for n in range(4)]
        return jnp.concatenate(cuts, axis=1)

    x_half = jnp.stack([x_columns(x)] + [moved(x_columns(x + 4 - o), "x", -o) for o in (1, 2, 3)])
    x_other = moved(x_half, "tp", 1)
    x_here = jnp.where(t == 0, jnp.concatenate([x_half, x_other], 2), jnp.concatenate([x_other, x_half], 2))
    x_all = jnp.stack([x_here, moved(x_here, "c", 1)], axis=1)

    def summed(own, arrived):
        total = own.astype(F32)
        for a in arrived:
            total = total + a.astype(F32)
        return total.astype(BF)

    dk_row = summed(dks[0], [moved(dks[o], "y", o) for o in (1, 2, 3)])
    dv_col = summed(dvs[0], [moved(dvs[o], "x", o) for o in (1, 2, 3)])
    dk = summed(dk_row[0], [moved(dk_row[o], "x", o) for o in (1, 2, 3)])
    dv = summed(dv_col[0], [moved(dv_col[o], "y", o) for o in (1, 2, 3)])
    dkv = jnp.concatenate([dk, dv], axis=2)

    dq = (dq_own + moved(dq_out, "z", 1).astype(F32)).astype(BF)
    query_grad = own_first(c, dq[0], moved(dq[1], "c", 1), 1)

    dkv_far = moved(dkv[1], "c", 1)
    k_here = own_first(c, dkv[0, :, :HEAD], dkv_far[:, :HEAD], 1)
    v_here = own_first(c, dkv[0, :, HEAD:], dkv_far[:, HEAD:], 1)
    half = key_matrix.shape[0] // 2

    def input_part(which):
        km = lax.dynamic_slice_in_dim(key_matrix, which * half, half, 0)
        vm = lax.dynamic_slice_in_dim(value_matrix, which * half, half, 0)
        return nt(k_here, km) + nt(v_here, vm)

    input_far = moved(input_part(1 - t).astype(BF), "tp", 1)
    input_grad = (input_part(t) + input_far.astype(F32)).astype(BF)

    dkv_all = jnp.stack([dkv] + [moved(dkv, "x", -o) for o in (1, 2, 3)])
    tokens = 8 * TOK
    weight = lax.dot_general(
        x_all.reshape(tokens, 8 * HEAD),
        dkv_all.reshape(tokens, 2 * HEAD),
        (((0,), (0,)), ((), ())),
        preferred_element_type=F32,
    )
    pieces = weight.astype(BF).reshape(8, HEAD, 2 * HEAD)
    rows = lax.all_to_all(pieces, ("y", "z"), 0, 0, tiled=True).astype(F32).sum(axis=0)
    half_rows = HEAD // 2
    mine = lax.dynamic_slice_in_dim(rows, c * half_rows, half_rows, 0)
    far = moved(lax.dynamic_slice_in_dim(rows, (1 - c) * half_rows, half_rows, 0), "c", 1)
    key_weight = own_first(c, mine[:, :HEAD], far[:, :HEAD], 1)
    value_weight = own_first(c, mine[:, HEAD:], far[:, HEAD:], 1)
    return (query_grad, input_grad, key_weight, value_weight)


def solution(mesh):
    torus = Mesh(mesh.devices.reshape(4, 2, 4, 2, mesh.shape["tp"]), ("y", "z", "x", "c", "tp"))
    return jax.shard_map(
        local,
        mesh=torus,
        in_specs=(P(SEQ, "tp"),) * 5 + (P(None, "tp"),) * 2 + (P(),),
        out_specs=(P(SEQ, "tp"),) * 4,
        check_vma=False,
    )
```

```python
import math

import jax
import jax.numpy as jnp
from jax import lax
from jax.experimental import pallas as pl
from jax.experimental.pallas import tpu as pltpu
from jax.sharding import Mesh
from jax.sharding import PartitionSpec as P


HEAD = 128
WINDOW = 4096
GROUP = 4
TOK = 128
SEQ = ("y", "z", "x", "c")
BF = jnp.bfloat16
F32 = jnp.float32
NEG = -1e30

PARTS = 4
T = TOK // PARTS
KSLOTS = 16
QSLOTS = 8
KR = KSLOTS * T
QR = QSLOTS * GROUP * T
SPAN = PARTS // 2
SCALE = 1.0 / math.sqrt(HEAD)
SCORE2 = SCALE * math.log2(math.e)
VMEM_LIMIT = 60 * 1024 * 1024


def moved(array, axis, by):
    n = lax.axis_size(axis)
    return lax.ppermute(array, axis, [(i, (i + by) % n) for i in range(n)])


def nt(a, b):
    return lax.dot_general(a, b, (((1,), (1,)), ((), ())), preferred_element_type=F32)


def nn(a, b):
    return lax.dot_general(a, b, (((1,), (0,)), ((), ())), preferred_element_type=F32)


def load_parts(kv_refs, qg_refs, kpos_ref, ks, vs, qs, gs, kposb):
    for part in range(PARTS):
        tok = slice(part * T, (part + 1) * T)
        for a in range(2):
            rows = slice(a * 8 * T, (a + 1) * 8 * T)
            ks[part, rows, :] = kv_refs[a][:, :, tok, :HEAD].reshape(8 * T, HEAD)
            vs[part, rows, :] = kv_refs[a][:, :, tok, HEAD:].reshape(8 * T, HEAD)
        for h in range(GROUP):
            for s in range(4):
                row = (h * QSLOTS + s * 2) * T
                qs[part, row : row + 2 * T, :] = qg_refs[s][:, tok, h * HEAD : (h + 1) * HEAD].reshape(2 * T, HEAD)
                col = (GROUP + h) * HEAD
                gs[part, row : row + 2 * T, :] = qg_refs[s][:, tok, col : col + HEAD].reshape(2 * T, HEAD)
    for slot in range(KSLOTS):
        column = jnp.broadcast_to(kpos_ref[slot : slot + 1, :], (TOK, 128)).T
        for part in range(PARTS):
            kposb[part, slot * T : (slot + 1) * T, :] = column[part * T : (part + 1) * T, :]


def masked_scores(delta, i, ip, ks, qs, kposb, qpos_ref):
    s = nt(ks[ip], qs[i]) * SCORE2
    if delta == 0 or delta == SPAN:
        kp = jnp.concatenate([kposb[ip]] * (QR // 128), axis=1)
        qp = qpos_ref[i]
        valid = (kp <= qp) if delta == 0 else (kp > qp - float(WINDOW))
        s = jnp.where(valid, s, NEG)
    return s


def stats_kernel(*refs):
    kv_refs, qg_refs = refs[0:2], refs[2:6]
    kpos_ref, qpos_ref = refs[6:8]
    out_refs = refs[8:12]
    ks, vs, qs, gs, kposb, ms, ls, ws = refs[12:]
    load_parts(kv_refs, qg_refs, kpos_ref, ks, vs, qs, gs, kposb)
    ms[...] = jnp.full(ms.shape, NEG, F32)
    ls[...] = jnp.zeros(ls.shape, F32)
    ws[...] = jnp.zeros(ws.shape, F32)
    for delta in range(SPAN + 1):

        def body(i, carry, delta=delta):
            ip = i - delta
            s = masked_scores(delta, i, ip, ks, qs, kposb, qpos_ref).reshape(KR // 8, 8, QR)
            dp = nt(vs[ip], gs[i]).reshape(KR // 8, 8, QR)
            old = ms[i]
            new = jnp.maximum(old, jnp.max(s, axis=0))
            e = jnp.exp2(s - new[None])
            fade = jnp.exp2(old - new)
            ls[i] = ls[i] * fade + jnp.sum(e, axis=0)
            ws[i] = ws[i] * fade + jnp.sum(e * dp, axis=0)
            ms[i] = new
            return carry

        lax.fori_loop(delta, PARTS, body, 0)
    rows = []
    for i in range(PARTS):
        m8 = ms[i]
        top = jnp.max(m8, axis=0, keepdims=True)
        fade = jnp.exp2(m8 - top)
        total = jnp.sum(ls[i] * fade, axis=0, keepdims=True)
        weighted = jnp.sum(ws[i] * fade, axis=0, keepdims=True)
        rows += [top, total, weighted, jnp.zeros((1, QR), F32)]
    stats = jnp.concatenate(rows, axis=0)
    per_head = QSLOTS * T
    for o in range(4):
        for h in range(GROUP):
            cols = slice(h * per_head, (h + 1) * per_head)
            piece = stats[:, cols]
            out_refs[o][:, cols] = pltpu.roll(piece, o * 2 * T, 1) if o else piece


def grads_kernel(*refs):
    kv_refs, qg_refs = refs[0:2], refs[2:6]
    kpos_ref, qpos_ref = refs[6:8]
    st_refs = refs[8:12]
    dkv_refs, dq_refs = refs[12:14], refs[14:18]
    ks, vs, qs, gs, kposb, kt, dks, dvs, dqt, lse, mean = refs[18:]
    load_parts(kv_refs, qg_refs, kpos_ref, ks, vs, qs, gs, kposb)
    for part in range(PARTS):
        kt[part] = ks[part].T
        st = [r[part * 4 : part * 4 + 3, :] for r in st_refs]
        top = jnp.maximum(jnp.maximum(st[0][0:1], st[1][0:1]), jnp.maximum(st[2][0:1], st[3][0:1]))
        fade = [jnp.exp2(a[0:1] - top) for a in st]
        total = sum(a[1:2] * f for a, f in zip(st, fade))
        lse[part] = top + jnp.log2(total)
        mean[part] = sum(a[2:3] * f for a, f in zip(st, fade)) / total
    for delta in range(SPAN + 1):

        def body(i, carry, delta=delta):
            ip = i - delta
            q, g = qs[i], gs[i]
            p = jnp.exp2(masked_scores(delta, i, ip, ks, qs, kposb, qpos_ref) - lse[i])
            ds = (p * (nt(vs[ip], g) - mean[i])).astype(BF)
            p = p.astype(BF)
            dk, dv, dq = nn(ds, q), nn(p, g), nn(kt[ip], ds)
            if delta == 0:
                dks[ip], dvs[ip], dqt[i] = dk, dv, dq
            else:
                dks[ip] += dk
                dvs[ip] += dv
                dqt[i] += dq
            return carry

        lax.fori_loop(delta, PARTS, body, 0)
    for part in range(PARTS):
        tok = slice(part * T, (part + 1) * T)
        for a in range(2):
            rows = slice(a * 8 * T, (a + 1) * 8 * T)
            dkv_refs[a][:, :, tok, :HEAD] = (dks[part, rows, :] * SCALE).astype(BF).reshape(4, 2, T, HEAD)
            dkv_refs[a][:, :, tok, HEAD:] = dvs[part, rows, :].astype(BF).reshape(4, 2, T, HEAD)
        dq = dqt[part].T * SCALE
        for h in range(GROUP):
            for s in range(4):
                row = (h * QSLOTS + s * 2) * T
                piece = dq[row : row + 2 * T, :].reshape(2, T, HEAD)
                dq_refs[s][:, tok, h * HEAD : (h + 1) * HEAD] = piece.astype(dq_refs[s].dtype)


def common_scratch():
    return [
        pltpu.VMEM((PARTS, KR, HEAD), BF),
        pltpu.VMEM((PARTS, KR, HEAD), BF),
        pltpu.VMEM((PARTS, QR, HEAD), BF),
        pltpu.VMEM((PARTS, QR, HEAD), BF),
        pltpu.VMEM((PARTS, KR, 128), F32),
    ]


def run_stats(kvs, qgs, kpos, qpos):
    return pl.pallas_call(
        stats_kernel,
        out_shape=[jax.ShapeDtypeStruct((PARTS * 4, QR), F32)] * 4,
        scratch_shapes=common_scratch() + [pltpu.VMEM((PARTS, 8, QR), F32)] * 3,
        compiler_params=pltpu.CompilerParams(vmem_limit_bytes=VMEM_LIMIT),
        cost_estimate=pl.CostEstimate(flops=6_000_000_000, bytes_accessed=3_000_000, transcendentals=5_000_000),
        name="stats",
    )(*kvs, *qgs, kpos, qpos)


def run_grads(kvs, qgs, kpos, qpos, sts):
    dkv = jax.ShapeDtypeStruct((4, 2, TOK, 2 * HEAD), BF)
    dq = [jax.ShapeDtypeStruct((2, TOK, GROUP * HEAD), F32 if s == 0 else BF) for s in range(4)]
    out = pl.pallas_call(
        grads_kernel,
        out_shape=[dkv, dkv] + dq,
        scratch_shapes=common_scratch()
        + [
            pltpu.VMEM((PARTS, HEAD, KR), BF),
            pltpu.VMEM((PARTS, KR, HEAD), F32),
            pltpu.VMEM((PARTS, KR, HEAD), F32),
            pltpu.VMEM((PARTS, HEAD, QR), F32),
            pltpu.VMEM((PARTS, 1, QR), F32),
            pltpu.VMEM((PARTS, 1, QR), F32),
        ],
        compiler_params=pltpu.CompilerParams(vmem_limit_bytes=VMEM_LIMIT),
        cost_estimate=pl.CostEstimate(flops=12_000_000_000, bytes_accessed=6_000_000, transcendentals=5_000_000),
        name="grads",
    )(*kvs, *qgs, kpos, qpos, *sts)
    return out[0:2], out[2:6]


def pack_kernel(at_ref, q_ref, g_ref, k_ref, v_ref, kv_own, qg_own, kv_send, qg_send):
    wide = GROUP * HEAD
    mine = at_ref[0]
    for which, kv, qg in ((mine, kv_own.at[0], qg_own.at[0]), (1 - mine, kv_send, qg_send)):
        cols = pl.ds(pl.multiple_of(which * wide, 128), wide)
        small = pl.ds(pl.multiple_of(which * HEAD, 128), HEAD)
        kv[:, :HEAD] = k_ref[:, small]
        kv[:, HEAD:] = v_ref[:, small]
        qg[:, :wide] = q_ref[:, cols]
        qg[:, wide:] = g_ref[:, cols]
    kv_own[1] = kv_send[...]
    qg_own[1] = qg_send[...]


def run_pack(at, q, g, k, v):
    kv, qg = (TOK, 2 * HEAD), (TOK, 2 * GROUP * HEAD)
    vmem = pl.BlockSpec(memory_space=pltpu.VMEM)
    return pl.pallas_call(
        pack_kernel,
        out_shape=[jax.ShapeDtypeStruct(a, BF) for a in ((2, *kv), (2, *qg), kv, qg)],
        in_specs=[pl.BlockSpec(memory_space=pltpu.SMEM)] + [vmem] * 4,
        name="pack",
    )(at, q, g, k, v)


def columns_kernel(at_ref, in_ref, *out_refs):
    for o in range(4):
        target = (at_ref[1] + o) % 4
        for n in range(4):
            cols = pl.ds(pl.multiple_of(n * 4 * HEAD + target * HEAD, 128), HEAD)
            out_refs[o][:, n * HEAD : (n + 1) * HEAD] = in_ref[:, cols]


def run_columns(at, layer_input):
    return pl.pallas_call(
        columns_kernel,
        out_shape=[jax.ShapeDtypeStruct((TOK, 4 * HEAD), BF)] * 4,
        in_specs=[pl.BlockSpec(memory_space=pltpu.SMEM), pl.BlockSpec(memory_space=pltpu.VMEM)],
        name="columns",
    )(at, layer_input)


def finish_kernel(in_ref, k_ref, v_ref):
    for h in range(2):
        total = in_ref[h].astype(F32)
        for n in range(1, 8):
            total = total + in_ref[2 * n + h].astype(F32)
        k_ref[:, h * HEAD : (h + 1) * HEAD] = total[:, :HEAD]
        v_ref[:, h * HEAD : (h + 1) * HEAD] = total[:, HEAD:]


def run_finish(got):
    out = jax.ShapeDtypeStruct((HEAD // 2, 2 * HEAD), F32)
    return pl.pallas_call(finish_kernel, out_shape=[out, out], name="finish")(got)


def positions(run_placement, y, z, x, c):
    def device(yy, zz, xx, cc):
        return (((yy % 4) * 2 + zz % 2) * 4 + xx % 4) * 2 + cc % 2

    a, b, e = jnp.meshgrid(jnp.arange(2), jnp.arange(4), jnp.arange(2), indexing="ij")
    keys = device(y, z + a, x + b, c + e).reshape(KSLOTS)
    a, e = jnp.meshgrid(jnp.arange(4), jnp.arange(2), indexing="ij")
    queries = device(y + a, z, x, c + e).reshape(QSLOTS)
    index = jnp.concatenate([keys, queries]).astype(jnp.int32)
    pick = (index[:, None] == jnp.arange(64, dtype=jnp.int32)[None, :]).astype(BF)
    slots = nt(pick, run_placement.astype(BF)).astype(BF)
    lane = jnp.arange(TOK, dtype=jnp.int32)
    spread = jnp.where(lane[None, :] // 2 == jnp.arange(64, dtype=jnp.int32)[:, None], 2.0, 0.0).astype(BF)
    pos = nn(slots, spread) + ((lane // 2) * TOK + lane % 2).astype(F32)[None, :]
    kpos = pos[:KSLOTS]
    qpos = pos[KSLOTS:].reshape(QSLOTS, PARTS, T).transpose(1, 0, 2).reshape(PARTS, 1, 1, QSLOTS * T)
    qpos = jnp.broadcast_to(qpos, (PARTS, 1, GROUP, QSLOTS * T)).reshape(PARTS, 1, QR)
    return kpos, qpos


def own_first(c, mine, other, axis):
    return jnp.where(c == 0, jnp.concatenate([mine, other], axis), jnp.concatenate([other, mine], axis))


def after(array, *gates):
    return lax.optimization_barrier((array, *gates))[0]


def step(query_rows, key_rows, value_rows, output_grad, layer_input, key_matrix, value_matrix, run_placement):
    y, z, x, c, t = (lax.axis_index(a) for a in ("y", "z", "x", "c", "tp"))
    at = jnp.stack([c, x]).astype(jnp.int32)
    kv_pair, qg_pair, kv_send, qg_send = run_pack(at, query_rows, output_grad, key_rows, value_rows)
    kv_own = kv_pair.at[1].set(moved(kv_send, "c", 1))
    qg_own = qg_pair.at[1].set(moved(qg_send, "c", 1))
    kpos, qpos = positions(run_placement, y, z, x, c)
    kv_row = jnp.stack([kv_own] + [moved(kv_own, "x", -o) for o in (1, 2, 3)])
    qgs = [qg_own] + [moved(qg_own, "y", -o) for o in (1, 2, 3)]
    kvs = [kv_row, moved(kv_row, "z", 1)]

    half = key_matrix.shape[0] // 2
    cuts = [lax.dynamic_slice_in_dim(after(m, kv_row), (1 - t) * half, half, 0) for m in (key_matrix, value_matrix)]
    m_far = moved(jnp.where(c == 0, *cuts), "tp", 1)
    x_pieces = run_columns(at, after(layer_input, kv_row))
    kpos = after(kpos, *x_pieces)

    sts = run_stats(kvs, qgs, kpos, qpos)
    sts = [sts[0]] + [moved(sts[o], "y", -o) for o in (1, 2, 3)]
    x_half = jnp.stack([x_pieces[0]] + [moved(x_pieces[4 - o], "x", -o) for o in (1, 2, 3)])
    dkvs, dqs = run_grads(kvs, qgs, kpos, qpos, sts)

    def total_of(own, arrived):
        total = own.astype(F32)
        for a in arrived:
            total = total + a.astype(F32)
        return total.astype(BF)

    dkv_row = total_of(dkvs[0], [moved(dkvs[1], "z", 1)])
    dq = total_of(dqs[0], [moved(dqs[o], "y", o) for o in (1, 2, 3)])
    x_other = moved(x_half, "tp", 1)
    x_here = jnp.where(t == 0, jnp.concatenate([x_half, x_other], 2), jnp.concatenate([x_other, x_half], 2))
    x_all = jnp.stack([x_here, moved(x_here, "c", 1)], axis=1)
    m_core = moved(m_far, "c", 1)
    k_far = jnp.where(c == 0, m_far, m_core)
    v_far = jnp.where(c == 0, m_core, m_far)

    dkv = total_of(dkv_row[0], [moved(dkv_row[o], "x", o) for o in (1, 2, 3)])
    dkv_all = jnp.stack([dkv] + [moved(dkv, "x", -o) for o in (1, 2, 3)])
    dkv_far = moved(dkv[1], "c", 1)
    k_here = own_first(c, dkv[0, :, :HEAD], dkv_far[:, :HEAD], 1)
    v_here = own_first(c, dkv[0, :, HEAD:], dkv_far[:, HEAD:], 1)
    kv_here = jnp.concatenate([k_here, v_here], 1)
    kv_there = moved(kv_here, "tp", 1)

    query_grad = own_first(c, dq[0], moved(dq[1], "c", 1), 1)

    tokens = 8 * TOK
    weight = lax.dot_general(
        x_all.reshape(tokens, 8 * HEAD),
        dkv_all.reshape(tokens, 2 * HEAD),
        (((0,), (0,)), ((), ())),
        preferred_element_type=F32,
    )
    pieces = weight.astype(BF).reshape(16, HEAD // 2, 2 * HEAD)
    got = lax.all_to_all(pieces, ("y", "z", "c"), 0, 0, tiled=True)
    key_weight, value_weight = run_finish(got)

    km = lax.dynamic_slice_in_dim(key_matrix, t * half, half, 0)
    vm = lax.dynamic_slice_in_dim(value_matrix, t * half, half, 0)
    wide = 2 * HEAD
    total = nt(kv_here[:, :wide], km) + nt(kv_here[:, wide:], vm)
    input_grad = (total + nt(kv_there[:, :wide], k_far) + nt(kv_there[:, wide:], v_far)).astype(BF)
    return (query_grad, input_grad, key_weight, value_weight)


def solution(mesh):
    torus = Mesh(mesh.devices.reshape(4, 2, 4, 2, mesh.shape["tp"]), ("y", "z", "x", "c", "tp"))
    return jax.shard_map(
        step,
        mesh=torus,
        in_specs=(P(SEQ, "tp"),) * 5 + (P(None, "tp"),) * 2 + (P(),),
        out_specs=(P(SEQ, "tp"),) * 4,
        check_vma=False,
    )
```

```python
import math

import jax
import jax.numpy as jnp
from jax import lax
from jax.experimental import pallas as pl
from jax.experimental.pallas import tpu as pltpu
from jax.sharding import Mesh
from jax.sharding import PartitionSpec as P


HEAD = 128
WINDOW = 4096
GROUP = 4
TOK = 128
SEQ = ("y", "z", "x", "c")
BF = jnp.bfloat16
F32 = jnp.float32
NEG = -1e30

PARTS = 4
T = TOK // PARTS
KSLOTS = 16
QSLOTS = 8
KR = KSLOTS * T
QR = QSLOTS * GROUP * T
SPAN = PARTS // 2
SCALE = 1.0 / math.sqrt(HEAD)
SCORE2 = SCALE * math.log2(math.e)
VMEM_LIMIT = 60 * 1024 * 1024


def moved(array, axis, by):
    n = lax.axis_size(axis)
    return lax.ppermute(array, axis, [(i, (i + by) % n) for i in range(n)])


def nt(a, b):
    return lax.dot_general(a, b, (((1,), (1,)), ((), ())), preferred_element_type=F32)


def nn(a, b):
    return lax.dot_general(a, b, (((1,), (0,)), ((), ())), preferred_element_type=F32)


def load_parts(kv_refs, qg_refs, kpos_ref, ks, vs, qs, gs, kposb):
    for part in range(PARTS):
        tok = slice(part * T, (part + 1) * T)
        for b in range(4):
            rows = slice(b * 4 * T, (b + 1) * 4 * T)
            ks[part, rows, :] = kv_refs[b][:, :, tok, :HEAD].reshape(4 * T, HEAD)
            vs[part, rows, :] = kv_refs[b][:, :, tok, HEAD:].reshape(4 * T, HEAD)
        for h in range(GROUP):
            for s in range(4):
                row = (h * QSLOTS + s * 2) * T
                qs[part, row : row + 2 * T, :] = qg_refs[s][:, tok, h * HEAD : (h + 1) * HEAD].reshape(2 * T, HEAD)
                col = (GROUP + h) * HEAD
                gs[part, row : row + 2 * T, :] = qg_refs[s][:, tok, col : col + HEAD].reshape(2 * T, HEAD)
    for slot in range(KSLOTS):
        column = jnp.broadcast_to(kpos_ref[slot : slot + 1, :], (TOK, 128)).T
        for part in range(PARTS):
            kposb[part, slot * T : (slot + 1) * T, :] = column[part * T : (part + 1) * T, :]


def masked_scores(delta, i, ip, ks, qs, kposb, qpos_ref):
    s = nt(ks[ip], qs[i]) * SCORE2
    if delta == 0 or delta == SPAN:
        kp = jnp.concatenate([kposb[ip]] * (QR // 128), axis=1)
        qp = qpos_ref[i]
        valid = (kp <= qp) if delta == 0 else (kp > qp - float(WINDOW))
        s = jnp.where(valid, s, NEG)
    return s


def stats_kernel(*refs):
    kv_refs, qg_refs = refs[0:4], refs[4:8]
    kpos_ref, qpos_ref = refs[8:10]
    out_refs = refs[10:14]
    ks, vs, qs, gs, kposb, ms, ls, ws = refs[14:]
    load_parts(kv_refs, qg_refs, kpos_ref, ks, vs, qs, gs, kposb)
    ms[...] = jnp.full(ms.shape, NEG, F32)
    ls[...] = jnp.zeros(ls.shape, F32)
    ws[...] = jnp.zeros(ws.shape, F32)
    for delta in range(SPAN + 1):

        def body(i, carry, delta=delta):
            ip = i - delta
            s = masked_scores(delta, i, ip, ks, qs, kposb, qpos_ref).reshape(KR // 8, 8, QR)
            dp = nt(vs[ip], gs[i]).reshape(KR // 8, 8, QR)
            old = ms[i]
            new = jnp.maximum(old, jnp.max(s, axis=0))
            e = jnp.exp2(s - new[None])
            fade = jnp.exp2(old - new)
            ls[i] = ls[i] * fade + jnp.sum(e, axis=0)
            ws[i] = ws[i] * fade + jnp.sum(e * dp, axis=0)
            ms[i] = new
            return carry

        lax.fori_loop(delta, PARTS, body, 0)
    rows = []
    for i in range(PARTS):
        m8 = ms[i]
        top = jnp.max(m8, axis=0, keepdims=True)
        fade = jnp.exp2(m8 - top)
        total = jnp.sum(ls[i] * fade, axis=0, keepdims=True)
        weighted = jnp.sum(ws[i] * fade, axis=0, keepdims=True)
        rows += [top, total, weighted, jnp.zeros((1, QR), F32)]
    stats = jnp.concatenate(rows, axis=0)
    per_head = QSLOTS * T
    for o in range(4):
        for h in range(GROUP):
            cols = slice(h * per_head, (h + 1) * per_head)
            piece = stats[:, cols]
            out_refs[o][:, cols] = pltpu.roll(piece, o * 2 * T, 1) if o else piece


def grads_kernel(*refs):
    kv_refs, qg_refs = refs[0:4], refs[4:8]
    kpos_ref, qpos_ref = refs[8:10]
    st_refs = refs[10:14]
    dkv_refs, dq_refs = refs[14:16], refs[16:20]
    ks, vs, qs, gs, kposb, kt, dks, dvs, dqt, lse, mean = refs[20:]
    load_parts(kv_refs, qg_refs, kpos_ref, ks, vs, qs, gs, kposb)
    for part in range(PARTS):
        kt[part] = ks[part].T
        st = [r[part * 4 : part * 4 + 3, :] for r in st_refs]
        top = jnp.maximum(jnp.maximum(st[0][0:1], st[1][0:1]), jnp.maximum(st[2][0:1], st[3][0:1]))
        fade = [jnp.exp2(a[0:1] - top) for a in st]
        total = sum(a[1:2] * f for a, f in zip(st, fade))
        lse[part] = top + jnp.log2(total)
        mean[part] = sum(a[2:3] * f for a, f in zip(st, fade)) / total
    for delta in range(SPAN + 1):

        def body(i, carry, delta=delta):
            ip = i - delta
            q, g = qs[i], gs[i]
            p = jnp.exp2(masked_scores(delta, i, ip, ks, qs, kposb, qpos_ref) - lse[i])
            ds = (p * (nt(vs[ip], g) - mean[i])).astype(BF)
            p = p.astype(BF)
            dk, dv, dq = nn(ds, q), nn(p, g), nn(kt[ip], ds)
            if delta == 0:
                dks[ip], dvs[ip], dqt[i] = dk, dv, dq
            else:
                dks[ip] += dk
                dvs[ip] += dv
                dqt[i] += dq
            return carry

        lax.fori_loop(delta, PARTS, body, 0)
    for part in range(PARTS):
        tok = slice(part * T, (part + 1) * T)
        for b in range(4):
            for a in range(2):
                rows = slice((b * 4 + a * 2) * T, (b * 4 + a * 2 + 2) * T)
                dkv_refs[a][b, :, tok, :HEAD] = (dks[part, rows, :] * SCALE).astype(BF).reshape(2, T, HEAD)
                dkv_refs[a][b, :, tok, HEAD:] = dvs[part, rows, :].astype(BF).reshape(2, T, HEAD)
        dq = dqt[part].T * SCALE
        for h in range(GROUP):
            for s in range(4):
                row = (h * QSLOTS + s * 2) * T
                piece = dq[row : row + 2 * T, :].reshape(2, T, HEAD)
                dq_refs[s][:, tok, h * HEAD : (h + 1) * HEAD] = piece.astype(dq_refs[s].dtype)


def common_scratch():
    return [
        pltpu.VMEM((PARTS, KR, HEAD), BF),
        pltpu.VMEM((PARTS, KR, HEAD), BF),
        pltpu.VMEM((PARTS, QR, HEAD), BF),
        pltpu.VMEM((PARTS, QR, HEAD), BF),
        pltpu.VMEM((PARTS, KR, 128), F32),
    ]


def run_stats(kvs, qgs, kpos, qpos):
    return pl.pallas_call(
        stats_kernel,
        out_shape=[jax.ShapeDtypeStruct((PARTS * 4, QR), F32)] * 4,
        scratch_shapes=common_scratch() + [pltpu.VMEM((PARTS, 8, QR), F32)] * 3,
        compiler_params=pltpu.CompilerParams(vmem_limit_bytes=VMEM_LIMIT),
        cost_estimate=pl.CostEstimate(flops=6_000_000_000, bytes_accessed=3_000_000, transcendentals=5_000_000),
        name="stats",
    )(*kvs, *qgs, kpos, qpos)


def run_grads(kvs, qgs, kpos, qpos, sts):
    dkv = jax.ShapeDtypeStruct((4, 2, TOK, 2 * HEAD), BF)
    dq = [jax.ShapeDtypeStruct((2, TOK, GROUP * HEAD), F32 if s == 0 else BF) for s in range(4)]
    out = pl.pallas_call(
        grads_kernel,
        out_shape=[dkv, dkv] + dq,
        scratch_shapes=common_scratch()
        + [
            pltpu.VMEM((PARTS, HEAD, KR), BF),
            pltpu.VMEM((PARTS, KR, HEAD), F32),
            pltpu.VMEM((PARTS, KR, HEAD), F32),
            pltpu.VMEM((PARTS, HEAD, QR), F32),
            pltpu.VMEM((PARTS, 1, QR), F32),
            pltpu.VMEM((PARTS, 1, QR), F32),
        ],
        compiler_params=pltpu.CompilerParams(vmem_limit_bytes=VMEM_LIMIT),
        cost_estimate=pl.CostEstimate(flops=12_000_000_000, bytes_accessed=6_000_000, transcendentals=5_000_000),
        name="grads",
    )(*kvs, *qgs, kpos, qpos, *sts)
    return out[0:2], out[2:6]


def pack_kernel(at_ref, q_ref, g_ref, k_ref, v_ref, kv_own, qg_own, kv_send, qg_send):
    wide = GROUP * HEAD
    mine = at_ref[0]
    for which, kv, qg in ((mine, kv_own.at[0], qg_own.at[0]), (1 - mine, kv_send, qg_send)):
        cols = pl.ds(pl.multiple_of(which * wide, 128), wide)
        small = pl.ds(pl.multiple_of(which * HEAD, 128), HEAD)
        kv[:, :HEAD] = k_ref[:, small]
        kv[:, HEAD:] = v_ref[:, small]
        qg[:, :wide] = q_ref[:, cols]
        qg[:, wide:] = g_ref[:, cols]
    kv_own[1] = kv_send[...]
    qg_own[1] = qg_send[...]


def run_pack(at, q, g, k, v):
    kv, qg = (TOK, 2 * HEAD), (TOK, 2 * GROUP * HEAD)
    vmem = pl.BlockSpec(memory_space=pltpu.VMEM)
    return pl.pallas_call(
        pack_kernel,
        out_shape=[jax.ShapeDtypeStruct(a, BF) for a in ((2, *kv), (2, *qg), kv, qg)],
        in_specs=[pl.BlockSpec(memory_space=pltpu.SMEM)] + [vmem] * 4,
        name="pack",
    )(at, q, g, k, v)


def columns_kernel(at_ref, mine_ref, far_ref, *out_refs):
    for ref, half in ((mine_ref, at_ref[2]), (far_ref, 1 - at_ref[2])):
        for o in range(4):
            target = (at_ref[1] + o) % 4
            for n in range(4):
                src = pl.ds(pl.multiple_of(n * 4 * HEAD + target * HEAD, 128), HEAD)
                dst = pl.ds(pl.multiple_of(half * 4 * HEAD + n * HEAD, 128), HEAD)
                out_refs[o][:, dst] = ref[:, src]


def run_columns(at, mine, far):
    vmem = pl.BlockSpec(memory_space=pltpu.VMEM)
    return pl.pallas_call(
        columns_kernel,
        out_shape=[jax.ShapeDtypeStruct((TOK, 8 * HEAD), BF)] * 4,
        in_specs=[pl.BlockSpec(memory_space=pltpu.SMEM), vmem, vmem],
        name="columns",
    )(at, mine, far)


def finish_kernel(in_ref, k_ref, v_ref):
    for h in range(2):
        total = in_ref[h].astype(F32)
        for n in range(1, 8):
            total = total + in_ref[2 * n + h].astype(F32)
        k_ref[:, h * HEAD : (h + 1) * HEAD] = total[:, :HEAD]
        v_ref[:, h * HEAD : (h + 1) * HEAD] = total[:, HEAD:]


def run_finish(got):
    out = jax.ShapeDtypeStruct((HEAD // 2, 2 * HEAD), F32)
    return pl.pallas_call(finish_kernel, out_shape=[out, out], name="finish")(got)


def positions(run_placement, y, z, x, c):
    def device(yy, zz, xx, cc):
        return (((yy % 4) * 2 + zz % 2) * 4 + xx % 4) * 2 + cc % 2

    b, a, e = jnp.meshgrid(jnp.arange(4), jnp.arange(2), jnp.arange(2), indexing="ij")
    keys = device(y, z + a, x + b, c + e).reshape(KSLOTS)
    a, e = jnp.meshgrid(jnp.arange(4), jnp.arange(2), indexing="ij")
    queries = device(y + a, z, x, c + e).reshape(QSLOTS)
    index = jnp.concatenate([keys, queries]).astype(jnp.int32)
    pick = (index[:, None] == jnp.arange(64, dtype=jnp.int32)[None, :]).astype(BF)
    slots = nt(pick, run_placement.astype(BF)).astype(BF)
    lane = jnp.arange(TOK, dtype=jnp.int32)
    spread = jnp.where(lane[None, :] // 2 == jnp.arange(64, dtype=jnp.int32)[:, None], 2.0, 0.0).astype(BF)
    pos = nn(slots, spread) + ((lane // 2) * TOK + lane % 2).astype(F32)[None, :]
    kpos = pos[:KSLOTS]
    qpos = pos[KSLOTS:].reshape(QSLOTS, PARTS, T).transpose(1, 0, 2).reshape(PARTS, 1, 1, QSLOTS * T)
    qpos = jnp.broadcast_to(qpos, (PARTS, 1, GROUP, QSLOTS * T)).reshape(PARTS, 1, QR)
    return kpos, qpos


def own_first(c, mine, other, axis):
    return jnp.where(c == 0, jnp.concatenate([mine, other], axis), jnp.concatenate([other, mine], axis))


def after(array, *gates):
    return lax.optimization_barrier((array, *gates))[0]


def step(query_rows, key_rows, value_rows, output_grad, layer_input, key_matrix, value_matrix, run_placement):
    y, z, x, c, t = (lax.axis_index(a) for a in ("y", "z", "x", "c", "tp"))
    at = jnp.stack([c, x, t]).astype(jnp.int32)
    x_far = moved(layer_input, "tp", 1)
    kv_pair, qg_pair, kv_send, qg_send = run_pack(at, query_rows, output_grad, key_rows, value_rows)
    qg_own = qg_pair.at[1].set(moved(qg_send, "c", 1))
    kv_own = kv_pair.at[1].set(moved(kv_send, "c", 1))
    qgs = [qg_own] + [moved(qg_own, "y", -o) for o in (1, 2, 3)]
    kv_both = jnp.stack([kv_own, moved(kv_own, "z", 1)])
    kvs = [kv_both] + [moved(kv_both, "x", -o) for o in (1, 2, 3)]
    kpos, qpos = positions(run_placement, y, z, x, c)

    half = key_matrix.shape[0] // 2
    cuts = [lax.dynamic_slice_in_dim(after(m, kv_both), (1 - t) * half, half, 0) for m in (key_matrix, value_matrix)]
    x_pieces = run_columns(at, after(layer_input, kv_both), x_far)
    x_here = jnp.stack([x_pieces[0]] + [moved(x_pieces[4 - o], "x", -o) for o in (1, 2, 3)])
    m_far = moved(jnp.where(c == 0, *cuts), "tp", 1)
    kpos = after(kpos, *x_pieces)

    sts = run_stats(kvs, qgs, kpos, qpos)
    sts = [sts[0]] + [moved(sts[o], "y", -o) for o in (1, 2, 3)]
    dkvs, dqs = run_grads(kvs, qgs, kpos, qpos, sts)

    def total_of(own, arrived):
        total = own.astype(F32)
        for a in arrived:
            total = total + a.astype(F32)
        return total.astype(BF)

    dkv_row = total_of(dkvs[0], [moved(dkvs[1], "z", 1)])
    dq = total_of(dqs[0], [moved(dqs[o], "y", o) for o in (1, 2, 3)])
    x_all = jnp.stack([x_here, moved(x_here, "c", 1)], axis=1)
    m_core = moved(m_far, "c", 1)
    k_far = jnp.where(c == 0, m_far, m_core)
    v_far = jnp.where(c == 0, m_core, m_far)

    dkv = total_of(dkv_row[0], [moved(dkv_row[o], "x", o) for o in (1, 2, 3)])
    dkv_all = jnp.stack([dkv] + [moved(dkv, "x", -o) for o in (1, 2, 3)])
    dkv_far = moved(dkv[1], "c", 1)
    k_here = own_first(c, dkv[0, :, :HEAD], dkv_far[:, :HEAD], 1)
    v_here = own_first(c, dkv[0, :, HEAD:], dkv_far[:, HEAD:], 1)
    kv_here = jnp.concatenate([k_here, v_here], 1)
    kv_there = moved(kv_here, "tp", 1)

    query_grad = own_first(c, dq[0], moved(dq[1], "c", 1), 1)

    tokens = 8 * TOK
    weight = lax.dot_general(
        x_all.reshape(tokens, 8 * HEAD),
        dkv_all.reshape(tokens, 2 * HEAD),
        (((0,), (0,)), ((), ())),
        preferred_element_type=F32,
    )
    pieces = weight.astype(BF).reshape(16, HEAD // 2, 2 * HEAD)
    got = lax.all_to_all(pieces, ("y", "z", "c"), 0, 0, tiled=True)
    key_weight, value_weight = run_finish(got)

    km = lax.dynamic_slice_in_dim(key_matrix, t * half, half, 0)
    vm = lax.dynamic_slice_in_dim(value_matrix, t * half, half, 0)
    wide = 2 * HEAD
    total = nt(kv_here[:, :wide], km) + nt(kv_here[:, wide:], vm)
    input_grad = (total + nt(kv_there[:, :wide], k_far) + nt(kv_there[:, wide:], v_far)).astype(BF)
    return (query_grad, input_grad, key_weight, value_weight)


def solution(mesh):
    torus = Mesh(mesh.devices.reshape(4, 2, 4, 2, mesh.shape["tp"]), ("y", "z", "x", "c", "tp"))
    return jax.shard_map(
        step,
        mesh=torus,
        in_specs=(P(SEQ, "tp"),) * 5 + (P(None, "tp"),) * 2 + (P(),),
        out_specs=(P(SEQ, "tp"),) * 4,
        check_vma=False,
    )
```

```python
import math

import jax
import jax.numpy as jnp
from jax import lax
from jax.experimental import pallas as pl
from jax.experimental.pallas import tpu as pltpu
from jax.sharding import Mesh
from jax.sharding import PartitionSpec as P


HEAD = 128
WINDOW = 4096
GROUP = 4
TOK = 128
SEQ = ("y", "z", "x", "c")
BF = jnp.bfloat16
F32 = jnp.float32
NEG = -1e30

PARTS = 4
T = TOK // PARTS
KSLOTS = 16
QSLOTS = 8
KR = KSLOTS * T
QR = QSLOTS * GROUP * T
SPAN = PARTS // 2
SCALE = 1.0 / math.sqrt(HEAD)
SCORE2 = SCALE * math.log2(math.e)
VMEM_LIMIT = 60 * 1024 * 1024


def moved(array, axis, by):
    n = lax.axis_size(axis)
    return lax.ppermute(array, axis, [(i, (i + by) % n) for i in range(n)])


def nt(a, b):
    return lax.dot_general(a, b, (((1,), (1,)), ((), ())), preferred_element_type=F32)


def nn(a, b):
    return lax.dot_general(a, b, (((1,), (0,)), ((), ())), preferred_element_type=F32)


def load_parts(kv_refs, qg_refs, kpos_ref, ks, vs, qs, gs, kposb):
    for part in range(PARTS):
        tok = slice(part * T, (part + 1) * T)
        for b in range(4):
            rows = slice(b * 4 * T, (b + 1) * 4 * T)
            ks[part, rows, :] = kv_refs[b][:, :, tok, :HEAD].reshape(4 * T, HEAD)
            vs[part, rows, :] = kv_refs[b][:, :, tok, HEAD:].reshape(4 * T, HEAD)
        for h in range(GROUP):
            for s in range(4):
                row = (h * QSLOTS + s * 2) * T
                qs[part, row : row + 2 * T, :] = qg_refs[s][:, tok, h * HEAD : (h + 1) * HEAD].reshape(2 * T, HEAD)
                col = (GROUP + h) * HEAD
                gs[part, row : row + 2 * T, :] = qg_refs[s][:, tok, col : col + HEAD].reshape(2 * T, HEAD)
    for slot in range(KSLOTS):
        column = jnp.broadcast_to(kpos_ref[slot : slot + 1, :], (TOK, 128)).T
        for part in range(PARTS):
            kposb[part, slot * T : (slot + 1) * T, :] = column[part * T : (part + 1) * T, :]


def masked_scores(delta, i, ip, ks, qs, kposb, qpos_ref):
    s = nt(ks[ip], qs[i]) * SCORE2
    if delta == 0 or delta == SPAN:
        kp = jnp.concatenate([kposb[ip]] * (QR // 128), axis=1)
        qp = qpos_ref[i]
        valid = (kp <= qp) if delta == 0 else (kp > qp - float(WINDOW))
        s = jnp.where(valid, s, NEG)
    return s


def stats_kernel(*refs):
    kv_refs, qg_refs = refs[0:4], refs[4:8]
    kpos_ref, qpos_ref = refs[8:10]
    out_refs = refs[10:14]
    ks, vs, qs, gs, kposb, ms, ls, ws = refs[14:]
    load_parts(kv_refs, qg_refs, kpos_ref, ks, vs, qs, gs, kposb)
    ms[...] = jnp.full(ms.shape, NEG, F32)
    ls[...] = jnp.zeros(ls.shape, F32)
    ws[...] = jnp.zeros(ws.shape, F32)
    for delta in range(SPAN + 1):

        def body(i, carry, delta=delta):
            ip = i - delta
            s = masked_scores(delta, i, ip, ks, qs, kposb, qpos_ref).reshape(KR // 8, 8, QR)
            dp = nt(vs[ip], gs[i]).reshape(KR // 8, 8, QR)
            old = ms[i]
            new = jnp.maximum(old, jnp.max(s, axis=0))
            e = jnp.exp2(s - new[None])
            fade = jnp.exp2(old - new)
            ls[i] = ls[i] * fade + jnp.sum(e, axis=0)
            ws[i] = ws[i] * fade + jnp.sum(e * dp, axis=0)
            ms[i] = new
            return carry

        lax.fori_loop(delta, PARTS, body, 0)
    rows = []
    for i in range(PARTS):
        m8 = ms[i]
        top = jnp.max(m8, axis=0, keepdims=True)
        fade = jnp.exp2(m8 - top)
        total = jnp.sum(ls[i] * fade, axis=0, keepdims=True)
        weighted = jnp.sum(ws[i] * fade, axis=0, keepdims=True)
        rows += [top, total, weighted, jnp.zeros((1, QR), F32)]
    stats = jnp.concatenate(rows, axis=0)
    per_head = QSLOTS * T
    for o in range(4):
        for h in range(GROUP):
            cols = slice(h * per_head, (h + 1) * per_head)
            piece = stats[:, cols]
            out_refs[o][:, cols] = pltpu.roll(piece, o * 2 * T, 1) if o else piece


def grads_kernel(*refs):
    kv_refs, qg_refs = refs[0:4], refs[4:8]
    kpos_ref, qpos_ref = refs[8:10]
    st_refs = refs[10:14]
    dkv_near, dkv_first, dkv_last, dq_refs = refs[14], refs[15], refs[16], refs[17:21]
    ks, vs, qs, gs, kposb, kt, dks, dvs, dqt, lse, mean = refs[21:]
    far = (dkv_last.at[1], dkv_first.at[0], dkv_first.at[1], dkv_last.at[0])
    load_parts(kv_refs, qg_refs, kpos_ref, ks, vs, qs, gs, kposb)
    for part in range(PARTS):
        kt[part] = ks[part].T
        st = [r[part * 4 : part * 4 + 3, :] for r in st_refs]
        top = jnp.maximum(jnp.maximum(st[0][0:1], st[1][0:1]), jnp.maximum(st[2][0:1], st[3][0:1]))
        fade = [jnp.exp2(a[0:1] - top) for a in st]
        total = sum(a[1:2] * f for a, f in zip(st, fade))
        lse[part] = top + jnp.log2(total)
        mean[part] = sum(a[2:3] * f for a, f in zip(st, fade)) / total
    for delta in range(SPAN + 1):

        def body(i, carry, delta=delta):
            ip = i - delta
            q, g = qs[i], gs[i]
            p = jnp.exp2(masked_scores(delta, i, ip, ks, qs, kposb, qpos_ref) - lse[i])
            ds = (p * (nt(vs[ip], g) - mean[i])).astype(BF)
            p = p.astype(BF)
            dk, dv, dq = nn(ds, q), nn(p, g), nn(kt[ip], ds)
            if delta == 0:
                dks[ip], dvs[ip], dqt[i] = dk, dv, dq
            else:
                dks[ip] += dk
                dvs[ip] += dv
                dqt[i] += dq
            return carry

        lax.fori_loop(delta, PARTS, body, 0)
    for part in range(PARTS):
        tok = slice(part * T, (part + 1) * T)
        for b in range(4):
            for a in range(2):
                rows = slice((b * 4 + a * 2) * T, (b * 4 + a * 2 + 2) * T)
                ref = far[b] if a else dkv_near.at[b]
                ref[:, tok, :HEAD] = (dks[part, rows, :] * SCALE).astype(BF).reshape(2, T, HEAD)
                ref[:, tok, HEAD:] = dvs[part, rows, :].astype(BF).reshape(2, T, HEAD)
        dq = dqt[part].T * SCALE
        for h in range(GROUP):
            for s in range(4):
                row = (h * QSLOTS + s * 2) * T
                piece = dq[row : row + 2 * T, :].reshape(2, T, HEAD)
                dq_refs[s][:, tok, h * HEAD : (h + 1) * HEAD] = piece.astype(dq_refs[s].dtype)


def common_scratch():
    return [
        pltpu.VMEM((PARTS, KR, HEAD), BF),
        pltpu.VMEM((PARTS, KR, HEAD), BF),
        pltpu.VMEM((PARTS, QR, HEAD), BF),
        pltpu.VMEM((PARTS, QR, HEAD), BF),
        pltpu.VMEM((PARTS, KR, 128), F32),
    ]


def run_stats(kvs, qgs, kpos, qpos):
    return pl.pallas_call(
        stats_kernel,
        out_shape=[jax.ShapeDtypeStruct((PARTS * 4, QR), F32)] * 4,
        scratch_shapes=common_scratch() + [pltpu.VMEM((PARTS, 8, QR), F32)] * 3,
        compiler_params=pltpu.CompilerParams(vmem_limit_bytes=VMEM_LIMIT),
        cost_estimate=pl.CostEstimate(flops=6_000_000_000, bytes_accessed=3_000_000, transcendentals=5_000_000),
        name="stats",
    )(*kvs, *qgs, kpos, qpos)


def run_grads(kvs, qgs, kpos, qpos, sts):
    dkv = [jax.ShapeDtypeStruct((n, 2, TOK, 2 * HEAD), BF) for n in (4, 2, 2)]
    dq = [jax.ShapeDtypeStruct((2, TOK, GROUP * HEAD), F32 if s == 0 else BF) for s in range(4)]
    out = pl.pallas_call(
        grads_kernel,
        out_shape=dkv + dq,
        scratch_shapes=common_scratch()
        + [
            pltpu.VMEM((PARTS, HEAD, KR), BF),
            pltpu.VMEM((PARTS, KR, HEAD), F32),
            pltpu.VMEM((PARTS, KR, HEAD), F32),
            pltpu.VMEM((PARTS, HEAD, QR), F32),
            pltpu.VMEM((PARTS, 1, QR), F32),
            pltpu.VMEM((PARTS, 1, QR), F32),
        ],
        compiler_params=pltpu.CompilerParams(vmem_limit_bytes=VMEM_LIMIT),
        cost_estimate=pl.CostEstimate(flops=12_000_000_000, bytes_accessed=6_000_000, transcendentals=5_000_000),
        name="grads",
    )(*kvs, *qgs, kpos, qpos, *sts)
    return out[0], out[1:3], out[3:7]


def pack_kernel(at_ref, q_ref, g_ref, k_ref, v_ref, kv_own, qg_own, kv_send, qg_send):
    wide = GROUP * HEAD
    mine = at_ref[0]
    for which, kv, qg in ((mine, kv_own.at[0], qg_own.at[0]), (1 - mine, kv_send, qg_send)):
        cols = pl.ds(pl.multiple_of(which * wide, 128), wide)
        small = pl.ds(pl.multiple_of(which * HEAD, 128), HEAD)
        kv[:, :HEAD] = k_ref[:, small]
        kv[:, HEAD:] = v_ref[:, small]
        qg[:, :wide] = q_ref[:, cols]
        qg[:, wide:] = g_ref[:, cols]
    kv_own[1] = kv_send[...]
    qg_own[1] = qg_send[...]


def run_pack(at, q, g, k, v):
    kv, qg = (TOK, 2 * HEAD), (TOK, 2 * GROUP * HEAD)
    vmem = pl.BlockSpec(memory_space=pltpu.VMEM)
    return pl.pallas_call(
        pack_kernel,
        out_shape=[jax.ShapeDtypeStruct(a, BF) for a in ((2, *kv), (2, *qg), kv, qg)],
        in_specs=[pl.BlockSpec(memory_space=pltpu.SMEM)] + [vmem] * 4,
        name="pack",
    )(at, q, g, k, v)


def columns_kernel(at_ref, in_ref, *out_refs):
    for o in range(4):
        target = (at_ref[1] + o) % 4
        for n in range(4):
            src = pl.ds(pl.multiple_of(n * 4 * HEAD + target * HEAD, 128), HEAD)
            out_refs[o][:, n * HEAD : (n + 1) * HEAD] = in_ref[:, src]


def run_columns(at, layer_input):
    return pl.pallas_call(
        columns_kernel,
        out_shape=[jax.ShapeDtypeStruct((TOK, 4 * HEAD), BF)] * 4,
        in_specs=[pl.BlockSpec(memory_space=pltpu.SMEM), pl.BlockSpec(memory_space=pltpu.VMEM)],
        name="columns",
    )(at, layer_input)


def finish_kernel(in_ref, k_ref, v_ref):
    for h in range(2):
        total = in_ref[h].astype(F32)
        for n in range(1, 8):
            total = total + in_ref[2 * n + h].astype(F32)
        k_ref[:, h * HEAD : (h + 1) * HEAD] = total[:, :HEAD]
        v_ref[:, h * HEAD : (h + 1) * HEAD] = total[:, HEAD:]


def run_finish(got):
    out = jax.ShapeDtypeStruct((HEAD // 2, 2 * HEAD), F32)
    return pl.pallas_call(finish_kernel, out_shape=[out, out], name="finish")(got)


def positions(run_placement, y, z, x, c):
    def device(yy, zz, xx, cc):
        return (((yy % 4) * 2 + zz % 2) * 4 + xx % 4) * 2 + cc % 2

    b, a, e = jnp.meshgrid(jnp.arange(4), jnp.arange(2), jnp.arange(2), indexing="ij")
    keys = device(y, z + a, x + b, c + e).reshape(KSLOTS)
    a, e = jnp.meshgrid(jnp.arange(4), jnp.arange(2), indexing="ij")
    queries = device(y + a, z, x, c + e).reshape(QSLOTS)
    index = jnp.concatenate([keys, queries]).astype(jnp.int32)
    pick = (index[:, None] == jnp.arange(64, dtype=jnp.int32)[None, :]).astype(BF)
    slots = nt(pick, run_placement.astype(BF)).astype(BF)
    lane = jnp.arange(TOK, dtype=jnp.int32)
    spread = jnp.where(lane[None, :] // 2 == jnp.arange(64, dtype=jnp.int32)[:, None], 2.0, 0.0).astype(BF)
    pos = nn(slots, spread) + ((lane // 2) * TOK + lane % 2).astype(F32)[None, :]
    kpos = pos[:KSLOTS]
    qpos = pos[KSLOTS:].reshape(QSLOTS, PARTS, T).transpose(1, 0, 2).reshape(PARTS, 1, 1, QSLOTS * T)
    qpos = jnp.broadcast_to(qpos, (PARTS, 1, GROUP, QSLOTS * T)).reshape(PARTS, 1, QR)
    return kpos, qpos


def own_first(c, mine, other, axis):
    return jnp.where(c == 0, jnp.concatenate([mine, other], axis), jnp.concatenate([other, mine], axis))


def after(array, *gates):
    return lax.optimization_barrier((array, *gates))[0]


def step(query_rows, key_rows, value_rows, output_grad, layer_input, key_matrix, value_matrix, run_placement):
    y, z, x, c, t = (lax.axis_index(a) for a in ("y", "z", "x", "c", "tp"))
    at = jnp.stack([c, x, t]).astype(jnp.int32)
    kv_pair, qg_pair, kv_send, qg_send = run_pack(at, query_rows, output_grad, key_rows, value_rows)
    qg_own = qg_pair.at[1].set(moved(qg_send, "c", 1))
    kv_own = kv_pair.at[1].set(moved(kv_send, "c", 1))
    qgs = [qg_own] + [moved(qg_own, "y", -o) for o in (1, 2, 3)]
    kv_both = jnp.stack([kv_own, moved(kv_own, "z", 1)])
    kvs = [kv_both] + [moved(kv_both, "x", -o) for o in (1, 2, 3)]
    kpos, qpos = positions(run_placement, y, z, x, c)

    half = key_matrix.shape[0] // 2
    cuts = [lax.dynamic_slice_in_dim(after(m, kv_both), (1 - t) * half, half, 0) for m in (key_matrix, value_matrix)]
    x_pieces = run_columns(at, after(layer_input, kv_both))
    x_half = jnp.stack([x_pieces[0]] + [moved(x_pieces[4 - o], "x", -o) for o in (1, 2, 3)])
    x_other = moved(x_half, "tp", 1)
    x_here = jnp.where(t == 0, jnp.concatenate([x_half, x_other], 2), jnp.concatenate([x_other, x_half], 2))
    m_far = moved(jnp.where(c == 0, *cuts), "tp", 1)
    kpos = after(kpos, *x_pieces)

    sts = run_stats(kvs, qgs, kpos, qpos)
    sts = [sts[0]] + [moved(sts[o], "y", -o) for o in (1, 2, 3)]
    dkv_near, dkv_sent, dqs = run_grads(kvs, qgs, kpos, qpos, sts)

    def total_of(own, arrived):
        total = own.astype(F32)
        for a in arrived:
            total = total + a.astype(F32)
        return total.astype(BF)

    first = moved(dkv_sent[0], "z", 1)
    row1, row2 = (total_of(dkv_near[o], [first[o - 1]]) for o in (1, 2))
    last = moved(dkv_sent[1], "z", 1)
    near = after(dkv_near, row1)
    row3, row0 = (total_of(near[o], [last[n]]) for n, o in enumerate((3, 0)))
    dq = total_of(dqs[0], [moved(dqs[o], "y", o) for o in (1, 2, 3)])
    x_all = jnp.stack([x_here, moved(x_here, "c", 1)], axis=1)
    m_core = moved(m_far, "c", 1)
    k_far = jnp.where(c == 0, m_far, m_core)
    v_far = jnp.where(c == 0, m_core, m_far)

    dkv = total_of(row0, [moved(row, "x", o) for o, row in ((2, row2), (1, row1), (3, row3))])
    dkv_all = jnp.stack([dkv] + [moved(dkv, "x", -o) for o in (1, 2, 3)])
    dkv_far = moved(dkv[1], "c", 1)
    k_here = own_first(c, dkv[0, :, :HEAD], dkv_far[:, :HEAD], 1)
    v_here = own_first(c, dkv[0, :, HEAD:], dkv_far[:, HEAD:], 1)
    kv_here = jnp.concatenate([k_here, v_here], 1)
    kv_there = moved(kv_here, "tp", 1)

    query_grad = own_first(c, dq[0], moved(dq[1], "c", 1), 1)

    tokens = 8 * TOK
    weight = lax.dot_general(
        x_all.reshape(tokens, 8 * HEAD),
        dkv_all.reshape(tokens, 2 * HEAD),
        (((0,), (0,)), ((), ())),
        preferred_element_type=F32,
    )
    pieces = weight.astype(BF).reshape(16, HEAD // 2, 2 * HEAD)
    got = lax.all_to_all(pieces, ("y", "z", "c"), 0, 0, tiled=True)
    key_weight, value_weight = run_finish(got)

    km = lax.dynamic_slice_in_dim(key_matrix, t * half, half, 0)
    vm = lax.dynamic_slice_in_dim(value_matrix, t * half, half, 0)
    wide = 2 * HEAD
    total = nt(kv_here[:, :wide], km) + nt(kv_here[:, wide:], vm)
    input_grad = (total + nt(kv_there[:, :wide], k_far) + nt(kv_there[:, wide:], v_far)).astype(BF)
    return (query_grad, input_grad, key_weight, value_weight)


def solution(mesh):
    torus = Mesh(mesh.devices.reshape(4, 2, 4, 2, mesh.shape["tp"]), ("y", "z", "x", "c", "tp"))
    return jax.shard_map(
        step,
        mesh=torus,
        in_specs=(P(SEQ, "tp"),) * 5 + (P(None, "tp"),) * 2 + (P(),),
        out_specs=(P(SEQ, "tp"),) * 4,
        check_vma=False,
    )
```

```python
import math

import jax
import jax.numpy as jnp
from jax import lax
from jax.experimental import pallas as pl
from jax.experimental.pallas import tpu as pltpu
from jax.sharding import Mesh
from jax.sharding import PartitionSpec as P


HEAD = 128
WINDOW = 4096
GROUP = 4
TOK = 128
SEQ = ("y", "z", "x", "c")
BF = jnp.bfloat16
F32 = jnp.float32
NEG = -1e30

PARTS = 4
T = TOK // PARTS
KSLOTS = 16
QSLOTS = 8
KR = KSLOTS * T
QR = QSLOTS * GROUP * T
SPAN = PARTS // 2
SCALE = 1.0 / math.sqrt(HEAD)
SCORE2 = SCALE * math.log2(math.e)
VMEM_LIMIT = 60 * 1024 * 1024


def moved(array, axis, by):
    n = lax.axis_size(axis)
    return lax.ppermute(array, axis, [(i, (i + by) % n) for i in range(n)])


def nt(a, b):
    return lax.dot_general(a, b, (((1,), (1,)), ((), ())), preferred_element_type=F32)


def nn(a, b):
    return lax.dot_general(a, b, (((1,), (0,)), ((), ())), preferred_element_type=F32)


def part_copies(part, kv_refs, qg_refs, kv, qg, sem):
    tok = pl.ds(part * T, T)
    for b in range(4):
        yield pltpu.make_async_copy(kv_refs[b].at[:, :, tok, :], kv.at[part, b], sem.at[part, b])
    for s in range(4):
        yield pltpu.make_async_copy(qg_refs[s].at[:, tok, :], qg.at[part, s], sem.at[part, 4 + s])


def start_loads(kv_refs, qg_refs, kpos_ref, kv, qg, kposb, sem):
    for part in range(PARTS):
        for copy in part_copies(part, kv_refs, qg_refs, kv, qg, sem):
            copy.start()
    for slot in range(KSLOTS):
        column = jnp.broadcast_to(kpos_ref[slot : slot + 1, :], (TOK, 128)).T
        for part in range(PARTS):
            kposb[part, slot * T : (slot + 1) * T, :] = column[part * T : (part + 1) * T, :]


def keys_of(kv, ip):
    return kv[ip, :, :, :, :, :HEAD].reshape(KR, HEAD)


def values_of(kv, ip):
    return kv[ip, :, :, :, :, HEAD:].reshape(KR, HEAD)


def heads_of(qg, i, first):
    cols = [(first + h) * HEAD for h in range(GROUP)]
    return jnp.concatenate([qg[i, :, :, :, c : c + HEAD].reshape(QSLOTS * T, HEAD) for c in cols], axis=0)


def masked_scores(delta, i, ip, k, q, kposb, qpos_ref):
    s = nt(k, q) * SCORE2
    if delta == 0 or delta == SPAN:
        kp = jnp.concatenate([kposb[ip]] * (QR // 128), axis=1)
        qp = qpos_ref[i]
        valid = (kp <= qp) if delta == 0 else (kp > qp - float(WINDOW))
        s = jnp.where(valid, s, NEG)
    return s


def stats_kernel(*refs):
    kv_refs, qg_refs = refs[0:4], refs[4:8]
    kpos_ref, qpos_ref = refs[8:10]
    out_refs = refs[10:14]
    kv, qg, kposb, ms, ls, ws, sem = refs[14:]
    start_loads(kv_refs, qg_refs, kpos_ref, kv, qg, kposb, sem)
    ms[...] = jnp.full(ms.shape, NEG, F32)
    ls[...] = jnp.zeros(ls.shape, F32)
    ws[...] = jnp.zeros(ws.shape, F32)
    for delta in range(SPAN + 1):

        def body(i, carry, delta=delta):
            ip = i - delta
            if delta == 0:
                for copy in part_copies(i, kv_refs, qg_refs, kv, qg, sem):
                    copy.wait()
            s = masked_scores(delta, i, ip, keys_of(kv, ip), heads_of(qg, i, 0), kposb, qpos_ref)
            s = s.reshape(KR // 8, 8, QR)
            dp = nt(values_of(kv, ip), heads_of(qg, i, GROUP)).reshape(KR // 8, 8, QR)
            old = ms[i]
            new = jnp.maximum(old, jnp.max(s, axis=0))
            e = jnp.exp2(s - new[None])
            fade = jnp.exp2(old - new)
            ls[i] = ls[i] * fade + jnp.sum(e, axis=0)
            ws[i] = ws[i] * fade + jnp.sum(e * dp, axis=0)
            ms[i] = new
            return carry

        lax.fori_loop(delta, PARTS, body, 0)
    rows = []
    for i in range(PARTS):
        m8 = ms[i]
        top = jnp.max(m8, axis=0, keepdims=True)
        fade = jnp.exp2(m8 - top)
        total = jnp.sum(ls[i] * fade, axis=0, keepdims=True)
        weighted = jnp.sum(ws[i] * fade, axis=0, keepdims=True)
        rows += [top, total, weighted, jnp.zeros((1, QR), F32)]
    stats = jnp.concatenate(rows, axis=0)
    per_head = QSLOTS * T
    for o in range(4):
        for h in range(GROUP):
            cols = slice(h * per_head, (h + 1) * per_head)
            piece = stats[:, cols]
            out_refs[o][:, cols] = pltpu.roll(piece, o * 2 * T, 1) if o else piece


def grads_kernel(*refs):
    kv_refs, qg_refs = refs[0:4], refs[4:8]
    kpos_ref, qpos_ref = refs[8:10]
    st_refs = refs[10:14]
    dkv_near, dkv_first, dkv_last, dq_refs = refs[14], refs[15], refs[16], refs[17:21]
    kv, qg, kposb, kt, qt, gt, dks, dvs, dqt, lse, mean, dkv_out, dq_wide, dq_out, sem, out_sem = refs[21:]
    start_loads(kv_refs, qg_refs, kpos_ref, kv, qg, kposb, sem)
    for part in range(PARTS):
        st = [r[part * 4 : part * 4 + 3, :] for r in st_refs]
        top = jnp.maximum(jnp.maximum(st[0][0:1], st[1][0:1]), jnp.maximum(st[2][0:1], st[3][0:1]))
        fade = [jnp.exp2(a[0:1] - top) for a in st]
        total = sum(a[1:2] * f for a, f in zip(st, fade))
        lse[part] = top + jnp.log2(total)
        mean[part] = sum(a[2:3] * f for a, f in zip(st, fade)) / total

    def dkv_copies(part):
        tok = slice(part * T, (part + 1) * T)
        pairs = (
            (dkv_out.at[part, 0], dkv_near.at[:, :, tok, :]),
            (dkv_out.at[part, 1, 1:3], dkv_first.at[:, :, tok, :]),
            (dkv_out.at[part, 1, 3], dkv_last.at[0, :, tok, :]),
            (dkv_out.at[part, 1, 0], dkv_last.at[1, :, tok, :]),
        )
        return [pltpu.make_async_copy(a, b, out_sem.at[part, n]) for n, (a, b) in enumerate(pairs)]

    def dq_copies(part):
        tok = slice(part * T, (part + 1) * T)
        pairs = [(dq_wide.at[part], dq_refs[0].at[:, tok, :])]
        pairs += [(dq_out.at[part, s - 1], dq_refs[s].at[:, tok, :]) for s in (1, 2, 3)]
        return [pltpu.make_async_copy(a, b, out_sem.at[part, 4 + n]) for n, (a, b) in enumerate(pairs)]

    def emit_dkv(part):
        dk = (dks[part] * SCALE).astype(BF).T.reshape(4, 2, 2, T, HEAD)
        dv = dvs[part].astype(BF).T.reshape(4, 2, 2, T, HEAD)
        for a in range(2):
            dkv_out[part, a, :, :, :, :HEAD] = dk[:, a]
            dkv_out[part, a, :, :, :, HEAD:] = dv[:, a]
        for copy in dkv_copies(part):
            copy.start()

    def emit_dq(part):
        dq = dqt[part].T * SCALE
        for h in range(GROUP):
            cols = slice(h * HEAD, (h + 1) * HEAD)
            rows = dq[h * QSLOTS * T : (h + 1) * QSLOTS * T, :].reshape(4, 2, T, HEAD)
            dq_wide[part, :, :, cols] = rows[0]
            dq_out[part, :, :, :, cols] = rows[1:4].astype(BF)
        for copy in dq_copies(part):
            copy.start()

    for delta in range(SPAN + 1):

        def body(i, carry, delta=delta):
            ip = i - delta
            if delta == 0:
                for copy in part_copies(i, kv_refs, qg_refs, kv, qg, sem):
                    copy.wait()
            k, q, g = keys_of(kv, ip), heads_of(qg, i, 0), heads_of(qg, i, GROUP)
            if delta == 0:
                kt[i], qt[i], gt[i] = k.T, q.T, g.T
            p = jnp.exp2(masked_scores(delta, i, ip, k, q, kposb, qpos_ref) - lse[i])
            ds = (p * (nt(values_of(kv, ip), g) - mean[i])).astype(BF)
            p = p.astype(BF)
            dk, dv, dq = nt(qt[i], ds), nt(gt[i], p), nn(kt[ip], ds)
            if delta == 0:
                dks[ip], dvs[ip], dqt[i] = dk, dv, dq
            else:
                dks[ip] += dk
                dvs[ip] += dv
                dqt[i] += dq
            return carry

        lax.fori_loop(delta, PARTS, body, 0)
        for part in range(PARTS):
            if delta == min(SPAN, PARTS - 1 - part):
                emit_dkv(part)
            if delta == min(SPAN, part):
                emit_dq(part)
    for part in range(PARTS):
        for copy in dkv_copies(part) + dq_copies(part):
            copy.wait()


def common_scratch():
    return [
        pltpu.VMEM((PARTS, 4, 2, 2, T, 2 * HEAD), BF),
        pltpu.VMEM((PARTS, 4, 2, T, 2 * GROUP * HEAD), BF),
        pltpu.VMEM((PARTS, KR, 128), F32),
    ]


def in_places(small):
    return [pl.BlockSpec(memory_space=pl.ANY)] * 8 + [pl.BlockSpec(memory_space=pltpu.VMEM)] * small


def run_stats(kvs, qgs, kpos, qpos):
    return pl.pallas_call(
        stats_kernel,
        out_shape=[jax.ShapeDtypeStruct((PARTS * 4, QR), F32)] * 4,
        in_specs=in_places(2),
        scratch_shapes=common_scratch()
        + [pltpu.VMEM((PARTS, 8, QR), F32)] * 3
        + [pltpu.SemaphoreType.DMA((PARTS, 8))],
        compiler_params=pltpu.CompilerParams(vmem_limit_bytes=VMEM_LIMIT),
        cost_estimate=pl.CostEstimate(flops=6_000_000_000, bytes_accessed=3_000_000, transcendentals=5_000_000),
        name="stats",
    )(*kvs, *qgs, kpos, qpos)


def run_grads(kvs, qgs, kpos, qpos, sts):
    dkv = [jax.ShapeDtypeStruct((n, 2, TOK, 2 * HEAD), BF) for n in (4, 2, 2)]
    dq = [jax.ShapeDtypeStruct((2, TOK, GROUP * HEAD), F32 if s == 0 else BF) for s in range(4)]
    out = pl.pallas_call(
        grads_kernel,
        out_shape=dkv + dq,
        in_specs=in_places(6),
        out_specs=[pl.BlockSpec(memory_space=pl.ANY)] * 7,
        scratch_shapes=common_scratch()
        + [
            pltpu.VMEM((PARTS, HEAD, KR), BF),
            pltpu.VMEM((PARTS, HEAD, QR), BF),
            pltpu.VMEM((PARTS, HEAD, QR), BF),
            pltpu.VMEM((PARTS, HEAD, KR), F32),
            pltpu.VMEM((PARTS, HEAD, KR), F32),
            pltpu.VMEM((PARTS, HEAD, QR), F32),
            pltpu.VMEM((PARTS, 1, QR), F32),
            pltpu.VMEM((PARTS, 1, QR), F32),
            pltpu.VMEM((PARTS, 2, 4, 2, T, 2 * HEAD), BF),
            pltpu.VMEM((PARTS, 2, T, GROUP * HEAD), F32),
            pltpu.VMEM((PARTS, 3, 2, T, GROUP * HEAD), BF),
            pltpu.SemaphoreType.DMA((PARTS, 8)),
            pltpu.SemaphoreType.DMA((PARTS, 8)),
        ],
        compiler_params=pltpu.CompilerParams(vmem_limit_bytes=VMEM_LIMIT),
        cost_estimate=pl.CostEstimate(flops=12_000_000_000, bytes_accessed=6_000_000, transcendentals=5_000_000),
        name="grads",
    )(*kvs, *qgs, kpos, qpos, *sts)
    return out[0], out[1:3], out[3:7]


def pack_kernel(at_ref, q_ref, g_ref, k_ref, v_ref, kv_own, qg_own, kv_send, qg_send, sem):
    wide = GROUP * HEAD
    mine = at_ref[0]
    copies = []
    for which, kv, qg in ((1 - mine, kv_send, qg_send), (mine, kv_own.at[0], qg_own.at[0])):
        cols = pl.ds(pl.multiple_of(which * wide, 128), wide)
        small = pl.ds(pl.multiple_of(which * HEAD, 128), HEAD)
        for src, dst in (
            (k_ref.at[:, small], kv.at[:, :HEAD]),
            (v_ref.at[:, small], kv.at[:, HEAD:]),
            (q_ref.at[:, cols], qg.at[:, :wide]),
            (g_ref.at[:, cols], qg.at[:, wide:]),
        ):
            copies.append(pltpu.make_async_copy(src, dst, sem.at[len(copies)]))
            copies[-1].start()
    for copy in copies:
        copy.wait()


def run_pack(at, q, g, k, v):
    kv, qg = (TOK, 2 * HEAD), (TOK, 2 * GROUP * HEAD)
    anywhere = pl.BlockSpec(memory_space=pl.ANY)
    return pl.pallas_call(
        pack_kernel,
        out_shape=[jax.ShapeDtypeStruct(a, BF) for a in ((2, *kv), (2, *qg), kv, qg)],
        in_specs=[pl.BlockSpec(memory_space=pltpu.SMEM)] + [anywhere] * 4,
        out_specs=[anywhere] * 4,
        scratch_shapes=[pltpu.SemaphoreType.DMA((8,))],
        name="pack",
    )(at, q, g, k, v)


def columns_kernel(at_ref, mine_ref, far_ref, out_0, out_1, out_2, out_3, sem):
    copies = []
    for ref, half in ((mine_ref, at_ref[2]), (far_ref, 1 - at_ref[2])):
        for o, out in enumerate((out_0, out_1, out_2, out_3)):
            target = (at_ref[1] + o) % 4
            for n in range(4):
                src = pl.ds(pl.multiple_of(n * 4 * HEAD + target * HEAD, 128), HEAD)
                dst = pl.ds(pl.multiple_of(half * 4 * HEAD + n * HEAD, 128), HEAD)
                copies.append(pltpu.make_async_copy(ref.at[:, src], out.at[:, dst], sem.at[len(copies)]))
                copies[-1].start()
    for copy in copies:
        copy.wait()


def run_columns(at, mine, far):
    anywhere = pl.BlockSpec(memory_space=pl.ANY)
    return pl.pallas_call(
        columns_kernel,
        out_shape=[jax.ShapeDtypeStruct((TOK, 8 * HEAD), BF)] * 4,
        in_specs=[pl.BlockSpec(memory_space=pltpu.SMEM), anywhere, anywhere],
        out_specs=[anywhere] * 4,
        scratch_shapes=[pltpu.SemaphoreType.DMA((32,))],
        name="columns",
    )(at, mine, far)


def finish_kernel(in_ref, k_ref, v_ref):
    for h in range(2):
        total = in_ref[h].astype(F32)
        for n in range(1, 8):
            total = total + in_ref[2 * n + h].astype(F32)
        k_ref[:, h * HEAD : (h + 1) * HEAD] = total[:, :HEAD]
        v_ref[:, h * HEAD : (h + 1) * HEAD] = total[:, HEAD:]


def run_finish(got):
    out = jax.ShapeDtypeStruct((HEAD // 2, 2 * HEAD), F32)
    return pl.pallas_call(finish_kernel, out_shape=[out, out], name="finish")(got)


def positions(run_placement, y, z, x, c):
    def device(yy, zz, xx, cc):
        return (((yy % 4) * 2 + zz % 2) * 4 + xx % 4) * 2 + cc % 2

    b, a, e = jnp.meshgrid(jnp.arange(4), jnp.arange(2), jnp.arange(2), indexing="ij")
    keys = device(y, z + a, x + b, c + e).reshape(KSLOTS)
    a, e = jnp.meshgrid(jnp.arange(4), jnp.arange(2), indexing="ij")
    queries = device(y + a, z, x, c + e).reshape(QSLOTS)
    index = jnp.concatenate([keys, queries]).astype(jnp.int32)
    pick = (index[:, None] == jnp.arange(64, dtype=jnp.int32)[None, :]).astype(BF)
    slots = nt(pick, run_placement.astype(BF)).astype(BF)
    lane = jnp.arange(TOK, dtype=jnp.int32)
    spread = jnp.where(lane[None, :] // 2 == jnp.arange(64, dtype=jnp.int32)[:, None], 2.0, 0.0).astype(BF)
    pos = nn(slots, spread) + ((lane // 2) * TOK + lane % 2).astype(F32)[None, :]
    kpos = pos[:KSLOTS]
    qpos = pos[KSLOTS:].reshape(QSLOTS, PARTS, T).transpose(1, 0, 2).reshape(PARTS, 1, 1, QSLOTS * T)
    qpos = jnp.broadcast_to(qpos, (PARTS, 1, GROUP, QSLOTS * T)).reshape(PARTS, 1, QR)
    return kpos, qpos


def own_first(c, mine, other, axis):
    return jnp.where(c == 0, jnp.concatenate([mine, other], axis), jnp.concatenate([other, mine], axis))


def after(array, *gates):
    return lax.optimization_barrier((array, *gates))[0]


def step(query_rows, key_rows, value_rows, output_grad, layer_input, key_matrix, value_matrix, run_placement):
    y, z, x, c, t = (lax.axis_index(a) for a in ("y", "z", "x", "c", "tp"))
    at = jnp.stack([c, x, t]).astype(jnp.int32)
    kv_pair, qg_pair, kv_send, qg_send = run_pack(at, query_rows, output_grad, key_rows, value_rows)
    qg_own = qg_pair.at[1].set(moved(qg_send, "c", 1))
    kv_own = kv_pair.at[1].set(moved(kv_send, "c", 1))
    qgs = [qg_own] + [moved(qg_own, "y", -o) for o in (1, 2, 3)]
    kv_both = jnp.stack([kv_own, moved(kv_own, "z", 1)])
    kvs = [kv_both] + [moved(kv_both, "x", -o) for o in (1, 2, 3)]
    kpos, qpos = positions(run_placement, y, z, x, c)

    half = key_matrix.shape[0] // 2
    cuts = [lax.dynamic_slice_in_dim(after(m, kv_both), (1 - t) * half, half, 0) for m in (key_matrix, value_matrix)]
    x_far = moved(layer_input, "tp", 1)
    m_far = moved(jnp.where(c == 0, *cuts), "tp", 1)

    sts = run_stats(kvs, qgs, kpos, qpos)
    sts = [sts[0]] + [moved(sts[o], "y", -o) for o in (1, 2, 3)]
    x_pieces = run_columns(at, layer_input, after(x_far, sts[0]))
    x_here = jnp.stack([x_pieces[0]] + [moved(x_pieces[4 - o], "x", -o) for o in (1, 2, 3)])
    dkv_near, dkv_sent, dqs = run_grads(kvs, qgs, kpos, qpos, sts)

    def total_of(own, arrived):
        total = own.astype(F32)
        for a in arrived:
            total = total + a.astype(F32)
        return total.astype(BF)

    first = moved(dkv_sent[0], "z", 1)
    row1, row2 = (total_of(dkv_near[o], [first[o - 1]]) for o in (1, 2))
    last = moved(dkv_sent[1], "z", 1)
    near = after(dkv_near, row1)
    row3, row0 = (total_of(near[o], [last[n]]) for n, o in enumerate((3, 0)))
    dq = total_of(dqs[0], [moved(dqs[o], "y", o) for o in (1, 2, 3)])
    x_all = jnp.stack([x_here, moved(x_here, "c", 1)], axis=1)
    m_core = moved(m_far, "c", 1)
    k_far = jnp.where(c == 0, m_far, m_core)
    v_far = jnp.where(c == 0, m_core, m_far)

    dkv = total_of(row0, [moved(row, "x", o) for o, row in ((2, row2), (1, row1), (3, row3))])
    dkv_all = jnp.stack([dkv] + [moved(dkv, "x", -o) for o in (1, 2, 3)])
    dkv_far = moved(dkv[1], "c", 1)
    k_here = own_first(c, dkv[0, :, :HEAD], dkv_far[:, :HEAD], 1)
    v_here = own_first(c, dkv[0, :, HEAD:], dkv_far[:, HEAD:], 1)
    kv_here = jnp.concatenate([k_here, v_here], 1)
    kv_there = moved(kv_here, "tp", 1)

    query_grad = own_first(c, dq[0], moved(dq[1], "c", 1), 1)

    tokens = 8 * TOK
    weight = lax.dot_general(
        x_all.reshape(tokens, 8 * HEAD),
        dkv_all.reshape(tokens, 2 * HEAD),
        (((0,), (0,)), ((), ())),
        preferred_element_type=F32,
    )
    pieces = weight.astype(BF).reshape(16, HEAD // 2, 2 * HEAD)
    got = lax.all_to_all(pieces, ("y", "z", "c"), 0, 0, tiled=True)
    key_weight, value_weight = run_finish(got)

    km = lax.dynamic_slice_in_dim(key_matrix, t * half, half, 0)
    vm = lax.dynamic_slice_in_dim(value_matrix, t * half, half, 0)
    wide = 2 * HEAD
    total = nt(kv_here[:, :wide], km) + nt(kv_here[:, wide:], vm)
    input_grad = (total + nt(kv_there[:, :wide], k_far) + nt(kv_there[:, wide:], v_far)).astype(BF)
    return (query_grad, input_grad, key_weight, value_weight)


def solution(mesh):
    torus = Mesh(mesh.devices.reshape(4, 2, 4, 2, mesh.shape["tp"]), ("y", "z", "x", "c", "tp"))
    return jax.shard_map(
        step,
        mesh=torus,
        in_specs=(P(SEQ, "tp"),) * 5 + (P(None, "tp"),) * 2 + (P(),),
        out_specs=(P(SEQ, "tp"),) * 4,
        check_vma=False,
    )
```

```python
import math

import jax
import jax.numpy as jnp
from jax import lax
from jax.experimental import pallas as pl
from jax.experimental.pallas import tpu as pltpu
from jax.sharding import Mesh
from jax.sharding import PartitionSpec as P


HEAD = 128
WINDOW = 4096
GROUP = 4
TOK = 128
SEQ = ("y", "z", "x", "c")
BF = jnp.bfloat16
F32 = jnp.float32
NEG = -1e30

PARTS = 4
T = TOK // PARTS
KSLOTS = 16
QSLOTS = 8
KR = KSLOTS * T
QR = QSLOTS * GROUP * T
SPAN = PARTS // 2
SCALE = 1.0 / math.sqrt(HEAD)
SCORE2 = SCALE * math.log2(math.e)
VMEM_LIMIT = 60 * 1024 * 1024


def moved(array, axis, by):
    n = lax.axis_size(axis)
    return lax.ppermute(array, axis, [(i, (i + by) % n) for i in range(n)])


def nt(a, b):
    return lax.dot_general(a, b, (((1,), (1,)), ((), ())), preferred_element_type=F32)


def nn(a, b):
    return lax.dot_general(a, b, (((1,), (0,)), ((), ())), preferred_element_type=F32)


def part_copies(part, kv_refs, qg_refs, kv, qg, sem):
    tok = pl.ds(part * T, T)
    for b in range(4):
        yield pltpu.make_async_copy(kv_refs[b].at[:, :, tok, :], kv.at[part, b], sem.at[part, b])
    for s in range(4):
        yield pltpu.make_async_copy(qg_refs[s].at[:, tok, :], qg.at[part, s], sem.at[part, 4 + s])


def start_loads(kv_refs, qg_refs, kpos_ref, kv, qg, kposb, sem):
    for part in range(PARTS):
        for copy in part_copies(part, kv_refs, qg_refs, kv, qg, sem):
            copy.start()
    for slot in range(KSLOTS):
        column = jnp.broadcast_to(kpos_ref[slot : slot + 1, :], (TOK, 128)).T
        for part in range(PARTS):
            kposb[part, slot * T : (slot + 1) * T, :] = column[part * T : (part + 1) * T, :]


def keys_of(kv, ip):
    return kv[ip, :, :, :, :, :HEAD].reshape(KR, HEAD)


def values_of(kv, ip):
    return kv[ip, :, :, :, :, HEAD:].reshape(KR, HEAD)


def heads_of(qg, i, first):
    cols = [(first + h) * HEAD for h in range(GROUP)]
    return jnp.concatenate([qg[i, :, :, :, c : c + HEAD].reshape(QSLOTS * T, HEAD) for c in cols], axis=0)


def masked_scores(delta, i, ip, k, q, kposb, qpos_ref):
    s = nt(k, q) * SCORE2
    if delta == 0 or delta == SPAN:
        kp = jnp.concatenate([kposb[ip]] * (QR // 128), axis=1)
        qp = qpos_ref[i]
        valid = (kp <= qp) if delta == 0 else (kp > qp - float(WINDOW))
        s = jnp.where(valid, s, NEG)
    return s


def stats_kernel(*refs):
    kv_refs, qg_refs = refs[0:4], refs[4:8]
    kpos_ref, qpos_ref = refs[8:10]
    out_refs = refs[10:14]
    kv, qg, kposb, ms, ls, ws, sem = refs[14:]
    start_loads(kv_refs, qg_refs, kpos_ref, kv, qg, kposb, sem)
    ms[...] = jnp.full(ms.shape, NEG, F32)
    ls[...] = jnp.zeros(ls.shape, F32)
    ws[...] = jnp.zeros(ws.shape, F32)
    for delta in range(SPAN + 1):

        def body(i, carry, delta=delta):
            ip = i - delta
            if delta == 0:
                for copy in part_copies(i, kv_refs, qg_refs, kv, qg, sem):
                    copy.wait()
            s = masked_scores(delta, i, ip, keys_of(kv, ip), heads_of(qg, i, 0), kposb, qpos_ref)
            s = s.reshape(KR // 8, 8, QR)
            dp = nt(values_of(kv, ip), heads_of(qg, i, GROUP)).reshape(KR // 8, 8, QR)
            old = ms[i]
            new = jnp.maximum(old, jnp.max(s, axis=0))
            e = jnp.exp2(s - new[None])
            fade = jnp.exp2(old - new)
            ls[i] = ls[i] * fade + jnp.sum(e, axis=0)
            ws[i] = ws[i] * fade + jnp.sum(e * dp, axis=0)
            ms[i] = new
            return carry

        lax.fori_loop(delta, PARTS, body, 0)
    rows = []
    for i in range(PARTS):
        m8 = ms[i]
        top = jnp.max(m8, axis=0, keepdims=True)
        fade = jnp.exp2(m8 - top)
        total = jnp.sum(ls[i] * fade, axis=0, keepdims=True)
        weighted = jnp.sum(ws[i] * fade, axis=0, keepdims=True)
        rows += [top, total, weighted, jnp.zeros((1, QR), F32)]
    stats = jnp.concatenate(rows, axis=0)
    per_head = QSLOTS * T
    for o in range(4):
        for h in range(GROUP):
            cols = slice(h * per_head, (h + 1) * per_head)
            piece = stats[:, cols]
            out_refs[o][:, cols] = pltpu.roll(piece, o * 2 * T, 1) if o else piece


def grads_kernel(*refs):
    kv_refs, qg_refs = refs[0:4], refs[4:8]
    kpos_ref, qpos_ref = refs[8:10]
    st_refs = refs[10:14]
    dkv_near, dkv_first, dkv_last, dq_refs = refs[14], refs[15], refs[16], refs[17:21]
    kv, qg, kposb, kt, dks, dvs, dqt, lse, mean, dkv_out, dq_wide, dq_out, sem, out_sem = refs[21:]
    start_loads(kv_refs, qg_refs, kpos_ref, kv, qg, kposb, sem)
    for part in range(PARTS):
        st = [r[part * 4 : part * 4 + 3, :] for r in st_refs]
        top = jnp.maximum(jnp.maximum(st[0][0:1], st[1][0:1]), jnp.maximum(st[2][0:1], st[3][0:1]))
        fade = [jnp.exp2(a[0:1] - top) for a in st]
        total = sum(a[1:2] * f for a, f in zip(st, fade))
        lse[part] = top + jnp.log2(total)
        mean[part] = sum(a[2:3] * f for a, f in zip(st, fade)) / total

    def dkv_copies(part):
        tok = slice(part * T, (part + 1) * T)
        pairs = (
            (dkv_out.at[part, 0], dkv_near.at[:, :, tok, :]),
            (dkv_out.at[part, 1, 1:3], dkv_first.at[:, :, tok, :]),
            (dkv_out.at[part, 1, 3], dkv_last.at[0, :, tok, :]),
            (dkv_out.at[part, 1, 0], dkv_last.at[1, :, tok, :]),
        )
        return [pltpu.make_async_copy(a, b, out_sem.at[part, n]) for n, (a, b) in enumerate(pairs)]

    def dq_copies(part):
        tok = slice(part * T, (part + 1) * T)
        pairs = [(dq_wide.at[part], dq_refs[0].at[:, tok, :])]
        pairs += [(dq_out.at[part, s - 1], dq_refs[s].at[:, tok, :]) for s in (1, 2, 3)]
        return [pltpu.make_async_copy(a, b, out_sem.at[part, 4 + n]) for n, (a, b) in enumerate(pairs)]

    def emit_dkv(part):
        dk = (dks[part] * SCALE).astype(BF).reshape(4, 2, 2, T, HEAD)
        dv = dvs[part].astype(BF).reshape(4, 2, 2, T, HEAD)
        for a in range(2):
            dkv_out[part, a, :, :, :, :HEAD] = dk[:, a]
            dkv_out[part, a, :, :, :, HEAD:] = dv[:, a]
        for copy in dkv_copies(part):
            copy.start()

    def emit_dq(part):
        dq = dqt[part].T * SCALE
        for h in range(GROUP):
            cols = slice(h * HEAD, (h + 1) * HEAD)
            rows = dq[h * QSLOTS * T : (h + 1) * QSLOTS * T, :].reshape(4, 2, T, HEAD)
            dq_wide[part, :, :, cols] = rows[0]
            dq_out[part, :, :, :, cols] = rows[1:4].astype(BF)
        for copy in dq_copies(part):
            copy.start()

    for delta in range(SPAN + 1):

        def body(i, carry, delta=delta):
            ip = i - delta
            if delta == 0:
                for copy in part_copies(i, kv_refs, qg_refs, kv, qg, sem):
                    copy.wait()
            k, q, g = keys_of(kv, ip), heads_of(qg, i, 0), heads_of(qg, i, GROUP)
            if delta == 0:
                kt[i] = k.T
            p = jnp.exp2(masked_scores(delta, i, ip, k, q, kposb, qpos_ref) - lse[i])
            ds = (p * (nt(values_of(kv, ip), g) - mean[i])).astype(BF)
            p = p.astype(BF)
            dk, dv, dq = nn(ds, q), nn(p, g), nn(kt[ip], ds)
            if delta == 0:
                dks[ip], dvs[ip], dqt[i] = dk, dv, dq
            else:
                dks[ip] += dk
                dvs[ip] += dv
                dqt[i] += dq
            return carry

        lax.fori_loop(delta, PARTS, body, 0)
        for part in range(PARTS):
            if delta == min(SPAN, PARTS - 1 - part):
                emit_dkv(part)
            if delta == min(SPAN, part):
                emit_dq(part)
    for part in range(PARTS):
        for copy in dkv_copies(part) + dq_copies(part):
            copy.wait()


def common_scratch():
    return [
        pltpu.VMEM((PARTS, 4, 2, 2, T, 2 * HEAD), BF),
        pltpu.VMEM((PARTS, 4, 2, T, 2 * GROUP * HEAD), BF),
        pltpu.VMEM((PARTS, KR, 128), F32),
    ]


def in_places(small):
    return [pl.BlockSpec(memory_space=pl.ANY)] * 8 + [pl.BlockSpec(memory_space=pltpu.VMEM)] * small


def run_stats(kvs, qgs, kpos, qpos):
    return pl.pallas_call(
        stats_kernel,
        out_shape=[jax.ShapeDtypeStruct((PARTS * 4, QR), F32)] * 4,
        in_specs=in_places(2),
        scratch_shapes=common_scratch()
        + [pltpu.VMEM((PARTS, 8, QR), F32)] * 3
        + [pltpu.SemaphoreType.DMA((PARTS, 8))],
        compiler_params=pltpu.CompilerParams(vmem_limit_bytes=VMEM_LIMIT),
        cost_estimate=pl.CostEstimate(flops=6_000_000_000, bytes_accessed=3_000_000, transcendentals=5_000_000),
        name="stats",
    )(*kvs, *qgs, kpos, qpos)


def run_grads(kvs, qgs, kpos, qpos, sts):
    dkv = [jax.ShapeDtypeStruct((n, 2, TOK, 2 * HEAD), BF) for n in (4, 2, 2)]
    dq = [jax.ShapeDtypeStruct((2, TOK, GROUP * HEAD), F32 if s == 0 else BF) for s in range(4)]
    out = pl.pallas_call(
        grads_kernel,
        out_shape=dkv + dq,
        in_specs=in_places(6),
        out_specs=[pl.BlockSpec(memory_space=pl.ANY)] * 7,
        scratch_shapes=common_scratch()
        + [
            pltpu.VMEM((PARTS, HEAD, KR), BF),
            pltpu.VMEM((PARTS, KR, HEAD), F32),
            pltpu.VMEM((PARTS, KR, HEAD), F32),
            pltpu.VMEM((PARTS, HEAD, QR), F32),
            pltpu.VMEM((PARTS, 1, QR), F32),
            pltpu.VMEM((PARTS, 1, QR), F32),
            pltpu.VMEM((PARTS, 2, 4, 2, T, 2 * HEAD), BF),
            pltpu.VMEM((PARTS, 2, T, GROUP * HEAD), F32),
            pltpu.VMEM((PARTS, 3, 2, T, GROUP * HEAD), BF),
            pltpu.SemaphoreType.DMA((PARTS, 8)),
            pltpu.SemaphoreType.DMA((PARTS, 8)),
        ],
        compiler_params=pltpu.CompilerParams(vmem_limit_bytes=VMEM_LIMIT),
        cost_estimate=pl.CostEstimate(flops=12_000_000_000, bytes_accessed=6_000_000, transcendentals=5_000_000),
        name="grads",
    )(*kvs, *qgs, kpos, qpos, *sts)
    return out[0], out[1:3], out[3:7]


def pack_kernel(at_ref, q_ref, g_ref, k_ref, v_ref, kv_own, qg_own, kv_send, qg_send):
    wide = GROUP * HEAD
    mine = at_ref[0]
    for which, kv, qg in ((mine, kv_own.at[0], qg_own.at[0]), (1 - mine, kv_send, qg_send)):
        cols = pl.ds(pl.multiple_of(which * wide, 128), wide)
        small = pl.ds(pl.multiple_of(which * HEAD, 128), HEAD)
        kv[:, :HEAD] = k_ref[:, small]
        kv[:, HEAD:] = v_ref[:, small]
        qg[:, :wide] = q_ref[:, cols]
        qg[:, wide:] = g_ref[:, cols]
    kv_own[1] = kv_send[...]
    qg_own[1] = qg_send[...]


def run_pack(at, q, g, k, v):
    kv, qg = (TOK, 2 * HEAD), (TOK, 2 * GROUP * HEAD)
    vmem = pl.BlockSpec(memory_space=pltpu.VMEM)
    return pl.pallas_call(
        pack_kernel,
        out_shape=[jax.ShapeDtypeStruct(a, BF) for a in ((2, *kv), (2, *qg), kv, qg)],
        in_specs=[pl.BlockSpec(memory_space=pltpu.SMEM)] + [vmem] * 4,
        name="pack",
    )(at, q, g, k, v)


def columns_kernel(at_ref, in_ref, *out_refs):
    for o in range(4):
        target = (at_ref[1] + o) % 4
        for n in range(4):
            src = pl.ds(pl.multiple_of(n * 4 * HEAD + target * HEAD, 128), HEAD)
            out_refs[o][:, n * HEAD : (n + 1) * HEAD] = in_ref[:, src]


def run_columns(at, layer_input):
    return pl.pallas_call(
        columns_kernel,
        out_shape=[jax.ShapeDtypeStruct((TOK, 4 * HEAD), BF)] * 4,
        in_specs=[pl.BlockSpec(memory_space=pltpu.SMEM), pl.BlockSpec(memory_space=pltpu.VMEM)],
        name="columns",
    )(at, layer_input)


def finish_kernel(in_ref, k_ref, v_ref):
    for h in range(2):
        total = in_ref[h].astype(F32)
        for n in range(1, 8):
            total = total + in_ref[2 * n + h].astype(F32)
        k_ref[:, h * HEAD : (h + 1) * HEAD] = total[:, :HEAD]
        v_ref[:, h * HEAD : (h + 1) * HEAD] = total[:, HEAD:]


def run_finish(got):
    out = jax.ShapeDtypeStruct((HEAD // 2, 2 * HEAD), F32)
    return pl.pallas_call(finish_kernel, out_shape=[out, out], name="finish")(got)


def positions(run_placement, y, z, x, c):
    def device(yy, zz, xx, cc):
        return (((yy % 4) * 2 + zz % 2) * 4 + xx % 4) * 2 + cc % 2

    b, a, e = jnp.meshgrid(jnp.arange(4), jnp.arange(2), jnp.arange(2), indexing="ij")
    keys = device(y, z + a, x + b, c + e).reshape(KSLOTS)
    a, e = jnp.meshgrid(jnp.arange(4), jnp.arange(2), indexing="ij")
    queries = device(y + a, z, x, c + e).reshape(QSLOTS)
    index = jnp.concatenate([keys, queries]).astype(jnp.int32)
    pick = (index[:, None] == jnp.arange(64, dtype=jnp.int32)[None, :]).astype(BF)
    slots = nt(pick, run_placement.astype(BF)).astype(BF)
    lane = jnp.arange(TOK, dtype=jnp.int32)
    spread = jnp.where(lane[None, :] // 2 == jnp.arange(64, dtype=jnp.int32)[:, None], 2.0, 0.0).astype(BF)
    pos = nn(slots, spread) + ((lane // 2) * TOK + lane % 2).astype(F32)[None, :]
    kpos = pos[:KSLOTS]
    qpos = pos[KSLOTS:].reshape(QSLOTS, PARTS, T).transpose(1, 0, 2).reshape(PARTS, 1, 1, QSLOTS * T)
    qpos = jnp.broadcast_to(qpos, (PARTS, 1, GROUP, QSLOTS * T)).reshape(PARTS, 1, QR)
    return kpos, qpos


def own_first(c, mine, other, axis):
    return jnp.where(c == 0, jnp.concatenate([mine, other], axis), jnp.concatenate([other, mine], axis))


def after(array, *gates):
    return lax.optimization_barrier((array, *gates))[0]


def step(query_rows, key_rows, value_rows, output_grad, layer_input, key_matrix, value_matrix, run_placement):
    y, z, x, c, t = (lax.axis_index(a) for a in ("y", "z", "x", "c", "tp"))
    at = jnp.stack([c, x, t]).astype(jnp.int32)
    kv_pair, qg_pair, kv_send, qg_send = run_pack(at, query_rows, output_grad, key_rows, value_rows)
    qg_own = qg_pair.at[1].set(moved(qg_send, "c", 1))
    kv_own = kv_pair.at[1].set(moved(kv_send, "c", 1))
    qgs = [qg_own] + [moved(qg_own, "y", -o) for o in (1, 2, 3)]
    kv_both = jnp.stack([kv_own, moved(kv_own, "z", 1)])
    kvs = [kv_both] + [moved(kv_both, "x", -o) for o in (1, 2, 3)]
    kpos, qpos = positions(run_placement, y, z, x, c)

    half = key_matrix.shape[0] // 2
    cuts = [lax.dynamic_slice_in_dim(after(m, kv_own), (1 - t) * half, half, 0) for m in (key_matrix, value_matrix)]
    x_pieces = run_columns(at, after(layer_input, kv_both))
    x_half = jnp.stack([x_pieces[0]] + [moved(x_pieces[4 - o], "x", -o) for o in (1, 2, 3)])
    x_other = moved(x_half, "tp", 1)
    x_here = jnp.where(t == 0, jnp.concatenate([x_half, x_other], 2), jnp.concatenate([x_other, x_half], 2))
    m_far = moved(jnp.where(c == 0, *cuts), "tp", 1)
    kpos = after(kpos, *x_pieces)

    sts = run_stats(kvs, qgs, kpos, qpos)
    sts = [sts[0]] + [moved(sts[o], "y", -o) for o in (1, 2, 3)]
    dkv_near, dkv_sent, dqs = run_grads(kvs, qgs, kpos, qpos, sts)

    def total_of(own, arrived):
        total = own.astype(F32)
        for a in arrived:
            total = total + a.astype(F32)
        return total.astype(BF)

    first = moved(dkv_sent[0], "z", 1)
    row1, row2 = (total_of(dkv_near[o], [first[o - 1]]) for o in (1, 2))
    last = moved(dkv_sent[1], "z", 1)
    near = after(dkv_near, row1)
    row3, row0 = (total_of(near[o], [last[n]]) for n, o in enumerate((3, 0)))
    dq = total_of(dqs[0], [moved(dqs[o], "y", o) for o in (1, 2, 3)])
    x_all = jnp.stack([x_here, moved(x_here, "c", 1)], axis=1)
    m_core = moved(m_far, "c", 1)
    k_far = jnp.where(c == 0, m_far, m_core)
    v_far = jnp.where(c == 0, m_core, m_far)

    dkv = total_of(row0, [moved(row, "x", o) for o, row in ((2, row2), (1, row1), (3, row3))])
    dkv_all = jnp.stack([dkv] + [moved(dkv, "x", -o) for o in (1, 2, 3)])
    dkv_far = moved(dkv[1], "c", 1)
    k_here = own_first(c, dkv[0, :, :HEAD], dkv_far[:, :HEAD], 1)
    v_here = own_first(c, dkv[0, :, HEAD:], dkv_far[:, HEAD:], 1)
    kv_here = jnp.concatenate([k_here, v_here], 1)
    kv_there = moved(kv_here, "tp", 1)

    query_grad = own_first(c, dq[0], moved(dq[1], "c", 1), 1)

    tokens = 8 * TOK
    weight = lax.dot_general(
        x_all.reshape(tokens, 8 * HEAD),
        dkv_all.reshape(tokens, 2 * HEAD),
        (((0,), (0,)), ((), ())),
        preferred_element_type=F32,
    )
    pieces = weight.astype(BF).reshape(16, HEAD // 2, 2 * HEAD)
    got = lax.all_to_all(pieces, ("y", "z", "c"), 0, 0, tiled=True)
    key_weight, value_weight = run_finish(got)

    km = lax.dynamic_slice_in_dim(key_matrix, t * half, half, 0)
    vm = lax.dynamic_slice_in_dim(value_matrix, t * half, half, 0)
    wide = 2 * HEAD
    total = nt(kv_here[:, :wide], km) + nt(kv_here[:, wide:], vm)
    input_grad = (total + nt(kv_there[:, :wide], k_far) + nt(kv_there[:, wide:], v_far)).astype(BF)
    return (query_grad, input_grad, key_weight, value_weight)


def solution(mesh):
    torus = Mesh(mesh.devices.reshape(4, 2, 4, 2, mesh.shape["tp"]), ("y", "z", "x", "c", "tp"))
    return jax.shard_map(
        step,
        mesh=torus,
        in_specs=(P(SEQ, "tp"),) * 5 + (P(None, "tp"),) * 2 + (P(),),
        out_specs=(P(SEQ, "tp"),) * 4,
        check_vma=False,
    )
```

```python
import math

import jax
import jax.numpy as jnp
from jax import lax
from jax.experimental import pallas as pl
from jax.experimental.pallas import tpu as pltpu
from jax.sharding import Mesh
from jax.sharding import PartitionSpec as P


HEAD = 128
WINDOW = 4096
GROUP = 4
TOK = 128
SEQ = ("y", "z", "x", "c")
BF = jnp.bfloat16
F32 = jnp.float32
NEG = -1e30

PARTS = 8
T = TOK // PARTS
KSLOTS = 16
QSLOTS = 8
KR = KSLOTS * T
QR = QSLOTS * GROUP * T
SPAN = PARTS // 2
SCALE = 1.0 / math.sqrt(HEAD)
SCORE2 = SCALE * math.log2(math.e)
VMEM_LIMIT = 60 * 1024 * 1024


def moved(array, axis, by):
    n = lax.axis_size(axis)
    return lax.ppermute(array, axis, [(i, (i + by) % n) for i in range(n)])


def nt(a, b):
    return lax.dot_general(a, b, (((1,), (1,)), ((), ())), preferred_element_type=F32)


def nn(a, b):
    return lax.dot_general(a, b, (((1,), (0,)), ((), ())), preferred_element_type=F32)


def part_copies(part, kv_refs, qg_refs, kv, qg, sem):
    tok = pl.ds(part * T, T)
    for b in range(4):
        yield pltpu.make_async_copy(kv_refs[b].at[:, :, tok, :], kv.at[part, b], sem.at[part, b])
    for s in range(4):
        yield pltpu.make_async_copy(qg_refs[s].at[:, tok, :], qg.at[part, s], sem.at[part, 4 + s])


def start_loads(kv_refs, qg_refs, kpos_ref, kv, qg, kposb, sem):
    for part in range(PARTS):
        for copy in part_copies(part, kv_refs, qg_refs, kv, qg, sem):
            copy.start()
    for slot in range(KSLOTS):
        column = jnp.broadcast_to(kpos_ref[slot : slot + 1, :], (TOK, 128)).T
        for part in range(PARTS):
            kposb[part, slot * T : (slot + 1) * T, :] = column[part * T : (part + 1) * T, :]


def lanes(first, count):
    return pl.ds(pl.multiple_of(first * KR, 128), count * KR)


def keys_of(kv, first, count):
    return kv[pl.ds(first, count), :, :, :, :, :HEAD].reshape(count * KR, HEAD)


def values_of(kv, first, count):
    return kv[pl.ds(first, count), :, :, :, :, HEAD:].reshape(count * KR, HEAD)


def heads_of(qg, i, first):
    cols = [(first + h) * HEAD for h in range(GROUP)]
    return jnp.concatenate([qg[i, :, :, :, c : c + HEAD].reshape(QSLOTS * T, HEAD) for c in cols], axis=0)


def masked_scores(i, count, k, q, kposb, qpos_ref):
    s = nt(k, q) * SCORE2
    pieces = [s[n * KR : (n + 1) * KR] for n in range(count)]
    qp = qpos_ref[i]
    kp = jnp.concatenate([kposb[i]] * (QR // 128), axis=1)
    pieces[-1] = jnp.where(kp <= qp, pieces[-1], NEG)
    if count == SPAN + 1:
        kp = jnp.concatenate([kposb[i - SPAN]] * (QR // 128), axis=1)
        pieces[0] = jnp.where(kp > qp - float(WINDOW), pieces[0], NEG)
    return jnp.concatenate(pieces, axis=0)


def over_parts(body):
    for i in range(SPAN):
        body(i, i + 1)

    def full(i, carry):
        body(i, SPAN + 1)
        return carry

    lax.fori_loop(SPAN, PARTS, full, 0)


def stats_kernel(*refs):
    kv_refs, qg_refs = refs[0:4], refs[4:8]
    kpos_ref, qpos_ref = refs[8:10]
    out_refs = refs[10:14]
    kv, qg, kposb, ms, sem = refs[14:]
    start_loads(kv_refs, qg_refs, kpos_ref, kv, qg, kposb, sem)

    def body(i, count):
        for copy in part_copies(i, kv_refs, qg_refs, kv, qg, sem):
            copy.wait()
        first, rows = i - count + 1, count * KR
        s = masked_scores(i, count, keys_of(kv, first, count), heads_of(qg, i, 0), kposb, qpos_ref)
        dp = nt(values_of(kv, first, count), heads_of(qg, i, GROUP)).reshape(rows // 8, 8, QR)
        s = s.reshape(rows // 8, 8, QR)
        top = jnp.max(jnp.max(s, axis=0), axis=0, keepdims=True)
        e = jnp.exp2(s - top[None])
        total = jnp.sum(jnp.sum(e, axis=0), axis=0, keepdims=True)
        weighted = jnp.sum(jnp.sum(e * dp, axis=0), axis=0, keepdims=True)
        ms[i] = jnp.concatenate([top, total, weighted, jnp.zeros((5, QR), F32)], axis=0)

    over_parts(body)
    rows = [ms[i][0:4] for i in range(PARTS)]
    stats = jnp.concatenate(rows, axis=0)
    per_head = QSLOTS * T
    for o in range(4):
        for h in range(GROUP):
            cols = slice(h * per_head, (h + 1) * per_head)
            piece = stats[:, cols]
            out_refs[o][:, cols] = pltpu.roll(piece, o * 2 * T, 1) if o else piece


def grads_kernel(*refs):
    kv_refs, qg_refs = refs[0:4], refs[4:8]
    kpos_ref, qpos_ref = refs[8:10]
    st_refs = refs[10:14]
    dkv_near, dkv_first, dkv_last, dq_refs = refs[14], refs[15], refs[16], refs[17:21]
    kv, qg, kposb, kt, dks, dvs, dqt, lse, mean, dkv_out, dq_wide, dq_out, sem, out_sem = refs[21:]
    start_loads(kv_refs, qg_refs, kpos_ref, kv, qg, kposb, sem)
    for part in range(PARTS):
        st = [r[part * 4 : part * 4 + 3, :] for r in st_refs]
        top = jnp.maximum(jnp.maximum(st[0][0:1], st[1][0:1]), jnp.maximum(st[2][0:1], st[3][0:1]))
        fade = [jnp.exp2(a[0:1] - top) for a in st]
        total = sum(a[1:2] * f for a, f in zip(st, fade))
        lse[part] = top + jnp.log2(total)
        mean[part] = sum(a[2:3] * f for a, f in zip(st, fade)) / total

    def dkv_copies(part):
        tok = slice(part * T, (part + 1) * T)
        pairs = (
            (dkv_out.at[part, 0], dkv_near.at[:, :, tok, :]),
            (dkv_out.at[part, 1, 1:3], dkv_first.at[:, :, tok, :]),
            (dkv_out.at[part, 1, 3], dkv_last.at[0, :, tok, :]),
            (dkv_out.at[part, 1, 0], dkv_last.at[1, :, tok, :]),
        )
        return [pltpu.make_async_copy(a, b, out_sem.at[part, n]) for n, (a, b) in enumerate(pairs)]

    def dq_copies(part):
        tok = slice(part * T, (part + 1) * T)
        pairs = [(dq_wide.at[part], dq_refs[0].at[:, tok, :])]
        pairs += [(dq_out.at[part, s - 1], dq_refs[s].at[:, tok, :]) for s in (1, 2, 3)]
        return [pltpu.make_async_copy(a, b, out_sem.at[part, 4 + n]) for n, (a, b) in enumerate(pairs)]

    def emit_dkv(part):
        dk = (dks[part] * SCALE).astype(BF).reshape(4, 2, 2, T, HEAD)
        dv = dvs[part].astype(BF).reshape(4, 2, 2, T, HEAD)
        for a in range(2):
            dkv_out[part, a, :, :, :, :HEAD] = dk[:, a]
            dkv_out[part, a, :, :, :, HEAD:] = dv[:, a]
        for copy in dkv_copies(part):
            copy.start()

    def emit_dq(part):
        dq = dqt[part].T * SCALE
        for h in range(GROUP):
            cols = slice(h * HEAD, (h + 1) * HEAD)
            rows = dq[h * QSLOTS * T : (h + 1) * QSLOTS * T, :].reshape(4, 2, T, HEAD)
            dq_wide[part, :, :, cols] = rows[0]
            dq_out[part, :, :, :, cols] = rows[1:4].astype(BF)
        for copy in dq_copies(part):
            copy.start()

    def body(i, count):
        for copy in part_copies(i, kv_refs, qg_refs, kv, qg, sem):
            copy.wait()
        first = i - count + 1
        k, q, g = keys_of(kv, first, count), heads_of(qg, i, 0), heads_of(qg, i, GROUP)
        kt[:, lanes(i, 1)] = keys_of(kv, i, 1).T
        p = jnp.exp2(masked_scores(i, count, k, q, kposb, qpos_ref) - lse[i])
        ds = (p * (nt(values_of(kv, first, count), g) - mean[i])).astype(BF)
        p = p.astype(BF)
        dk, dv = nn(ds, q), nn(p, g)
        dqt[i] = nn(kt[:, lanes(first, count)], ds)
        for n in range(count - 1):
            dks[first + n] += dk[n * KR : (n + 1) * KR]
            dvs[first + n] += dv[n * KR : (n + 1) * KR]
        dks[i], dvs[i] = dk[(count - 1) * KR :], dv[(count - 1) * KR :]

    over_parts(body)
    for part in range(PARTS):
        emit_dkv(part)
        emit_dq(part)
    for part in range(PARTS):
        for copy in dkv_copies(part) + dq_copies(part):
            copy.wait()


def common_scratch():
    return [
        pltpu.VMEM((PARTS, 4, 2, 2, T, 2 * HEAD), BF),
        pltpu.VMEM((PARTS, 4, 2, T, 2 * GROUP * HEAD), BF),
        pltpu.VMEM((PARTS, KR, 128), F32),
    ]


def in_places(small):
    return [pl.BlockSpec(memory_space=pl.ANY)] * 8 + [pl.BlockSpec(memory_space=pltpu.VMEM)] * small


def run_stats(kvs, qgs, kpos, qpos):
    return pl.pallas_call(
        stats_kernel,
        out_shape=[jax.ShapeDtypeStruct((PARTS * 4, QR), F32)] * 4,
        in_specs=in_places(2),
        scratch_shapes=common_scratch()
        + [pltpu.VMEM((PARTS, 8, QR), F32)]
        + [pltpu.SemaphoreType.DMA((PARTS, 8))],
        compiler_params=pltpu.CompilerParams(vmem_limit_bytes=VMEM_LIMIT),
        cost_estimate=pl.CostEstimate(flops=6_000_000_000, bytes_accessed=3_000_000, transcendentals=5_000_000),
        name="stats",
    )(*kvs, *qgs, kpos, qpos)


def run_grads(kvs, qgs, kpos, qpos, sts):
    dkv = [jax.ShapeDtypeStruct((n, 2, TOK, 2 * HEAD), BF) for n in (4, 2, 2)]
    dq = [jax.ShapeDtypeStruct((2, TOK, GROUP * HEAD), F32 if s == 0 else BF) for s in range(4)]
    out = pl.pallas_call(
        grads_kernel,
        out_shape=dkv + dq,
        in_specs=in_places(6),
        out_specs=[pl.BlockSpec(memory_space=pl.ANY)] * 7,
        scratch_shapes=common_scratch()
        + [
            pltpu.VMEM((HEAD, PARTS * KR), BF),
            pltpu.VMEM((PARTS, KR, HEAD), F32),
            pltpu.VMEM((PARTS, KR, HEAD), F32),
            pltpu.VMEM((PARTS, HEAD, QR), F32),
            pltpu.VMEM((PARTS, 1, QR), F32),
            pltpu.VMEM((PARTS, 1, QR), F32),
            pltpu.VMEM((PARTS, 2, 4, 2, T, 2 * HEAD), BF),
            pltpu.VMEM((PARTS, 2, T, GROUP * HEAD), F32),
            pltpu.VMEM((PARTS, 3, 2, T, GROUP * HEAD), BF),
            pltpu.SemaphoreType.DMA((PARTS, 8)),
            pltpu.SemaphoreType.DMA((PARTS, 8)),
        ],
        compiler_params=pltpu.CompilerParams(vmem_limit_bytes=VMEM_LIMIT),
        cost_estimate=pl.CostEstimate(flops=12_000_000_000, bytes_accessed=6_000_000, transcendentals=5_000_000),
        name="grads",
    )(*kvs, *qgs, kpos, qpos, *sts)
    return out[0], out[1:3], out[3:7]


def pack_kernel(q_ref, g_ref, k_ref, v_ref, kv_own, qg_own, kv_send, qg_send):
    wide = GROUP * HEAD
    mine = lax.axis_index("c")
    for which, kv, qg in ((mine, kv_own.at[0], qg_own.at[0]), (1 - mine, kv_send, qg_send)):
        cols = pl.ds(pl.multiple_of(which * wide, 128), wide)
        small = pl.ds(pl.multiple_of(which * HEAD, 128), HEAD)
        kv[:, :HEAD] = k_ref[:, small]
        kv[:, HEAD:] = v_ref[:, small]
        qg[:, :wide] = q_ref[:, cols]
        qg[:, wide:] = g_ref[:, cols]
    kv_own[1] = kv_send[...]
    qg_own[1] = qg_send[...]


def run_pack(q, g, k, v):
    kv, qg = (TOK, 2 * HEAD), (TOK, 2 * GROUP * HEAD)
    vmem = pl.BlockSpec(memory_space=pltpu.VMEM)
    return pl.pallas_call(
        pack_kernel,
        out_shape=[jax.ShapeDtypeStruct(a, BF) for a in ((2, *kv), (2, *qg), kv, qg)],
        in_specs=[vmem] * 4,
        name="pack",
    )(q, g, k, v)


def columns_kernel(mine_ref, far_ref, *out_refs):
    x, t = lax.axis_index("x"), lax.axis_index("tp")
    for ref, half in ((mine_ref, t), (far_ref, 1 - t)):
        for o in range(4):
            target = (x + o) % 4
            for n in range(4):
                src = pl.ds(pl.multiple_of(n * 4 * HEAD + target * HEAD, 128), HEAD)
                dst = pl.ds(pl.multiple_of(half * 4 * HEAD + n * HEAD, 128), HEAD)
                out_refs[o][:, dst] = ref[:, src]


def run_columns(mine, far):
    return pl.pallas_call(
        columns_kernel,
        out_shape=[jax.ShapeDtypeStruct((TOK, 8 * HEAD), BF)] * 4,
        in_specs=[pl.BlockSpec(memory_space=pltpu.VMEM)] * 2,
        name="columns",
    )(mine, far)


def finish_kernel(in_ref, k_ref, v_ref):
    for h in range(2):
        total = in_ref[h].astype(F32)
        for n in range(1, 8):
            total = total + in_ref[2 * n + h].astype(F32)
        k_ref[:, h * HEAD : (h + 1) * HEAD] = total[:, :HEAD]
        v_ref[:, h * HEAD : (h + 1) * HEAD] = total[:, HEAD:]


def run_finish(got):
    out = jax.ShapeDtypeStruct((HEAD // 2, 2 * HEAD), F32)
    return pl.pallas_call(finish_kernel, out_shape=[out, out], name="finish")(got)


def positions(run_placement, y, z, x, c):
    def device(yy, zz, xx, cc):
        return (((yy % 4) * 2 + zz % 2) * 4 + xx % 4) * 2 + cc % 2

    b, a, e = jnp.meshgrid(jnp.arange(4), jnp.arange(2), jnp.arange(2), indexing="ij")
    keys = device(y, z + a, x + b, c + e).reshape(KSLOTS)
    a, e = jnp.meshgrid(jnp.arange(4), jnp.arange(2), indexing="ij")
    queries = device(y + a, z, x, c + e).reshape(QSLOTS)
    index = jnp.concatenate([keys, queries]).astype(jnp.int32)
    pick = (index[:, None] == jnp.arange(64, dtype=jnp.int32)[None, :]).astype(BF)
    slots = nt(pick, run_placement.astype(BF)).astype(BF)
    lane = jnp.arange(TOK, dtype=jnp.int32)
    spread = jnp.where(lane[None, :] // 2 == jnp.arange(64, dtype=jnp.int32)[:, None], 2.0, 0.0).astype(BF)
    pos = nn(slots, spread) + ((lane // 2) * TOK + lane % 2).astype(F32)[None, :]
    kpos = pos[:KSLOTS]
    qpos = pos[KSLOTS:].reshape(QSLOTS, PARTS, T).transpose(1, 0, 2).reshape(PARTS, 1, 1, QSLOTS * T)
    qpos = jnp.broadcast_to(qpos, (PARTS, 1, GROUP, QSLOTS * T)).reshape(PARTS, 1, QR)
    return kpos, qpos


def own_first(c, mine, other, axis):
    return jnp.where(c == 0, jnp.concatenate([mine, other], axis), jnp.concatenate([other, mine], axis))


def after(array, *gates):
    return lax.optimization_barrier((array, *gates))[0]


def step(query_rows, key_rows, value_rows, output_grad, layer_input, key_matrix, value_matrix, run_placement):
    y, z, x, c, t = (lax.axis_index(a) for a in ("y", "z", "x", "c", "tp"))
    x_far = moved(layer_input, "tp", 1)
    kv_pair, qg_pair, kv_send, qg_send = run_pack(query_rows, output_grad, key_rows, value_rows)
    qg_own = qg_pair.at[1].set(moved(qg_send, "c", 1))
    kv_own = kv_pair.at[1].set(moved(kv_send, "c", 1))
    qgs = [qg_own] + [moved(qg_own, "y", -o) for o in (1, 2, 3)]
    kv_both = jnp.stack([kv_own, moved(kv_own, "z", 1)])
    kvs = [kv_both] + [moved(kv_both, "x", -o) for o in (1, 2, 3)]
    kpos, qpos = positions(run_placement, y, z, x, c)

    half = key_matrix.shape[0] // 2
    cuts = [lax.dynamic_slice_in_dim(after(m, kv_both), (1 - t) * half, half, 0) for m in (key_matrix, value_matrix)]
    x_pieces = run_columns(layer_input, x_far)
    m_far = moved(jnp.where(c == 0, *cuts), "tp", 1)

    sts = run_stats(kvs, qgs, kpos, qpos)
    sts = [sts[0]] + [moved(sts[o], "y", -o) for o in (1, 2, 3)]
    x_here = jnp.stack([x_pieces[0]] + [moved(x_pieces[4 - o], "x", -o) for o in (1, 2, 3)])
    dkv_near, dkv_sent, dqs = run_grads(kvs, qgs, kpos, qpos, sts)

    def total_of(own, arrived):
        total = own.astype(F32)
        for a in arrived:
            total = total + a.astype(F32)
        return total.astype(BF)

    first = moved(dkv_sent[0], "z", 1)
    row1, row2 = (total_of(dkv_near[o], [first[o - 1]]) for o in (1, 2))
    last = moved(dkv_sent[1], "z", 1)
    near = after(dkv_near, row1)
    row3, row0 = (total_of(near[o], [last[n]]) for n, o in enumerate((3, 0)))
    dq = total_of(dqs[0], [moved(dqs[o], "y", o) for o in (1, 2, 3)])
    x_all = jnp.stack([x_here, moved(x_here, "c", 1)], axis=1)
    m_core = moved(m_far, "c", 1)
    k_far = jnp.where(c == 0, m_far, m_core)
    v_far = jnp.where(c == 0, m_core, m_far)

    dkv = total_of(row0, [moved(row, "x", o) for o, row in ((2, row2), (1, row1), (3, row3))])
    dkv_all = jnp.stack([dkv] + [moved(dkv, "x", -o) for o in (1, 2, 3)])
    dkv_far = moved(dkv[1], "c", 1)
    k_here = own_first(c, dkv[0, :, :HEAD], dkv_far[:, :HEAD], 1)
    v_here = own_first(c, dkv[0, :, HEAD:], dkv_far[:, HEAD:], 1)
    kv_here = jnp.concatenate([k_here, v_here], 1)
    kv_there = moved(kv_here, "tp", 1)

    query_grad = own_first(c, dq[0], moved(dq[1], "c", 1), 1)

    tokens = 8 * TOK
    weight = lax.dot_general(
        x_all.reshape(tokens, 8 * HEAD),
        dkv_all.reshape(tokens, 2 * HEAD),
        (((0,), (0,)), ((), ())),
        preferred_element_type=F32,
    )
    pieces = weight.astype(BF).reshape(16, HEAD // 2, 2 * HEAD)
    got = lax.all_to_all(pieces, ("y", "z", "c"), 0, 0, tiled=True)
    key_weight, value_weight = run_finish(got)

    km = lax.dynamic_slice_in_dim(key_matrix, t * half, half, 0)
    vm = lax.dynamic_slice_in_dim(value_matrix, t * half, half, 0)
    wide = 2 * HEAD
    total = nt(kv_here[:, :wide], km) + nt(kv_here[:, wide:], vm)
    input_grad = (total + nt(kv_there[:, :wide], k_far) + nt(kv_there[:, wide:], v_far)).astype(BF)
    return (query_grad, input_grad, key_weight, value_weight)


def solution(mesh):
    torus = Mesh(mesh.devices.reshape(4, 2, 4, 2, mesh.shape["tp"]), ("y", "z", "x", "c", "tp"))
    return jax.shard_map(
        step,
        mesh=torus,
        in_specs=(P(SEQ, "tp"),) * 5 + (P(None, "tp"),) * 2 + (P(),),
        out_specs=(P(SEQ, "tp"),) * 4,
        check_vma=False,
    )
```

```python
import math

import jax
import jax.numpy as jnp
from jax import lax
from jax.experimental import pallas as pl
from jax.experimental.pallas import tpu as pltpu
from jax.sharding import Mesh
from jax.sharding import PartitionSpec as P


HEAD = 128
WINDOW = 4096
GROUP = 4
TOK = 128
SEQ = ("y", "z", "x", "c")
BF = jnp.bfloat16
F32 = jnp.float32
NEG = -1e30

PARTS = 8
T = TOK // PARTS
KSLOTS = 16
QSLOTS = 8
KR = KSLOTS * T
QR = QSLOTS * GROUP * T
SPAN = PARTS // 2
SCALE = 1.0 / math.sqrt(HEAD)
SCORE2 = SCALE * math.log2(math.e)
VMEM_LIMIT = 60 * 1024 * 1024


def moved(array, axis, by):
    n = lax.axis_size(axis)
    return lax.ppermute(array, axis, [(i, (i + by) % n) for i in range(n)])


def nt(a, b):
    return lax.dot_general(a, b, (((1,), (1,)), ((), ())), preferred_element_type=F32)


def nn(a, b):
    return lax.dot_general(a, b, (((1,), (0,)), ((), ())), preferred_element_type=F32)


def part_copies(part, kv_refs, qg_refs, kv, qg, sem):
    tok = pl.ds(part * T, T)
    for b in range(4):
        yield pltpu.make_async_copy(kv_refs[b].at[:, :, tok, :], kv.at[part, b], sem.at[part, b])
    for s in range(4):
        yield pltpu.make_async_copy(qg_refs[s].at[:, tok, :], qg.at[part, s], sem.at[part, 4 + s])


def start_loads(kv_refs, qg_refs, kpos_ref, kv, qg, kposb, sem):
    for part in range(PARTS):
        for copy in part_copies(part, kv_refs, qg_refs, kv, qg, sem):
            copy.start()
    for slot in range(KSLOTS):
        column = jnp.broadcast_to(kpos_ref[slot : slot + 1, :], (TOK, 128)).T
        for part in range(PARTS):
            kposb[part, slot * T : (slot + 1) * T, :] = column[part * T : (part + 1) * T, :]


def lanes(first, count):
    return pl.ds(pl.multiple_of(first * KR, 128), count * KR)


def keys_of(kv, first, count):
    return kv[pl.ds(first, count), :, :, :, :, :HEAD].reshape(count * KR, HEAD)


def values_of(kv, first, count):
    return kv[pl.ds(first, count), :, :, :, :, HEAD:].reshape(count * KR, HEAD)


def heads_of(qg, i, first):
    cols = [(first + h) * HEAD for h in range(GROUP)]
    return jnp.concatenate([qg[i, :, :, :, c : c + HEAD].reshape(QSLOTS * T, HEAD) for c in cols], axis=0)


def masked_scores(i, count, k, q, kposb, qpos_ref):
    s = nt(k, q) * SCORE2
    pieces = [s[n * KR : (n + 1) * KR] for n in range(count)]
    qp = qpos_ref[i]
    kp = jnp.concatenate([kposb[i]] * (QR // 128), axis=1)
    pieces[-1] = jnp.where(kp <= qp, pieces[-1], NEG)
    if count == SPAN + 1:
        kp = jnp.concatenate([kposb[i - SPAN]] * (QR // 128), axis=1)
        pieces[0] = jnp.where(kp > qp - float(WINDOW), pieces[0], NEG)
    return jnp.concatenate(pieces, axis=0)


def over_parts(body):
    for i in range(SPAN):
        body(i, i + 1)

    def full(i, carry):
        body(i, SPAN + 1)
        return carry

    lax.fori_loop(SPAN, PARTS, full, 0)


def stats_kernel(*refs):
    kv_refs, qg_refs = refs[0:4], refs[4:8]
    kpos_ref, qpos_ref = refs[8:10]
    out_refs = refs[10:14]
    kv, qg, kposb, ms, sem = refs[14:]
    start_loads(kv_refs, qg_refs, kpos_ref, kv, qg, kposb, sem)

    def body(i, count):
        for copy in part_copies(i, kv_refs, qg_refs, kv, qg, sem):
            copy.wait()
        first, rows = i - count + 1, count * KR
        s = masked_scores(i, count, keys_of(kv, first, count), heads_of(qg, i, 0), kposb, qpos_ref)
        dp = nt(values_of(kv, first, count), heads_of(qg, i, GROUP)).reshape(rows // 8, 8, QR)
        s = s.reshape(rows // 8, 8, QR)
        top = jnp.max(jnp.max(s, axis=0), axis=0, keepdims=True)
        e = jnp.exp2(s - top[None])
        total = jnp.sum(jnp.sum(e, axis=0), axis=0, keepdims=True)
        weighted = jnp.sum(jnp.sum(e * dp, axis=0), axis=0, keepdims=True)
        ms[i] = jnp.concatenate([top, total, weighted, jnp.zeros((5, QR), F32)], axis=0)

    over_parts(body)
    rows = [ms[i][0:4] for i in range(PARTS)]
    stats = jnp.concatenate(rows, axis=0)
    per_head = QSLOTS * T
    for o in range(4):
        for h in range(GROUP):
            cols = slice(h * per_head, (h + 1) * per_head)
            piece = stats[:, cols]
            out_refs[o][:, cols] = pltpu.roll(piece, o * 2 * T, 1) if o else piece


def grads_kernel(*refs):
    kv_refs, qg_refs = refs[0:4], refs[4:8]
    kpos_ref, qpos_ref = refs[8:10]
    st_refs = refs[10:14]
    dkv_near, dkv_first, dkv_last, dq_refs = refs[14], refs[15], refs[16], refs[17:21]
    kv, qg, kposb, kt, dks, dvs, dqt, lse, mean, dkv_out, dq_wide, dq_out, sem, out_sem = refs[21:]
    start_loads(kv_refs, qg_refs, kpos_ref, kv, qg, kposb, sem)
    for part in range(PARTS):
        st = [r[part * 4 : part * 4 + 3, :] for r in st_refs]
        top = jnp.maximum(jnp.maximum(st[0][0:1], st[1][0:1]), jnp.maximum(st[2][0:1], st[3][0:1]))
        fade = [jnp.exp2(a[0:1] - top) for a in st]
        total = sum(a[1:2] * f for a, f in zip(st, fade))
        lse[part] = top + jnp.log2(total)
        mean[part] = sum(a[2:3] * f for a, f in zip(st, fade)) / total

    def dkv_copies(part):
        tok = slice(part * T, (part + 1) * T)
        pairs = (
            (dkv_out.at[part, 0], dkv_near.at[:, :, tok, :]),
            (dkv_out.at[part, 1, 1:3], dkv_first.at[:, :, tok, :]),
            (dkv_out.at[part, 1, 3], dkv_last.at[0, :, tok, :]),
            (dkv_out.at[part, 1, 0], dkv_last.at[1, :, tok, :]),
        )
        return [pltpu.make_async_copy(a, b, out_sem.at[part, n]) for n, (a, b) in enumerate(pairs)]

    def dq_copies(part):
        tok = slice(part * T, (part + 1) * T)
        pairs = [(dq_wide.at[part], dq_refs[0].at[:, tok, :])]
        pairs += [(dq_out.at[part, s - 1], dq_refs[s].at[:, tok, :]) for s in (1, 2, 3)]
        return [pltpu.make_async_copy(a, b, out_sem.at[part, 4 + n]) for n, (a, b) in enumerate(pairs)]

    def emit_dkv(part):
        dk = (dks[part] * SCALE).astype(BF).reshape(4, 2, 2, T, HEAD)
        dv = dvs[part].astype(BF).reshape(4, 2, 2, T, HEAD)
        for a in range(2):
            dkv_out[part, a, :, :, :, :HEAD] = dk[:, a]
            dkv_out[part, a, :, :, :, HEAD:] = dv[:, a]
        for copy in dkv_copies(part):
            copy.start()

    def emit_dq(part):
        dq = dqt[part].T * SCALE
        for h in range(GROUP):
            cols = slice(h * HEAD, (h + 1) * HEAD)
            rows = dq[h * QSLOTS * T : (h + 1) * QSLOTS * T, :].reshape(4, 2, T, HEAD)
            dq_wide[part, :, :, cols] = rows[0]
            dq_out[part, :, :, :, cols] = rows[1:4].astype(BF)
        for copy in dq_copies(part):
            copy.start()

    def body(i, count):
        for copy in part_copies(i, kv_refs, qg_refs, kv, qg, sem):
            copy.wait()
        first = i - count + 1
        k, q, g = keys_of(kv, first, count), heads_of(qg, i, 0), heads_of(qg, i, GROUP)
        kt[:, lanes(i, 1)] = keys_of(kv, i, 1).T
        p = jnp.exp2(masked_scores(i, count, k, q, kposb, qpos_ref) - lse[i])
        ds = (p * (nt(values_of(kv, first, count), g) - mean[i])).astype(BF)
        p = p.astype(BF)
        dk, dv = nn(ds, q), nn(p, g)
        dqt[i] = nn(kt[:, lanes(first, count)], ds)
        for n in range(count - 1):
            dks[first + n] += dk[n * KR : (n + 1) * KR]
            dvs[first + n] += dv[n * KR : (n + 1) * KR]
        dks[i], dvs[i] = dk[(count - 1) * KR :], dv[(count - 1) * KR :]

    over_parts(body)
    for part in range(PARTS):
        emit_dkv(part)
        emit_dq(part)
    for part in range(PARTS):
        for copy in dkv_copies(part) + dq_copies(part):
            copy.wait()


def common_scratch():
    return [
        pltpu.VMEM((PARTS, 4, 2, 2, T, 2 * HEAD), BF),
        pltpu.VMEM((PARTS, 4, 2, T, 2 * GROUP * HEAD), BF),
        pltpu.VMEM((PARTS, KR, 128), F32),
    ]


def in_places(small):
    return [pl.BlockSpec(memory_space=pl.ANY)] * 8 + [pl.BlockSpec(memory_space=pltpu.VMEM)] * small


def run_stats(kvs, qgs, kpos, qpos):
    return pl.pallas_call(
        stats_kernel,
        out_shape=[jax.ShapeDtypeStruct((PARTS * 4, QR), F32)] * 4,
        in_specs=in_places(2),
        scratch_shapes=common_scratch()
        + [pltpu.VMEM((PARTS, 8, QR), F32)]
        + [pltpu.SemaphoreType.DMA((PARTS, 8))],
        compiler_params=pltpu.CompilerParams(vmem_limit_bytes=VMEM_LIMIT),
        cost_estimate=pl.CostEstimate(flops=6_000_000_000, bytes_accessed=3_000_000, transcendentals=5_000_000),
        name="stats",
    )(*kvs, *qgs, kpos, qpos)


def run_grads(kvs, qgs, kpos, qpos, sts):
    dkv = [jax.ShapeDtypeStruct((n, 2, TOK, 2 * HEAD), BF) for n in (4, 2, 2)]
    dq = [jax.ShapeDtypeStruct((2, TOK, GROUP * HEAD), F32 if s == 0 else BF) for s in range(4)]
    out = pl.pallas_call(
        grads_kernel,
        out_shape=dkv + dq,
        in_specs=in_places(6),
        out_specs=[pl.BlockSpec(memory_space=pl.ANY)] * 7,
        scratch_shapes=common_scratch()
        + [
            pltpu.VMEM((HEAD, PARTS * KR), BF),
            pltpu.VMEM((PARTS, KR, HEAD), F32),
            pltpu.VMEM((PARTS, KR, HEAD), F32),
            pltpu.VMEM((PARTS, HEAD, QR), F32),
            pltpu.VMEM((PARTS, 1, QR), F32),
            pltpu.VMEM((PARTS, 1, QR), F32),
            pltpu.VMEM((PARTS, 2, 4, 2, T, 2 * HEAD), BF),
            pltpu.VMEM((PARTS, 2, T, GROUP * HEAD), F32),
            pltpu.VMEM((PARTS, 3, 2, T, GROUP * HEAD), BF),
            pltpu.SemaphoreType.DMA((PARTS, 8)),
            pltpu.SemaphoreType.DMA((PARTS, 8)),
        ],
        compiler_params=pltpu.CompilerParams(vmem_limit_bytes=VMEM_LIMIT),
        cost_estimate=pl.CostEstimate(flops=12_000_000_000, bytes_accessed=6_000_000, transcendentals=5_000_000),
        name="grads",
    )(*kvs, *qgs, kpos, qpos, *sts)
    return out[0], out[1:3], out[3:7]


def pack_kernel(q_ref, g_ref, k_ref, v_ref, kv_own, qg_own, kv_send, qg_send):
    wide = GROUP * HEAD
    mine = lax.axis_index("c")
    for which, kv, qg in ((mine, kv_own.at[0], qg_own.at[0]), (1 - mine, kv_send, qg_send)):
        cols = pl.ds(pl.multiple_of(which * wide, 128), wide)
        small = pl.ds(pl.multiple_of(which * HEAD, 128), HEAD)
        kv[:, :HEAD] = k_ref[:, small]
        kv[:, HEAD:] = v_ref[:, small]
        qg[:, :wide] = q_ref[:, cols]
        qg[:, wide:] = g_ref[:, cols]
    kv_own[1] = kv_send[...]
    qg_own[1] = qg_send[...]


def run_pack(q, g, k, v):
    kv, qg = (TOK, 2 * HEAD), (TOK, 2 * GROUP * HEAD)
    vmem = pl.BlockSpec(memory_space=pltpu.VMEM)
    return pl.pallas_call(
        pack_kernel,
        out_shape=[jax.ShapeDtypeStruct(a, BF) for a in ((2, *kv), (2, *qg), kv, qg)],
        in_specs=[vmem] * 4,
        name="pack",
    )(q, g, k, v)


def columns_kernel(in_ref, *out_refs):
    x = lax.axis_index("x")
    for o in range(4):
        target = (x + o) % 4
        for n in range(4):
            src = pl.ds(pl.multiple_of(n * 4 * HEAD + target * HEAD, 128), HEAD)
            out_refs[o][:, n * HEAD : (n + 1) * HEAD] = in_ref[:, src]


def run_columns(layer_input):
    return pl.pallas_call(
        columns_kernel,
        out_shape=[jax.ShapeDtypeStruct((TOK, 4 * HEAD), BF)] * 4,
        in_specs=[pl.BlockSpec(memory_space=pltpu.VMEM)],
        name="columns",
    )(layer_input)


def finish_kernel(in_ref, k_ref, v_ref):
    for h in range(2):
        total = in_ref[h].astype(F32)
        for n in range(1, 8):
            total = total + in_ref[2 * n + h].astype(F32)
        k_ref[:, h * HEAD : (h + 1) * HEAD] = total[:, :HEAD]
        v_ref[:, h * HEAD : (h + 1) * HEAD] = total[:, HEAD:]


def run_finish(got):
    out = jax.ShapeDtypeStruct((HEAD // 2, 2 * HEAD), F32)
    return pl.pallas_call(finish_kernel, out_shape=[out, out], name="finish")(got)


def positions(run_placement, y, z, x, c):
    def device(yy, zz, xx, cc):
        return (((yy % 4) * 2 + zz % 2) * 4 + xx % 4) * 2 + cc % 2

    b, a, e = jnp.meshgrid(jnp.arange(4), jnp.arange(2), jnp.arange(2), indexing="ij")
    keys = device(y, z + a, x + b, c + e).reshape(KSLOTS)
    a, e = jnp.meshgrid(jnp.arange(4), jnp.arange(2), indexing="ij")
    queries = device(y + a, z, x, c + e).reshape(QSLOTS)
    index = jnp.concatenate([keys, queries]).astype(jnp.int32)
    pick = (index[:, None] == jnp.arange(64, dtype=jnp.int32)[None, :]).astype(BF)
    slots = nt(pick, run_placement.astype(BF)).astype(BF)
    lane = jnp.arange(TOK, dtype=jnp.int32)
    spread = jnp.where(lane[None, :] // 2 == jnp.arange(64, dtype=jnp.int32)[:, None], 2.0, 0.0).astype(BF)
    pos = nn(slots, spread) + ((lane // 2) * TOK + lane % 2).astype(F32)[None, :]
    kpos = pos[:KSLOTS]
    qpos = pos[KSLOTS:].reshape(QSLOTS, PARTS, T).transpose(1, 0, 2).reshape(PARTS, 1, 1, QSLOTS * T)
    qpos = jnp.broadcast_to(qpos, (PARTS, 1, GROUP, QSLOTS * T)).reshape(PARTS, 1, QR)
    return kpos, qpos


def own_first(c, mine, other, axis):
    return jnp.where(c == 0, jnp.concatenate([mine, other], axis), jnp.concatenate([other, mine], axis))


def after(array, *gates):
    return lax.optimization_barrier((array, *gates))[0]


def step(query_rows, key_rows, value_rows, output_grad, layer_input, key_matrix, value_matrix, run_placement):
    y, z, x, c, t = (lax.axis_index(a) for a in ("y", "z", "x", "c", "tp"))
    kv_pair, qg_pair, kv_send, qg_send = run_pack(query_rows, output_grad, key_rows, value_rows)
    qg_own = qg_pair.at[1].set(moved(qg_send, "c", 1))
    kv_own = kv_pair.at[1].set(moved(kv_send, "c", 1))
    qgs = [qg_own] + [moved(qg_own, "y", -o) for o in (1, 2, 3)]
    kv_both = jnp.stack([kv_own, moved(kv_own, "z", 1)])
    kvs = [kv_both] + [moved(kv_both, "x", -o) for o in (1, 2, 3)]
    kpos, qpos = positions(run_placement, y, z, x, c)

    half = key_matrix.shape[0] // 2
    cuts = [lax.dynamic_slice_in_dim(after(m, kv_own), (1 - t) * half, half, 0) for m in (key_matrix, value_matrix)]
    x_pieces = run_columns(after(layer_input, kv_both, qpos))
    x_half = jnp.stack([x_pieces[0]] + [moved(x_pieces[4 - o], "x", -o) for o in (1, 2, 3)])
    x_other = moved(x_half, "tp", 1)
    x_here = jnp.where(t == 0, jnp.concatenate([x_half, x_other], 2), jnp.concatenate([x_other, x_half], 2))
    m_far = moved(jnp.where(c == 0, *cuts), "tp", 1)
    kpos = after(kpos, *x_pieces)

    sts = run_stats(kvs, qgs, kpos, qpos)
    sts = [sts[0]] + [moved(sts[o], "y", -o) for o in (1, 2, 3)]
    dkv_near, dkv_sent, dqs = run_grads(kvs, qgs, kpos, qpos, sts)

    def total_of(own, arrived):
        total = own.astype(F32)
        for a in arrived:
            total = total + a.astype(F32)
        return total.astype(BF)

    first = moved(dkv_sent[0], "z", 1)
    row1, row2 = (total_of(dkv_near[o], [first[o - 1]]) for o in (1, 2))
    last = moved(dkv_sent[1], "z", 1)
    near = after(dkv_near, row1)
    row3, row0 = (total_of(near[o], [last[n]]) for n, o in enumerate((3, 0)))
    dq = total_of(dqs[0], [moved(dqs[o], "y", o) for o in (1, 2, 3)])
    x_all = jnp.stack([x_here, moved(x_here, "c", 1)], axis=1)
    m_core = moved(m_far, "c", 1)
    k_far = jnp.where(c == 0, m_far, m_core)
    v_far = jnp.where(c == 0, m_core, m_far)

    got = [moved(row2, "x", 2), moved(row1, "x", 1)]
    dkv = total_of(row0, got + [moved(row3, "x", 3)])
    dkv_all = jnp.stack([dkv] + [moved(dkv, "x", -o) for o in (1, 2, 3)])
    dkv_far = moved(dkv[1], "c", 1)
    k_here = own_first(c, dkv[0, :, :HEAD], dkv_far[:, :HEAD], 1)
    v_here = own_first(c, dkv[0, :, HEAD:], dkv_far[:, HEAD:], 1)
    kv_here = jnp.concatenate([k_here, v_here], 1)
    kv_there = moved(kv_here, "tp", 1)

    query_grad = own_first(c, dq[0], moved(dq[1], "c", 1), 1)

    tokens = 8 * TOK
    weight = lax.dot_general(
        x_all.reshape(tokens, 8 * HEAD),
        dkv_all.reshape(tokens, 2 * HEAD),
        (((0,), (0,)), ((), ())),
        preferred_element_type=F32,
    )
    pieces = weight.astype(BF).reshape(16, HEAD // 2, 2 * HEAD)
    got = lax.all_to_all(pieces, ("y", "z", "c"), 0, 0, tiled=True)
    key_weight, value_weight = run_finish(got)

    km = lax.dynamic_slice_in_dim(key_matrix, t * half, half, 0)
    vm = lax.dynamic_slice_in_dim(value_matrix, t * half, half, 0)
    wide = 2 * HEAD
    total = nt(kv_here[:, :wide], km) + nt(kv_here[:, wide:], vm)
    input_grad = (total + nt(kv_there[:, :wide], k_far) + nt(kv_there[:, wide:], v_far)).astype(BF)
    return (query_grad, input_grad, key_weight, value_weight)


def solution(mesh):
    torus = Mesh(mesh.devices.reshape(4, 2, 4, 2, mesh.shape["tp"]), ("y", "z", "x", "c", "tp"))
    return jax.shard_map(
        step,
        mesh=torus,
        in_specs=(P(SEQ, "tp"),) * 5 + (P(None, "tp"),) * 2 + (P(),),
        out_specs=(P(SEQ, "tp"),) * 4,
        check_vma=False,
    )
```

```python
import math

import jax
import jax.numpy as jnp
from jax import lax
from jax.experimental import pallas as pl
from jax.experimental.pallas import tpu as pltpu
from jax.sharding import Mesh
from jax.sharding import PartitionSpec as P


HEAD = 128
WINDOW = 4096
GROUP = 4
TOK = 128
SEQ = ("y", "z", "x", "c")
BF = jnp.bfloat16
F32 = jnp.float32
NEG = -1e30

PARTS = 8
T = TOK // PARTS
KSLOTS = 16
QSLOTS = 8
KR = KSLOTS * T
QR = QSLOTS * GROUP * T
SPAN = PARTS // 2
SCALE = 1.0 / math.sqrt(HEAD)
SCORE2 = SCALE * math.log2(math.e)
VMEM_LIMIT = 60 * 1024 * 1024


def moved(array, axis, by):
    n = lax.axis_size(axis)
    return lax.ppermute(array, axis, [(i, (i + by) % n) for i in range(n)])


def nt(a, b):
    return lax.dot_general(a, b, (((1,), (1,)), ((), ())), preferred_element_type=F32)


def nn(a, b):
    return lax.dot_general(a, b, (((1,), (0,)), ((), ())), preferred_element_type=F32)


def part_copies(part, kv_refs, qg_refs, kv, qg, sem):
    tok = pl.ds(part * T, T)
    for b in range(4):
        yield pltpu.make_async_copy(kv_refs[b].at[:, :, tok, :], kv.at[part, b], sem.at[part, b])
    for s in range(4):
        yield pltpu.make_async_copy(qg_refs[s].at[:, tok, :], qg.at[part, s], sem.at[part, 4 + s])


def start_loads(kv_refs, qg_refs, kpos_ref, kv, qg, kposb, sem):
    for part in range(PARTS):
        for copy in part_copies(part, kv_refs, qg_refs, kv, qg, sem):
            copy.start()
    for slot in range(KSLOTS):
        column = jnp.broadcast_to(kpos_ref[slot : slot + 1, :], (TOK, 128)).T
        for part in range(PARTS):
            kposb[part, slot * T : (slot + 1) * T, :] = column[part * T : (part + 1) * T, :]


def lanes(first, count):
    return pl.ds(pl.multiple_of(first * KR, 128), count * KR)


def keys_of(kv, first, count):
    return kv[pl.ds(first, count), :, :, :, :, :HEAD].reshape(count * KR, HEAD)


def values_of(kv, first, count):
    return kv[pl.ds(first, count), :, :, :, :, HEAD:].reshape(count * KR, HEAD)


def heads_of(qg, i, first):
    cols = [(first + h) * HEAD for h in range(GROUP)]
    return jnp.concatenate([qg[i, :, :, :, c : c + HEAD].reshape(QSLOTS * T, HEAD) for c in cols], axis=0)


def masked_scores(i, count, k, q, kposb, qpos_ref):
    s = nt(k, q) * SCORE2
    pieces = [s[n * KR : (n + 1) * KR] for n in range(count)]
    qp = qpos_ref[i]
    kp = jnp.concatenate([kposb[i]] * (QR // 128), axis=1)
    pieces[-1] = jnp.where(kp <= qp, pieces[-1], NEG)
    if count == SPAN + 1:
        kp = jnp.concatenate([kposb[i - SPAN]] * (QR // 128), axis=1)
        pieces[0] = jnp.where(kp > qp - float(WINDOW), pieces[0], NEG)
    return jnp.concatenate(pieces, axis=0)


def over_parts(body):
    for i in range(SPAN):
        body(i, i + 1)

    def full(i, carry):
        body(i, SPAN + 1)
        return carry

    lax.fori_loop(SPAN, PARTS, full, 0)


def stats_kernel(*refs):
    kv_refs, qg_refs = refs[0:4], refs[4:8]
    kpos_ref, qpos_ref = refs[8:10]
    out_refs = refs[10:14]
    kv, qg, kposb, ms, sem = refs[14:]
    start_loads(kv_refs, qg_refs, kpos_ref, kv, qg, kposb, sem)

    def body(i, count):
        for copy in part_copies(i, kv_refs, qg_refs, kv, qg, sem):
            copy.wait()
        first, rows = i - count + 1, count * KR
        s = masked_scores(i, count, keys_of(kv, first, count), heads_of(qg, i, 0), kposb, qpos_ref)
        dp = nt(values_of(kv, first, count), heads_of(qg, i, GROUP)).reshape(rows // 8, 8, QR)
        s = s.reshape(rows // 8, 8, QR)
        top = jnp.max(jnp.max(s, axis=0), axis=0, keepdims=True)
        e = jnp.exp2(s - top[None])
        total = jnp.sum(jnp.sum(e, axis=0), axis=0, keepdims=True)
        weighted = jnp.sum(jnp.sum(e * dp, axis=0), axis=0, keepdims=True)
        ms[i] = jnp.concatenate([top, total, weighted, jnp.zeros((5, QR), F32)], axis=0)

    over_parts(body)
    rows = [ms[i][0:4] for i in range(PARTS)]
    stats = jnp.concatenate(rows, axis=0)
    per_head = QSLOTS * T
    for o in range(4):
        for h in range(GROUP):
            cols = slice(h * per_head, (h + 1) * per_head)
            piece = stats[:, cols]
            out_refs[o][:, cols] = pltpu.roll(piece, o * 2 * T, 1) if o else piece


def grads_kernel(*refs):
    kv_refs, qg_refs = refs[0:4], refs[4:8]
    kpos_ref, qpos_ref = refs[8:10]
    st_refs = refs[10:14]
    dkv_near, dkv_first, dkv_last, dq_refs = refs[14], refs[15], refs[16], refs[17:21]
    kv, qg, kposb, kt, dks, dvs, dqt, lse, mean, dkv_out, dq_wide, dq_out, sem, out_sem = refs[21:]
    start_loads(kv_refs, qg_refs, kpos_ref, kv, qg, kposb, sem)
    for part in range(PARTS):
        st = [r[part * 4 : part * 4 + 3, :] for r in st_refs]
        top = jnp.maximum(jnp.maximum(st[0][0:1], st[1][0:1]), jnp.maximum(st[2][0:1], st[3][0:1]))
        fade = [jnp.exp2(a[0:1] - top) for a in st]
        total = sum(a[1:2] * f for a, f in zip(st, fade))
        lse[part] = top + jnp.log2(total)
        mean[part] = sum(a[2:3] * f for a, f in zip(st, fade)) / total

    def dkv_copies(part):
        tok = slice(part * T, (part + 1) * T)
        pairs = (
            (dkv_out.at[part, 0], dkv_near.at[:, :, tok, :]),
            (dkv_out.at[part, 1, 1:3], dkv_first.at[:, :, tok, :]),
            (dkv_out.at[part, 1, 3], dkv_last.at[0, :, tok, :]),
            (dkv_out.at[part, 1, 0], dkv_last.at[1, :, tok, :]),
        )
        return [pltpu.make_async_copy(a, b, out_sem.at[part, n]) for n, (a, b) in enumerate(pairs)]

    def dq_copies(part):
        tok = slice(part * T, (part + 1) * T)
        pairs = [(dq_wide.at[part], dq_refs[0].at[:, tok, :])]
        pairs += [(dq_out.at[part, s - 1], dq_refs[s].at[:, tok, :]) for s in (1, 2, 3)]
        return [pltpu.make_async_copy(a, b, out_sem.at[part, 4 + n]) for n, (a, b) in enumerate(pairs)]

    def emit_dkv(part):
        dk = (dks[part] * SCALE).astype(BF).reshape(4, 2, 2, T, HEAD)
        dv = dvs[part].astype(BF).reshape(4, 2, 2, T, HEAD)
        for a in range(2):
            dkv_out[part, a, :, :, :, :HEAD] = dk[:, a]
            dkv_out[part, a, :, :, :, HEAD:] = dv[:, a]
        for copy in dkv_copies(part):
            copy.start()

    def emit_dq(part):
        dq = dqt[part].T * SCALE
        for h in range(GROUP):
            cols = slice(h * HEAD, (h + 1) * HEAD)
            rows = dq[h * QSLOTS * T : (h + 1) * QSLOTS * T, :].reshape(4, 2, T, HEAD)
            dq_wide[part, :, :, cols] = rows[0]
            dq_out[part, :, :, :, cols] = rows[1:4].astype(BF)
        for copy in dq_copies(part):
            copy.start()

    def body(i, count):
        for copy in part_copies(i, kv_refs, qg_refs, kv, qg, sem):
            copy.wait()
        first = i - count + 1
        k, q, g = keys_of(kv, first, count), heads_of(qg, i, 0), heads_of(qg, i, GROUP)
        kt[:, lanes(i, 1)] = keys_of(kv, i, 1).T
        p = jnp.exp2(masked_scores(i, count, k, q, kposb, qpos_ref) - lse[i])
        ds = (p * (nt(values_of(kv, first, count), g) - mean[i])).astype(BF)
        p = p.astype(BF)
        dk, dv = nn(ds, q), nn(p, g)
        dqt[i] = nn(kt[:, lanes(first, count)], ds)
        for n in range(count - 1):
            dks[first + n] += dk[n * KR : (n + 1) * KR]
            dvs[first + n] += dv[n * KR : (n + 1) * KR]
        dks[i], dvs[i] = dk[(count - 1) * KR :], dv[(count - 1) * KR :]

    over_parts(body)
    for part in range(PARTS):
        emit_dkv(part)
        emit_dq(part)
    for part in range(PARTS):
        for copy in dkv_copies(part) + dq_copies(part):
            copy.wait()


def common_scratch():
    return [
        pltpu.VMEM((PARTS, 4, 2, 2, T, 2 * HEAD), BF),
        pltpu.VMEM((PARTS, 4, 2, T, 2 * GROUP * HEAD), BF),
        pltpu.VMEM((PARTS, KR, 128), F32),
    ]


def in_places(small):
    return [pl.BlockSpec(memory_space=pl.ANY)] * 8 + [pl.BlockSpec(memory_space=pltpu.VMEM)] * small


def run_stats(kvs, qgs, kpos, qpos):
    return pl.pallas_call(
        stats_kernel,
        out_shape=[jax.ShapeDtypeStruct((PARTS * 4, QR), F32)] * 4,
        in_specs=in_places(2),
        scratch_shapes=common_scratch()
        + [pltpu.VMEM((PARTS, 8, QR), F32)]
        + [pltpu.SemaphoreType.DMA((PARTS, 8))],
        compiler_params=pltpu.CompilerParams(vmem_limit_bytes=VMEM_LIMIT),
        cost_estimate=pl.CostEstimate(flops=6_000_000_000, bytes_accessed=3_000_000, transcendentals=5_000_000),
        name="stats",
    )(*kvs, *qgs, kpos, qpos)


def run_grads(kvs, qgs, kpos, qpos, sts):
    dkv = [jax.ShapeDtypeStruct((n, 2, TOK, 2 * HEAD), BF) for n in (4, 2, 2)]
    dq = [jax.ShapeDtypeStruct((2, TOK, GROUP * HEAD), F32 if s == 0 else BF) for s in range(4)]
    out = pl.pallas_call(
        grads_kernel,
        out_shape=dkv + dq,
        in_specs=in_places(6),
        out_specs=[pl.BlockSpec(memory_space=pl.ANY)] * 7,
        scratch_shapes=common_scratch()
        + [
            pltpu.VMEM((HEAD, PARTS * KR), BF),
            pltpu.VMEM((PARTS, KR, HEAD), F32),
            pltpu.VMEM((PARTS, KR, HEAD), F32),
            pltpu.VMEM((PARTS, HEAD, QR), F32),
            pltpu.VMEM((PARTS, 1, QR), F32),
            pltpu.VMEM((PARTS, 1, QR), F32),
            pltpu.VMEM((PARTS, 2, 4, 2, T, 2 * HEAD), BF),
            pltpu.VMEM((PARTS, 2, T, GROUP * HEAD), F32),
            pltpu.VMEM((PARTS, 3, 2, T, GROUP * HEAD), BF),
            pltpu.SemaphoreType.DMA((PARTS, 8)),
            pltpu.SemaphoreType.DMA((PARTS, 8)),
        ],
        compiler_params=pltpu.CompilerParams(vmem_limit_bytes=VMEM_LIMIT),
        cost_estimate=pl.CostEstimate(flops=12_000_000_000, bytes_accessed=6_000_000, transcendentals=5_000_000),
        name="grads",
    )(*kvs, *qgs, kpos, qpos, *sts)
    return out[0], out[1:3], out[3:7]


def pack_kernel(q_ref, g_ref, k_ref, v_ref, kv_own, qg_own, kv_send, qg_send):
    wide = GROUP * HEAD
    mine = lax.axis_index("c")
    for which, kv, qg in ((mine, kv_own.at[0], qg_own.at[0]), (1 - mine, kv_send, qg_send)):
        cols = pl.ds(pl.multiple_of(which * wide, 128), wide)
        small = pl.ds(pl.multiple_of(which * HEAD, 128), HEAD)
        kv[:, :HEAD] = k_ref[:, small]
        kv[:, HEAD:] = v_ref[:, small]
        qg[:, :wide] = q_ref[:, cols]
        qg[:, wide:] = g_ref[:, cols]
    kv_own[1] = kv_send[...]
    qg_own[1] = qg_send[...]


def run_pack(q, g, k, v):
    kv, qg = (TOK, 2 * HEAD), (TOK, 2 * GROUP * HEAD)
    vmem = pl.BlockSpec(memory_space=pltpu.VMEM)
    return pl.pallas_call(
        pack_kernel,
        out_shape=[jax.ShapeDtypeStruct(a, BF) for a in ((2, *kv), (2, *qg), kv, qg)],
        in_specs=[vmem] * 4,
        name="pack",
    )(q, g, k, v)


def columns_kernel(in_ref, *out_refs):
    x = lax.axis_index("x")
    for o in range(4):
        target = (x + o) % 4
        for n in range(4):
            src = pl.ds(pl.multiple_of(n * 4 * HEAD + target * HEAD, 128), HEAD)
            out_refs[o][:, n * HEAD : (n + 1) * HEAD] = in_ref[:, src]


def run_columns(layer_input):
    return pl.pallas_call(
        columns_kernel,
        out_shape=[jax.ShapeDtypeStruct((TOK, 4 * HEAD), BF)] * 4,
        in_specs=[pl.BlockSpec(memory_space=pltpu.VMEM)],
        name="columns",
    )(layer_input)


def finish_kernel(in_ref, k_ref, v_ref, got, sem):
    copies = [pltpu.make_async_copy(in_ref.at[n], got.at[n], sem.at[n]) for n in range(16)]
    for copy in copies:
        copy.start()
    for copy in copies:
        copy.wait()
    for h in range(2):
        total = got[h].astype(F32)
        for n in range(1, 8):
            total = total + got[2 * n + h].astype(F32)
        k_ref[:, h * HEAD : (h + 1) * HEAD] = total[:, :HEAD]
        v_ref[:, h * HEAD : (h + 1) * HEAD] = total[:, HEAD:]


def run_finish(got):
    out = jax.ShapeDtypeStruct((HEAD // 2, 2 * HEAD), F32)
    return pl.pallas_call(
        finish_kernel,
        out_shape=[out, out],
        in_specs=[pl.BlockSpec(memory_space=pl.ANY)],
        scratch_shapes=[pltpu.VMEM((16, HEAD // 2, 2 * HEAD), BF), pltpu.SemaphoreType.DMA((16,))],
        name="finish",
    )(got)


def positions(run_placement, y, z, x, c):
    def device(yy, zz, xx, cc):
        return (((yy % 4) * 2 + zz % 2) * 4 + xx % 4) * 2 + cc % 2

    b, a, e = jnp.meshgrid(jnp.arange(4), jnp.arange(2), jnp.arange(2), indexing="ij")
    keys = device(y, z + a, x + b, c + e).reshape(KSLOTS)
    a, e = jnp.meshgrid(jnp.arange(4), jnp.arange(2), indexing="ij")
    queries = device(y + a, z, x, c + e).reshape(QSLOTS)
    index = jnp.concatenate([keys, queries]).astype(jnp.int32)
    pick = (index[:, None] == jnp.arange(64, dtype=jnp.int32)[None, :]).astype(BF)
    slots = nt(pick, run_placement.astype(BF)).astype(BF)
    lane = jnp.arange(TOK, dtype=jnp.int32)
    spread = jnp.where(lane[None, :] // 2 == jnp.arange(64, dtype=jnp.int32)[:, None], 2.0, 0.0).astype(BF)
    pos = nn(slots, spread) + ((lane // 2) * TOK + lane % 2).astype(F32)[None, :]
    kpos = pos[:KSLOTS]
    qpos = pos[KSLOTS:].reshape(QSLOTS, PARTS, T).transpose(1, 0, 2).reshape(PARTS, 1, 1, QSLOTS * T)
    qpos = jnp.broadcast_to(qpos, (PARTS, 1, GROUP, QSLOTS * T)).reshape(PARTS, 1, QR)
    return kpos, qpos


def own_first(c, mine, other, axis):
    return jnp.where(c == 0, jnp.concatenate([mine, other], axis), jnp.concatenate([other, mine], axis))


def after(array, *gates):
    return lax.optimization_barrier((array, *gates))[0]


def step(query_rows, key_rows, value_rows, output_grad, layer_input, key_matrix, value_matrix, run_placement):
    y, z, x, c, t = (lax.axis_index(a) for a in ("y", "z", "x", "c", "tp"))
    kv_pair, qg_pair, kv_send, qg_send = run_pack(query_rows, output_grad, key_rows, value_rows)
    qg_own = qg_pair.at[1].set(moved(qg_send, "c", 1))
    kv_own = kv_pair.at[1].set(moved(kv_send, "c", 1))
    qgs = [qg_own] + [moved(qg_own, "y", -o) for o in (1, 2, 3)]
    kv_both = jnp.stack([kv_own, moved(kv_own, "z", 1)])
    kvs = [kv_both] + [moved(kv_both, "x", -o) for o in (1, 2, 3)]
    kpos, qpos = positions(run_placement, y, z, x, c)

    half = key_matrix.shape[0] // 2
    cuts = [lax.dynamic_slice_in_dim(after(m, kv_own), (1 - t) * half, half, 0) for m in (key_matrix, value_matrix)]
    x_pieces = run_columns(after(layer_input, kv_both, qpos))
    x_half = jnp.stack([x_pieces[0]] + [moved(x_pieces[4 - o], "x", -o) for o in (1, 2, 3)])
    x_other = moved(x_half, "tp", 1)
    x_here = jnp.where(t == 0, jnp.concatenate([x_half, x_other], 2), jnp.concatenate([x_other, x_half], 2))
    m_far = moved(jnp.where(c == 0, *cuts), "tp", 1)
    kpos = after(kpos, *x_pieces)

    sts = run_stats(kvs, qgs, kpos, qpos)
    sts = [sts[0]] + [moved(sts[o], "y", -o) for o in (1, 2, 3)]
    dkv_near, dkv_sent, dqs = run_grads(kvs, qgs, kpos, qpos, sts)

    def total_of(own, arrived):
        total = own.astype(F32)
        for a in arrived:
            total = total + a.astype(F32)
        return total.astype(BF)

    first = moved(dkv_sent[0], "z", 1)
    row1, row2 = (total_of(dkv_near[o], [first[o - 1]]) for o in (1, 2))
    last = moved(dkv_sent[1], "z", 1)
    near = after(dkv_near, row1)
    row3, row0 = (total_of(near[o], [last[n]]) for n, o in enumerate((3, 0)))
    dq = total_of(dqs[0], [moved(dqs[o], "y", o) for o in (1, 2, 3)])
    x_all = jnp.stack([x_here, moved(x_here, "c", 1)], axis=1)
    m_core = moved(m_far, "c", 1)
    k_far = jnp.where(c == 0, m_far, m_core)
    v_far = jnp.where(c == 0, m_core, m_far)

    got = [moved(row2, "x", 2), moved(row1, "x", 1)]
    dkv = total_of(row0, got + [moved(row3, "x", 3)])
    dkv_all = jnp.stack([dkv] + [moved(dkv, "x", -o) for o in (1, 2, 3)])
    dkv_far = moved(dkv[1], "c", 1)
    k_here = own_first(c, dkv[0, :, :HEAD], dkv_far[:, :HEAD], 1)
    v_here = own_first(c, dkv[0, :, HEAD:], dkv_far[:, HEAD:], 1)
    kv_here = jnp.concatenate([k_here, v_here], 1)
    kv_there = moved(kv_here, "tp", 1)

    query_grad = own_first(c, dq[0], moved(dq[1], "c", 1), 1)

    tokens = 8 * TOK
    weight = lax.dot_general(
        x_all.reshape(tokens, 8 * HEAD),
        dkv_all.reshape(tokens, 2 * HEAD),
        (((0,), (0,)), ((), ())),
        preferred_element_type=F32,
    )
    pieces = weight.astype(BF).reshape(16, HEAD // 2, 2 * HEAD)
    got = lax.all_to_all(pieces, ("y", "z", "c"), 0, 0, tiled=True)
    key_weight, value_weight = run_finish(got)

    km = lax.dynamic_slice_in_dim(key_matrix, t * half, half, 0)
    vm = lax.dynamic_slice_in_dim(value_matrix, t * half, half, 0)
    wide = 2 * HEAD
    total = nt(kv_here[:, :wide], km) + nt(kv_here[:, wide:], vm)
    input_grad = (total + nt(kv_there[:, :wide], k_far) + nt(kv_there[:, wide:], v_far)).astype(BF)
    return (query_grad, input_grad, key_weight, value_weight)


def solution(mesh):
    torus = Mesh(mesh.devices.reshape(4, 2, 4, 2, mesh.shape["tp"]), ("y", "z", "x", "c", "tp"))
    return jax.shard_map(
        step,
        mesh=torus,
        in_specs=(P(SEQ, "tp"),) * 5 + (P(None, "tp"),) * 2 + (P(),),
        out_specs=(P(SEQ, "tp"),) * 4,
        check_vma=False,
    )
```

```python
import functools
import math

import jax
import jax.numpy as jnp
from jax import lax
from jax.experimental import pallas as pl
from jax.experimental.pallas import tpu as pltpu
from jax.sharding import Mesh
from jax.sharding import PartitionSpec as P


HEAD = 128
WINDOW = 4096
GROUP = 4
TOK = 128
SEQ = ("y", "z", "x", "c")
BF = jnp.bfloat16
F32 = jnp.float32
NEG = -1e30

PARTS = 8
T = TOK // PARTS
KSLOTS = 16
QSLOTS = 8
KR = KSLOTS * T
QR = QSLOTS * GROUP * T
SPAN = PARTS // 2
HALF = KR // 2
SCALE = 1.0 / math.sqrt(HEAD)
SCORE2 = SCALE * math.log2(math.e)
VMEM_LIMIT = 60 * 1024 * 1024


def moved(array, axis, by):
    n = lax.axis_size(axis)
    return lax.ppermute(array, axis, [(i, (i + by) % n) for i in range(n)])


def nt(a, b):
    return lax.dot_general(a, b, (((1,), (1,)), ((), ())), preferred_element_type=F32)


def nn(a, b):
    return lax.dot_general(a, b, (((1,), (0,)), ((), ())), preferred_element_type=F32)


def part_copies(part, kv_refs, qg_refs, kv, qg, sem):
    tok = pl.ds(part * T, T)
    for b in range(4):
        yield pltpu.make_async_copy(kv_refs[b].at[:, :, tok, :], kv.at[part, b], sem.at[part, b])
    for s in range(4):
        yield pltpu.make_async_copy(qg_refs[s].at[:, tok, :], qg.at[part, s], sem.at[part, 4 + s])


def start_loads(kv_refs, qg_refs, kpos_ref, kv, qg, kposb, sem):
    for part in range(PARTS):
        for copy in part_copies(part, kv_refs, qg_refs, kv, qg, sem):
            copy.start()
    for slot in range(KSLOTS):
        column = jnp.broadcast_to(kpos_ref[slot : slot + 1, :], (TOK, 128)).T
        for part in range(PARTS):
            kposb[part, slot * T : (slot + 1) * T, :] = column[part * T : (part + 1) * T, :]


def lanes(first, count):
    return pl.ds(pl.multiple_of(first * HALF, 128), count * HALF)


def keys_of(kv, first, count):
    return kv[pl.ds(first, count), :, :, :, :, :HEAD].reshape(count * KR, HEAD)


def values_of(kv, first, count):
    return kv[pl.ds(first, count), :, :, :, :, HEAD:].reshape(count * KR, HEAD)


def heads_of(qg, i, first):
    cols = [(first + h) * HEAD for h in range(GROUP)]
    return jnp.concatenate([qg[i, :, :, :, c : c + HEAD].reshape(QSLOTS * T, HEAD) for c in cols], axis=0)


def masked_scores(i, count, k, q, kposb, qpos_ref, size=KR):
    s = nt(k, q) * SCORE2
    pieces = [s[n * size : (n + 1) * size] for n in range(count)]
    qp = qpos_ref[i]
    kp = jnp.concatenate([kposb[i]] * (QR // 128), axis=1)
    pieces[-1] = jnp.where(kp <= qp, pieces[-1], NEG)
    if count == SPAN + 1:
        kp = jnp.concatenate([kposb[i - SPAN]] * (QR // 128), axis=1)
        pieces[0] = jnp.where(kp > qp - float(WINDOW), pieces[0], NEG)
    return jnp.concatenate(pieces, axis=0)


def over_parts(body):
    for i in range(SPAN):
        body(i, i + 1)

    def full(i, carry):
        body(i, SPAN + 1)
        return carry

    lax.fori_loop(SPAN, PARTS, full, 0)


def stats_kernel(*refs):
    kv_refs, qg_refs = refs[0:4], refs[4:8]
    kpos_ref, qpos_ref = refs[8:10]
    out_refs = refs[10:14]
    kv, qg, kposb, ms, sem = refs[14:]
    start_loads(kv_refs, qg_refs, kpos_ref, kv, qg, kposb, sem)

    def body(i, count):
        for copy in part_copies(i, kv_refs, qg_refs, kv, qg, sem):
            copy.wait()
        first, rows = i - count + 1, count * KR
        s = masked_scores(i, count, keys_of(kv, first, count), heads_of(qg, i, 0), kposb, qpos_ref)
        dp = nt(values_of(kv, first, count), heads_of(qg, i, GROUP)).reshape(rows // 8, 8, QR)
        s = s.reshape(rows // 8, 8, QR)
        top = jnp.max(jnp.max(s, axis=0), axis=0, keepdims=True)
        e = jnp.exp2(s - top[None])
        total = jnp.sum(jnp.sum(e, axis=0), axis=0, keepdims=True)
        weighted = jnp.sum(jnp.sum(e * dp, axis=0), axis=0, keepdims=True)
        ms[i] = jnp.concatenate([top, total, weighted, jnp.zeros((5, QR), F32)], axis=0)

    over_parts(body)
    rows = [ms[i][0:4] for i in range(PARTS)]
    stats = jnp.concatenate(rows, axis=0)
    per_head = QSLOTS * T
    for o in range(4):
        for h in range(GROUP):
            cols = slice(h * per_head, (h + 1) * per_head)
            piece = stats[:, cols]
            out_refs[o][:, cols] = pltpu.roll(piece, o * 2 * T, 1) if o else piece


def grads_kernel(near, *refs):
    kv_refs, qg_refs = refs[0:4], refs[4:8]
    kpos_ref, qpos_ref = refs[8:10]
    st_refs = refs[10:14]
    if near:
        dq_in, dkv_ref, dq_refs = refs[14], refs[15], refs[16:20]
        refs = refs[20:]
    else:
        dkv_ref, dq_part = refs[14:16]
        refs = refs[16:]
    kv, qg, kposb, kt, dks, dvs, dqt, lse, mean, dkv_out, dq_wide, dq_out, sem, out_sem = refs
    side = 0 if near else 1

    def loads(part):
        tok = pl.ds(part * T, T)
        for b in range(4):
            yield pltpu.make_async_copy(kv_refs[b].at[side, :, tok, :], kv.at[part, b], sem.at[part, b])
        for s in range(4):
            yield pltpu.make_async_copy(qg_refs[s].at[:, tok, :], qg.at[part, s], sem.at[part, 4 + s])
        if near:
            yield pltpu.make_async_copy(dq_in.at[part], dqt.at[part], sem.at[part, 8])

    def dkv_copy(part):
        tok = slice(part * T, (part + 1) * T)
        return pltpu.make_async_copy(dkv_out.at[part], dkv_ref.at[:, :, tok, :], out_sem.at[part, 0])

    def dq_copies(part):
        if not near:
            return [pltpu.make_async_copy(dqt.at[part], dq_part.at[part], out_sem.at[part, 1])]
        tok = slice(part * T, (part + 1) * T)
        pairs = [(dq_wide.at[part], dq_refs[0].at[:, tok, :])]
        pairs += [(dq_out.at[part, s - 1], dq_refs[s].at[:, tok, :]) for s in (1, 2, 3)]
        return [pltpu.make_async_copy(a, b, out_sem.at[part, 1 + n]) for n, (a, b) in enumerate(pairs)]

    for part in range(PARTS):
        for copy in loads(part):
            copy.start()
    for n in range(KSLOTS // 2):
        slot = (n // 2) * 4 + side * 2 + n % 2
        column = jnp.broadcast_to(kpos_ref[slot : slot + 1, :], (TOK, 128)).T
        for part in range(PARTS):
            kposb[part, n * T : (n + 1) * T, :] = column[part * T : (part + 1) * T, :]
    for part in range(PARTS):
        st = [r[part * 4 : part * 4 + 3, :] for r in st_refs]
        top = jnp.maximum(jnp.maximum(st[0][0:1], st[1][0:1]), jnp.maximum(st[2][0:1], st[3][0:1]))
        fade = [jnp.exp2(a[0:1] - top) for a in st]
        total = sum(a[1:2] * f for a, f in zip(st, fade))
        lse[part] = top + jnp.log2(total)
        mean[part] = sum(a[2:3] * f for a, f in zip(st, fade)) / total

    def body(i, count):
        for copy in loads(i):
            copy.wait()
        first = i - count + 1
        rows = count * HALF
        k = kv[pl.ds(first, count), :, :, :, :HEAD].reshape(rows, HEAD)
        v = kv[pl.ds(first, count), :, :, :, HEAD:].reshape(rows, HEAD)
        q, g = heads_of(qg, i, 0), heads_of(qg, i, GROUP)
        kt[:, lanes(i, 1)] = kv[i, :, :, :, :HEAD].reshape(HALF, HEAD).T
        p = jnp.exp2(masked_scores(i, count, k, q, kposb, qpos_ref, HALF) - lse[i])
        ds = (p * (nt(v, g) - mean[i])).astype(BF)
        p = p.astype(BF)
        dk, dv, dq = nn(ds, q), nn(p, g), nn(kt[:, lanes(first, count)], ds)
        dqt[i] = dqt[i] + dq if near else dq
        for n in range(count - 1):
            dks[first + n] += dk[n * HALF : (n + 1) * HALF]
            dvs[first + n] += dv[n * HALF : (n + 1) * HALF]
        dks[i], dvs[i] = dk[rows - HALF :], dv[rows - HALF :]

    over_parts(body)
    for part in range(PARTS):
        dkv_out[part, :, :, :, :HEAD] = (dks[part] * SCALE).astype(BF).reshape(4, 2, T, HEAD)
        dkv_out[part, :, :, :, HEAD:] = dvs[part].astype(BF).reshape(4, 2, T, HEAD)
        dkv_copy(part).start()
        if near:
            dq = dqt[part].T * SCALE
            for h in range(GROUP):
                cols = slice(h * HEAD, (h + 1) * HEAD)
                rows = dq[h * QSLOTS * T : (h + 1) * QSLOTS * T, :].reshape(4, 2, T, HEAD)
                dq_wide[part, :, :, cols] = rows[0]
                dq_out[part, :, :, :, cols] = rows[1:4].astype(BF)
        for copy in dq_copies(part):
            copy.start()
    for part in range(PARTS):
        for copy in [dkv_copy(part)] + dq_copies(part):
            copy.wait()


def common_scratch():
    return [
        pltpu.VMEM((PARTS, 4, 2, 2, T, 2 * HEAD), BF),
        pltpu.VMEM((PARTS, 4, 2, T, 2 * GROUP * HEAD), BF),
        pltpu.VMEM((PARTS, KR, 128), F32),
    ]


def in_places(small):
    return [pl.BlockSpec(memory_space=pl.ANY)] * 8 + [pl.BlockSpec(memory_space=pltpu.VMEM)] * small


def run_stats(kvs, qgs, kpos, qpos):
    return pl.pallas_call(
        stats_kernel,
        out_shape=[jax.ShapeDtypeStruct((PARTS * 4, QR), F32)] * 4,
        in_specs=in_places(2),
        scratch_shapes=common_scratch()
        + [pltpu.VMEM((PARTS, 8, QR), F32)]
        + [pltpu.SemaphoreType.DMA((PARTS, 8))],
        compiler_params=pltpu.CompilerParams(vmem_limit_bytes=VMEM_LIMIT),
        cost_estimate=pl.CostEstimate(flops=6_000_000_000, bytes_accessed=3_000_000, transcendentals=5_000_000),
        name="stats",
    )(*kvs, *qgs, kpos, qpos)


def run_grads(near, kvs, qgs, kpos, qpos, sts, extra=()):
    outs = [jax.ShapeDtypeStruct((4, 2, TOK, 2 * HEAD), BF)]
    if near:
        outs += [jax.ShapeDtypeStruct((2, TOK, GROUP * HEAD), F32 if s == 0 else BF) for s in range(4)]
    else:
        outs += [jax.ShapeDtypeStruct((PARTS, HEAD, QR), F32)]
    anywhere = pl.BlockSpec(memory_space=pl.ANY)
    return pl.pallas_call(
        functools.partial(grads_kernel, near),
        out_shape=outs,
        in_specs=in_places(6) + [anywhere] * len(extra),
        out_specs=[anywhere] * len(outs),
        scratch_shapes=[
            pltpu.VMEM((PARTS, 4, 2, T, 2 * HEAD), BF),
            pltpu.VMEM((PARTS, 4, 2, T, 2 * GROUP * HEAD), BF),
            pltpu.VMEM((PARTS, HALF, 128), F32),
            pltpu.VMEM((HEAD, PARTS * HALF), BF),
            pltpu.VMEM((PARTS, HALF, HEAD), F32),
            pltpu.VMEM((PARTS, HALF, HEAD), F32),
            pltpu.VMEM((PARTS, HEAD, QR), F32),
            pltpu.VMEM((PARTS, 1, QR), F32),
            pltpu.VMEM((PARTS, 1, QR), F32),
            pltpu.VMEM((PARTS, 4, 2, T, 2 * HEAD), BF),
            pltpu.VMEM((PARTS, 2, T, GROUP * HEAD), F32),
            pltpu.VMEM((PARTS, 3, 2, T, GROUP * HEAD), BF),
            pltpu.SemaphoreType.DMA((PARTS, 9)),
            pltpu.SemaphoreType.DMA((PARTS, 5)),
        ],
        compiler_params=pltpu.CompilerParams(vmem_limit_bytes=VMEM_LIMIT),
        cost_estimate=pl.CostEstimate(flops=6_000_000_000, bytes_accessed=6_000_000, transcendentals=2_500_000),
        name="grads_near" if near else "grads_far",
    )(*kvs, *qgs, kpos, qpos, *sts, *extra)


def pack_kernel(q_ref, g_ref, k_ref, v_ref, kv_own, qg_own, kv_send, qg_send):
    wide = GROUP * HEAD
    mine = lax.axis_index("c")
    for which, kv, qg in ((mine, kv_own.at[0], qg_own.at[0]), (1 - mine, kv_send, qg_send)):
        cols = pl.ds(pl.multiple_of(which * wide, 128), wide)
        small = pl.ds(pl.multiple_of(which * HEAD, 128), HEAD)
        kv[:, :HEAD] = k_ref[:, small]
        kv[:, HEAD:] = v_ref[:, small]
        qg[:, :wide] = q_ref[:, cols]
        qg[:, wide:] = g_ref[:, cols]
    kv_own[1] = kv_send[...]
    qg_own[1] = qg_send[...]


def run_pack(q, g, k, v):
    kv, qg = (TOK, 2 * HEAD), (TOK, 2 * GROUP * HEAD)
    vmem = pl.BlockSpec(memory_space=pltpu.VMEM)
    return pl.pallas_call(
        pack_kernel,
        out_shape=[jax.ShapeDtypeStruct(a, BF) for a in ((2, *kv), (2, *qg), kv, qg)],
        in_specs=[vmem] * 4,
        name="pack",
    )(q, g, k, v)


def columns_kernel(in_ref, *out_refs):
    x = lax.axis_index("x")
    for o in range(4):
        target = (x + o) % 4
        for n in range(4):
            src = pl.ds(pl.multiple_of(n * 4 * HEAD + target * HEAD, 128), HEAD)
            out_refs[o][:, n * HEAD : (n + 1) * HEAD] = in_ref[:, src]


def run_columns(layer_input):
    return pl.pallas_call(
        columns_kernel,
        out_shape=[jax.ShapeDtypeStruct((TOK, 4 * HEAD), BF)] * 4,
        in_specs=[pl.BlockSpec(memory_space=pltpu.VMEM)],
        name="columns",
    )(layer_input)


def finish_kernel(in_ref, k_ref, v_ref, got, sem):
    copies = [pltpu.make_async_copy(in_ref.at[n], got.at[n], sem.at[n]) for n in range(16)]
    for copy in copies:
        copy.start()
    for copy in copies:
        copy.wait()
    for h in range(2):
        total = got[h].astype(F32)
        for n in range(1, 8):
            total = total + got[2 * n + h].astype(F32)
        k_ref[:, h * HEAD : (h + 1) * HEAD] = total[:, :HEAD]
        v_ref[:, h * HEAD : (h + 1) * HEAD] = total[:, HEAD:]


def run_finish(got):
    out = jax.ShapeDtypeStruct((HEAD // 2, 2 * HEAD), F32)
    return pl.pallas_call(
        finish_kernel,
        out_shape=[out, out],
        in_specs=[pl.BlockSpec(memory_space=pltpu.HBM)],
        scratch_shapes=[pltpu.VMEM((16, HEAD // 2, 2 * HEAD), BF), pltpu.SemaphoreType.DMA((16,))],
        name="finish",
    )(got)


def positions(run_placement, y, z, x, c):
    def device(yy, zz, xx, cc):
        return (((yy % 4) * 2 + zz % 2) * 4 + xx % 4) * 2 + cc % 2

    b, a, e = jnp.meshgrid(jnp.arange(4), jnp.arange(2), jnp.arange(2), indexing="ij")
    keys = device(y, z + a, x + b, c + e).reshape(KSLOTS)
    a, e = jnp.meshgrid(jnp.arange(4), jnp.arange(2), indexing="ij")
    queries = device(y + a, z, x, c + e).reshape(QSLOTS)
    index = jnp.concatenate([keys, queries]).astype(jnp.int32)
    pick = (index[:, None] == jnp.arange(64, dtype=jnp.int32)[None, :]).astype(BF)
    slots = nt(pick, run_placement.astype(BF)).astype(BF)
    lane = jnp.arange(TOK, dtype=jnp.int32)
    spread = jnp.where(lane[None, :] // 2 == jnp.arange(64, dtype=jnp.int32)[:, None], 2.0, 0.0).astype(BF)
    pos = nn(slots, spread) + ((lane // 2) * TOK + lane % 2).astype(F32)[None, :]
    kpos = pos[:KSLOTS]
    qpos = pos[KSLOTS:].reshape(QSLOTS, PARTS, T).transpose(1, 0, 2).reshape(PARTS, 1, 1, QSLOTS * T)
    qpos = jnp.broadcast_to(qpos, (PARTS, 1, GROUP, QSLOTS * T)).reshape(PARTS, 1, QR)
    return kpos, qpos


def own_first(c, mine, other, axis):
    return jnp.where(c == 0, jnp.concatenate([mine, other], axis), jnp.concatenate([other, mine], axis))


def after(array, *gates):
    return lax.optimization_barrier((array, *gates))[0]


def step(query_rows, key_rows, value_rows, output_grad, layer_input, key_matrix, value_matrix, run_placement):
    y, z, x, c, t = (lax.axis_index(a) for a in ("y", "z", "x", "c", "tp"))
    kv_pair, qg_pair, kv_send, qg_send = run_pack(query_rows, output_grad, key_rows, value_rows)
    qg_own = qg_pair.at[1].set(moved(qg_send, "c", 1))
    kv_own = kv_pair.at[1].set(moved(kv_send, "c", 1))
    qgs = [qg_own] + [moved(qg_own, "y", -o) for o in (1, 2, 3)]
    kv_both = jnp.stack([kv_own, moved(kv_own, "z", 1)])
    kvs = [kv_both] + [moved(kv_both, "x", -o) for o in (1, 2, 3)]
    kpos, qpos = positions(run_placement, y, z, x, c)

    half = key_matrix.shape[0] // 2
    cuts = [lax.dynamic_slice_in_dim(after(m, kv_own), (1 - t) * half, half, 0) for m in (key_matrix, value_matrix)]
    x_pieces = run_columns(after(layer_input, kv_both, qpos))
    x_half = jnp.stack([x_pieces[0]] + [moved(x_pieces[4 - o], "x", -o) for o in (1, 2, 3)])
    x_other = moved(x_half, "tp", 1)
    x_here = jnp.where(t == 0, jnp.concatenate([x_half, x_other], 2), jnp.concatenate([x_other, x_half], 2))
    m_far = moved(jnp.where(c == 0, *cuts), "tp", 1)
    kpos = after(kpos, *x_pieces)

    sts = run_stats(kvs, qgs, kpos, qpos)
    sts = [sts[0]] + [moved(sts[o], "y", -o) for o in (1, 2, 3)]
    dkv_sent, dq_part = run_grads(False, kvs, qgs, kpos, qpos, sts)
    dkv_got = moved(dkv_sent, "z", 1)
    dkv_near, *dqs = run_grads(True, kvs, qgs, kpos, qpos, sts, (dq_part,))

    def total_of(own, arrived):
        total = own.astype(F32)
        for a in arrived:
            total = total + a.astype(F32)
        return total.astype(BF)

    rows = [total_of(dkv_near[o], [dkv_got[o]]) for o in range(4)]
    dq = total_of(dqs[0], [moved(dqs[o], "y", o) for o in (1, 2, 3)])
    x_all = jnp.stack([x_here, moved(x_here, "c", 1)], axis=1)
    m_core = moved(m_far, "c", 1)
    k_far = jnp.where(c == 0, m_far, m_core)
    v_far = jnp.where(c == 0, m_core, m_far)

    dkv = total_of(rows[0], [moved(rows[o], "x", o) for o in (2, 1, 3)])
    dkv_all = jnp.stack([dkv] + [moved(dkv, "x", -o) for o in (1, 2, 3)])
    dkv_far = moved(dkv[1], "c", 1)
    k_here = own_first(c, dkv[0, :, :HEAD], dkv_far[:, :HEAD], 1)
    v_here = own_first(c, dkv[0, :, HEAD:], dkv_far[:, HEAD:], 1)
    kv_here = jnp.concatenate([k_here, v_here], 1)
    kv_there = moved(kv_here, "tp", 1)

    query_grad = own_first(c, dq[0], moved(dq[1], "c", 1), 1)

    tokens = 8 * TOK
    weight = lax.dot_general(
        x_all.reshape(tokens, 8 * HEAD),
        dkv_all.reshape(tokens, 2 * HEAD),
        (((0,), (0,)), ((), ())),
        preferred_element_type=F32,
    )
    pieces = weight.astype(BF).reshape(16, HEAD // 2, 2 * HEAD)
    got = lax.all_to_all(pieces, ("y", "z", "c"), 0, 0, tiled=True)
    key_weight, value_weight = run_finish(got)

    km = lax.dynamic_slice_in_dim(key_matrix, t * half, half, 0)
    vm = lax.dynamic_slice_in_dim(value_matrix, t * half, half, 0)
    wide = 2 * HEAD
    total = nt(kv_here[:, :wide], km) + nt(kv_here[:, wide:], vm)
    input_grad = (total + nt(kv_there[:, :wide], k_far) + nt(kv_there[:, wide:], v_far)).astype(BF)
    return (query_grad, input_grad, key_weight, value_weight)


def solution(mesh):
    torus = Mesh(mesh.devices.reshape(4, 2, 4, 2, mesh.shape["tp"]), ("y", "z", "x", "c", "tp"))
    return jax.shard_map(
        step,
        mesh=torus,
        in_specs=(P(SEQ, "tp"),) * 5 + (P(None, "tp"),) * 2 + (P(),),
        out_specs=(P(SEQ, "tp"),) * 4,
        check_vma=False,
    )
```

```python
import functools
import math

import jax
import jax.numpy as jnp
from jax import lax
from jax.experimental import pallas as pl
from jax.experimental.pallas import tpu as pltpu
from jax.sharding import Mesh
from jax.sharding import PartitionSpec as P


HEAD = 128
WINDOW = 4096
GROUP = 4
TOK = 128
SEQ = ("y", "z", "x", "c")
BF = jnp.bfloat16
F32 = jnp.float32
NEG = -1e30

PARTS = 8
T = TOK // PARTS
KSLOTS = 16
QSLOTS = 8
KR = KSLOTS * T
QR = QSLOTS * GROUP * T
SPAN = PARTS // 2
SCALE = 1.0 / math.sqrt(HEAD)
SCORE2 = SCALE * math.log2(math.e)
VMEM_LIMIT = 60 * 1024 * 1024


def moved(array, axis, by):
    n = lax.axis_size(axis)
    return lax.ppermute(array, axis, [(i, (i + by) % n) for i in range(n)])


def nt(a, b):
    return lax.dot_general(a, b, (((1,), (1,)), ((), ())), preferred_element_type=F32)


def nn(a, b):
    return lax.dot_general(a, b, (((1,), (0,)), ((), ())), preferred_element_type=F32)


def part_copies(part, kv_refs, qg_refs, kv, qg, sem):
    tok = pl.ds(part * T, T)
    for b in range(4):
        yield pltpu.make_async_copy(kv_refs[b].at[:, :, tok, :], kv.at[part, b], sem.at[part, b])
    for s in range(4):
        yield pltpu.make_async_copy(qg_refs[s].at[:, tok, :], qg.at[part, s], sem.at[part, 4 + s])


def start_loads(kv_refs, qg_refs, kpos_ref, kv, qg, kposb, sem):
    for part in range(PARTS):
        for copy in part_copies(part, kv_refs, qg_refs, kv, qg, sem):
            copy.start()
    for slot in range(KSLOTS):
        column = jnp.broadcast_to(kpos_ref[slot : slot + 1, :], (TOK, 128)).T
        for part in range(PARTS):
            kposb[part, slot * T : (slot + 1) * T, :] = column[part * T : (part + 1) * T, :]


def lanes(first, count):
    return pl.ds(pl.multiple_of(first * KR, 128), count * KR)


def keys_of(kv, first, count):
    return kv[pl.ds(first, count), :, :, :, :, :HEAD].reshape(count * KR, HEAD)


def values_of(kv, first, count):
    return kv[pl.ds(first, count), :, :, :, :, HEAD:].reshape(count * KR, HEAD)


def heads_of(qg, i, first):
    cols = [(first + h) * HEAD for h in range(GROUP)]
    return jnp.concatenate([qg[i, :, :, :, c : c + HEAD].reshape(QSLOTS * T, HEAD) for c in cols], axis=0)


def masked_scores(i, count, k, q, kposb, qpos_ref):
    s = nt(k, q) * SCORE2
    pieces = [s[n * KR : (n + 1) * KR] for n in range(count)]
    qp = qpos_ref[i]
    kp = jnp.concatenate([kposb[i]] * (QR // 128), axis=1)
    pieces[-1] = jnp.where(kp <= qp, pieces[-1], NEG)
    if count == SPAN + 1:
        kp = jnp.concatenate([kposb[i - SPAN]] * (QR // 128), axis=1)
        pieces[0] = jnp.where(kp > qp - float(WINDOW), pieces[0], NEG)
    return jnp.concatenate(pieces, axis=0)


def over_parts(body):
    for i in range(SPAN):
        body(i, i + 1)

    def full(i, carry):
        body(i, SPAN + 1)
        return carry

    lax.fori_loop(SPAN, PARTS, full, 0)


def stats_kernel(*refs):
    kv_refs, qg_refs = refs[0:4], refs[4:8]
    kpos_ref, qpos_ref = refs[8:10]
    out_refs = refs[10:14]
    kv, qg, kposb, ms, sem = refs[14:]
    start_loads(kv_refs, qg_refs, kpos_ref, kv, qg, kposb, sem)

    def body(i, count):
        for copy in part_copies(i, kv_refs, qg_refs, kv, qg, sem):
            copy.wait()
        first, rows = i - count + 1, count * KR
        s = masked_scores(i, count, keys_of(kv, first, count), heads_of(qg, i, 0), kposb, qpos_ref)
        dp = nt(values_of(kv, first, count), heads_of(qg, i, GROUP)).reshape(rows // 8, 8, QR)
        s = s.reshape(rows // 8, 8, QR)
        top = jnp.max(jnp.max(s, axis=0), axis=0, keepdims=True)
        e = jnp.exp2(s - top[None])
        total = jnp.sum(jnp.sum(e, axis=0), axis=0, keepdims=True)
        weighted = jnp.sum(jnp.sum(e * dp, axis=0), axis=0, keepdims=True)
        ms[i] = jnp.concatenate([top, total, weighted, jnp.zeros((5, QR), F32)], axis=0)

    over_parts(body)
    stats = jnp.concatenate([ms[i][n : n + 1] for n in range(3) for i in range(PARTS)], axis=0)
    per_head = QSLOTS * T
    for o in range(4):
        for h in range(GROUP):
            cols = slice(h * per_head, (h + 1) * per_head)
            piece = stats[:, cols]
            out_refs[o][:, cols] = pltpu.roll(piece, o * 2 * T, 1) if o else piece


def grads_kernel(*refs):
    kv_refs, qg_refs = refs[0:4], refs[4:8]
    kpos_ref, qpos_ref = refs[8:10]
    st_refs = refs[10:14]
    dkv_near, dkv_first, dkv_last, dq_refs = refs[14], refs[15], refs[16], refs[17:21]
    kv, qg, kposb, kt, dks, dvs, dqt, lse, mean, dkv_out, dq_wide, dq_out, sem, out_sem = refs[21:]
    start_loads(kv_refs, qg_refs, kpos_ref, kv, qg, kposb, sem)
    kinds = [[r[n * PARTS : (n + 1) * PARTS, :] for r in st_refs] for n in range(3)]
    top = functools.reduce(jnp.maximum, kinds[0])
    fade = [jnp.exp2(a - top) for a in kinds[0]]
    total = sum(a * f for a, f in zip(kinds[1], fade))
    merged = top + jnp.log2(total)
    means = sum(a * f for a, f in zip(kinds[2], fade)) / total
    for part in range(PARTS):
        lse[part] = merged[part : part + 1]
        mean[part] = means[part : part + 1]

    def dkv_copies(part):
        tok = slice(part * T, (part + 1) * T)
        pairs = (
            (dkv_out.at[part, 0], dkv_near.at[:, :, tok, :]),
            (dkv_out.at[part, 1, 1:3], dkv_first.at[:, :, tok, :]),
            (dkv_out.at[part, 1, 3], dkv_last.at[0, :, tok, :]),
            (dkv_out.at[part, 1, 0], dkv_last.at[1, :, tok, :]),
        )
        return [pltpu.make_async_copy(a, b, out_sem.at[part, n]) for n, (a, b) in enumerate(pairs)]

    def dq_copies(part):
        tok = slice(part * T, (part + 1) * T)
        pairs = [(dq_wide.at[part], dq_refs[0].at[:, tok, :])]
        pairs += [(dq_out.at[part, s - 1], dq_refs[s].at[:, tok, :]) for s in (1, 2, 3)]
        return [pltpu.make_async_copy(a, b, out_sem.at[part, 4 + n]) for n, (a, b) in enumerate(pairs)]

    def emit_dkv(part):
        dk = (dks[part] * SCALE).astype(BF).reshape(4, 2, 2, T, HEAD)
        dv = dvs[part].astype(BF).reshape(4, 2, 2, T, HEAD)
        for a in range(2):
            dkv_out[part, a, :, :, :, :HEAD] = dk[:, a]
            dkv_out[part, a, :, :, :, HEAD:] = dv[:, a]
        for copy in dkv_copies(part):
            copy.start()

    def emit_dq(part):
        dq = dqt[part].T * SCALE
        for h in range(GROUP):
            cols = slice(h * HEAD, (h + 1) * HEAD)
            rows = dq[h * QSLOTS * T : (h + 1) * QSLOTS * T, :].reshape(4, 2, T, HEAD)
            dq_wide[part, :, :, cols] = rows[0]
            dq_out[part, :, :, :, cols] = rows[1:4].astype(BF)
        for copy in dq_copies(part):
            copy.start()

    def body(i, count):
        for copy in part_copies(i, kv_refs, qg_refs, kv, qg, sem):
            copy.wait()
        first = i - count + 1
        k, q, g = keys_of(kv, first, count), heads_of(qg, i, 0), heads_of(qg, i, GROUP)
        kt[:, lanes(i, 1)] = keys_of(kv, i, 1).T
        p = jnp.exp2(masked_scores(i, count, k, q, kposb, qpos_ref) - lse[i])
        ds = (p * (nt(values_of(kv, first, count), g) - mean[i])).astype(BF)
        p = p.astype(BF)
        dk, dv = nn(ds, q), nn(p, g)
        dqt[i] = nn(kt[:, lanes(first, count)], ds)
        for n in range(count - 1):
            dks[first + n] += dk[n * KR : (n + 1) * KR]
            dvs[first + n] += dv[n * KR : (n + 1) * KR]
        dks[i], dvs[i] = dk[(count - 1) * KR :], dv[(count - 1) * KR :]

    over_parts(body)
    for part in range(PARTS):
        emit_dkv(part)
        emit_dq(part)
    for part in range(PARTS):
        for copy in dkv_copies(part) + dq_copies(part):
            copy.wait()


def common_scratch():
    return [
        pltpu.VMEM((PARTS, 4, 2, 2, T, 2 * HEAD), BF),
        pltpu.VMEM((PARTS, 4, 2, T, 2 * GROUP * HEAD), BF),
        pltpu.VMEM((PARTS, KR, 128), F32),
    ]


def in_places(small):
    return [pl.BlockSpec(memory_space=pl.ANY)] * 8 + [pl.BlockSpec(memory_space=pltpu.VMEM)] * small


def run_stats(kvs, qgs, kpos, qpos):
    return pl.pallas_call(
        stats_kernel,
        out_shape=[jax.ShapeDtypeStruct((PARTS * 3, QR), F32)] * 4,
        in_specs=in_places(2),
        scratch_shapes=common_scratch()
        + [pltpu.VMEM((PARTS, 8, QR), F32)]
        + [pltpu.SemaphoreType.DMA((PARTS, 8))],
        compiler_params=pltpu.CompilerParams(vmem_limit_bytes=VMEM_LIMIT),
        cost_estimate=pl.CostEstimate(flops=6_000_000_000, bytes_accessed=3_000_000, transcendentals=5_000_000),
        name="stats",
    )(*kvs, *qgs, kpos, qpos)


def run_grads(kvs, qgs, kpos, qpos, sts):
    dkv = [jax.ShapeDtypeStruct((n, 2, TOK, 2 * HEAD), BF) for n in (4, 2, 2)]
    dq = [jax.ShapeDtypeStruct((2, TOK, GROUP * HEAD), F32 if s == 0 else BF) for s in range(4)]
    out = pl.pallas_call(
        grads_kernel,
        out_shape=dkv + dq,
        in_specs=in_places(6),
        out_specs=[pl.BlockSpec(memory_space=pl.ANY)] * 7,
        scratch_shapes=common_scratch()
        + [
            pltpu.VMEM((HEAD, PARTS * KR), BF),
            pltpu.VMEM((PARTS, KR, HEAD), F32),
            pltpu.VMEM((PARTS, KR, HEAD), F32),
            pltpu.VMEM((PARTS, HEAD, QR), F32),
            pltpu.VMEM((PARTS, 1, QR), F32),
            pltpu.VMEM((PARTS, 1, QR), F32),
            pltpu.VMEM((PARTS, 2, 4, 2, T, 2 * HEAD), BF),
            pltpu.VMEM((PARTS, 2, T, GROUP * HEAD), F32),
            pltpu.VMEM((PARTS, 3, 2, T, GROUP * HEAD), BF),
            pltpu.SemaphoreType.DMA((PARTS, 8)),
            pltpu.SemaphoreType.DMA((PARTS, 8)),
        ],
        compiler_params=pltpu.CompilerParams(vmem_limit_bytes=VMEM_LIMIT),
        cost_estimate=pl.CostEstimate(flops=12_000_000_000, bytes_accessed=6_000_000, transcendentals=5_000_000),
        name="grads",
    )(*kvs, *qgs, kpos, qpos, *sts)
    return out[0], out[1:3], out[3:7]


def pack_kernel(q_ref, g_ref, k_ref, v_ref, kv_own, qg_own, kv_send, qg_send):
    wide = GROUP * HEAD
    mine = lax.axis_index("c")
    for which, kv, qg in ((mine, kv_own.at[0], qg_own.at[0]), (1 - mine, kv_send, qg_send)):
        cols = pl.ds(pl.multiple_of(which * wide, 128), wide)
        small = pl.ds(pl.multiple_of(which * HEAD, 128), HEAD)
        kv[:, :HEAD] = k_ref[:, small]
        kv[:, HEAD:] = v_ref[:, small]
        qg[:, :wide] = q_ref[:, cols]
        qg[:, wide:] = g_ref[:, cols]


def run_pack(q, g, k, v):
    kv, qg = (TOK, 2 * HEAD), (TOK, 2 * GROUP * HEAD)
    vmem = pl.BlockSpec(memory_space=pltpu.VMEM)
    return pl.pallas_call(
        pack_kernel,
        out_shape=[jax.ShapeDtypeStruct(a, BF) for a in ((2, *kv), (2, *qg), kv, qg)],
        in_specs=[vmem] * 4,
        name="pack",
    )(q, g, k, v)


def columns_kernel(in_ref, *out_refs):
    x = lax.axis_index("x")
    for o in range(4):
        target = (x + o) % 4
        for n in range(4):
            src = pl.ds(pl.multiple_of(n * 4 * HEAD + target * HEAD, 128), HEAD)
            out_refs[o][:, n * HEAD : (n + 1) * HEAD] = in_ref[:, src]


def run_columns(layer_input):
    return pl.pallas_call(
        columns_kernel,
        out_shape=[jax.ShapeDtypeStruct((TOK, 4 * HEAD), BF)] * 4,
        in_specs=[pl.BlockSpec(memory_space=pltpu.VMEM)],
        name="columns",
    )(layer_input)


def finish_kernel(in_ref, k_ref, v_ref, got, sem):
    copies = [pltpu.make_async_copy(in_ref.at[n], got.at[n], sem.at[n]) for n in range(16)]
    for copy in copies:
        copy.start()
    for copy in copies:
        copy.wait()
    for h in range(2):
        total = got[h].astype(F32)
        for n in range(1, 8):
            total = total + got[2 * n + h].astype(F32)
        k_ref[:, h * HEAD : (h + 1) * HEAD] = total[:, :HEAD]
        v_ref[:, h * HEAD : (h + 1) * HEAD] = total[:, HEAD:]


def run_finish(got):
    out = jax.ShapeDtypeStruct((HEAD // 2, 2 * HEAD), F32)
    return pl.pallas_call(
        finish_kernel,
        out_shape=[out, out],
        in_specs=[pl.BlockSpec(memory_space=pl.ANY)],
        scratch_shapes=[pltpu.VMEM((16, HEAD // 2, 2 * HEAD), BF), pltpu.SemaphoreType.DMA((16,))],
        name="finish",
    )(got)


def positions(run_placement, y, z, x, c):
    def device(yy, zz, xx, cc):
        return (((yy % 4) * 2 + zz % 2) * 4 + xx % 4) * 2 + cc % 2

    b, a, e = jnp.meshgrid(jnp.arange(4), jnp.arange(2), jnp.arange(2), indexing="ij")
    keys = device(y, z + a, x + b, c + e).reshape(KSLOTS)
    a, e = jnp.meshgrid(jnp.arange(4), jnp.arange(2), indexing="ij")
    queries = device(y + a, z, x, c + e).reshape(QSLOTS)
    index = jnp.concatenate([keys, queries]).astype(jnp.int32)
    pick = (index[:, None] == jnp.arange(64, dtype=jnp.int32)[None, :]).astype(BF)
    slots = nt(pick, run_placement.astype(BF)).astype(BF)
    lane = jnp.arange(TOK, dtype=jnp.int32)
    spread = jnp.where(lane[None, :] // 2 == jnp.arange(64, dtype=jnp.int32)[:, None], 2.0, 0.0).astype(BF)
    pos = nn(slots, spread) + ((lane // 2) * TOK + lane % 2).astype(F32)[None, :]
    kpos = pos[:KSLOTS]
    qpos = pos[KSLOTS:].reshape(QSLOTS, PARTS, T).transpose(1, 0, 2).reshape(PARTS, 1, 1, QSLOTS * T)
    qpos = jnp.broadcast_to(qpos, (PARTS, 1, GROUP, QSLOTS * T)).reshape(PARTS, 1, QR)
    return kpos, qpos


def own_first(c, mine, other, axis):
    return jnp.where(c == 0, jnp.concatenate([mine, other], axis), jnp.concatenate([other, mine], axis))


def after(array, *gates):
    return lax.optimization_barrier((array, *gates))[0]


def step(query_rows, key_rows, value_rows, output_grad, layer_input, key_matrix, value_matrix, run_placement):
    y, z, x, c, t = (lax.axis_index(a) for a in ("y", "z", "x", "c", "tp"))
    kv_pair, qg_pair, kv_send, qg_send = run_pack(query_rows, output_grad, key_rows, value_rows)
    qg_own = qg_pair.at[1].set(moved(qg_send, "c", 1))
    kv_own = kv_pair.at[1].set(moved(kv_send, "c", 1))
    q_next = moved(qg_own, "y", -1)
    q_rest = [moved(qg_own, "y", -o) for o in (2, 3)]
    qgs = [qg_own, q_next] + q_rest
    kv_both = jnp.stack([kv_own, moved(kv_own, "z", 1)])
    kvs = [kv_both] + [moved(kv_both, "x", -o) for o in (1, 2, 3)]
    kpos, qpos = positions(run_placement, y, z, x, c)

    half = key_matrix.shape[0] // 2
    cuts = [lax.dynamic_slice_in_dim(after(m, kv_own), (1 - t) * half, half, 0) for m in (key_matrix, value_matrix)]
    x_pieces = run_columns(after(layer_input, kv_both, qpos))
    x_half = jnp.stack([x_pieces[0]] + [moved(x_pieces[4 - o], "x", -o) for o in (1, 2, 3)])
    x_other = moved(x_half, "tp", 1)
    x_here = jnp.where(t == 0, jnp.concatenate([x_half, x_other], 2), jnp.concatenate([x_other, x_half], 2))
    m_far = moved(jnp.where(c == 0, *cuts), "tp", 1)
    kpos = after(kpos, *x_pieces)

    sts = run_stats(kvs, qgs, kpos, qpos)
    sts = [sts[0]] + [moved(sts[o], "y", -o) for o in (1, 2, 3)]
    dkv_near, dkv_sent, dqs = run_grads(kvs, qgs, kpos, qpos, sts)

    def total_of(own, arrived):
        total = own.astype(F32)
        for a in arrived:
            total = total + a.astype(F32)
        return total.astype(BF)

    first = moved(dkv_sent[0], "z", 1)
    row1, row2 = (total_of(dkv_near[o], [first[o - 1]]) for o in (1, 2))
    last = moved(dkv_sent[1], "z", 1)
    near = after(dkv_near, row1)
    row3, row0 = (total_of(near[o], [last[n]]) for n, o in enumerate((3, 0)))
    dq = total_of(dqs[0], [moved(dqs[o], "y", o) for o in (1, 2, 3)])
    x_all = jnp.stack([x_here, moved(x_here, "c", 1)], axis=1)
    m_core = moved(m_far, "c", 1)
    k_far = jnp.where(c == 0, m_far, m_core)
    v_far = jnp.where(c == 0, m_core, m_far)

    got = [moved(row2, "x", 2), moved(row1, "x", 1)]
    dkv = total_of(row0, got + [moved(row3, "x", 3)])
    dkv_all = jnp.stack([dkv] + [moved(dkv, "x", -o) for o in (1, 2, 3)])
    dkv_far = moved(dkv[1], "c", 1)
    k_here = own_first(c, dkv[0, :, :HEAD], dkv_far[:, :HEAD], 1)
    v_here = own_first(c, dkv[0, :, HEAD:], dkv_far[:, HEAD:], 1)
    kv_here = jnp.concatenate([k_here, v_here], 1)
    kv_there = moved(kv_here, "tp", 1)

    query_grad = own_first(c, dq[0], moved(dq[1], "c", 1), 1)

    tokens = 8 * TOK
    weight = lax.dot_general(
        x_all.reshape(tokens, 8 * HEAD),
        dkv_all.reshape(tokens, 2 * HEAD),
        (((0,), (0,)), ((), ())),
        preferred_element_type=F32,
    )
    pieces = weight.astype(BF).reshape(16, HEAD // 2, 2 * HEAD)
    got = lax.all_to_all(pieces, ("y", "z", "c"), 0, 0, tiled=True)
    key_weight, value_weight = run_finish(got)

    km = lax.dynamic_slice_in_dim(key_matrix, t * half, half, 0)
    vm = lax.dynamic_slice_in_dim(value_matrix, t * half, half, 0)
    wide = 2 * HEAD
    total = nt(kv_here[:, :wide], km) + nt(kv_here[:, wide:], vm)
    input_grad = (total + nt(kv_there[:, :wide], k_far) + nt(kv_there[:, wide:], v_far)).astype(BF)
    return (query_grad, input_grad, key_weight, value_weight)


def solution(mesh):
    torus = Mesh(mesh.devices.reshape(4, 2, 4, 2, mesh.shape["tp"]), ("y", "z", "x", "c", "tp"))
    return jax.shard_map(
        step,
        mesh=torus,
        in_specs=(P(SEQ, "tp"),) * 5 + (P(None, "tp"),) * 2 + (P(),),
        out_specs=(P(SEQ, "tp"),) * 4,
        check_vma=False,
    )
```
